8 devices in a mesh: dp: 2 (over z, y), ep: 4 (over x, core).
Axes of the slice: x: 2, y: 2, z: 1, core: 2. Of those that a mesh axis runs over, the one named last changes fastest.
Arguments:
- tok_x: bfloat16 [512, 2048], P(('dp', 'ep')), parts along dimension 0
- route_ids: int32 [512, 8], P(('dp', 'ep')), parts along dimension 0
- route_gate: float32 [512, 8], P(('dp', 'ep')), parts along dimension 0
- w_in: bfloat16 [128, 2048, 768], P('ep')
- w_out: bfloat16 [128, 768, 2048], P('ep')
- shared_in: bfloat16 [2048, 768], replicated
- shared_out: bfloat16 [768, 2048], replicated
Outputs:
- output: bfloat16 [512, 2048], P(('dp', 'ep')), parts along dimension 0
There are 2 independent parts. The reference program is written for one: setup_inputs(seed, part) draws one part's arguments, and reference() takes and returns one part's arrays. A program takes and returns all parts, laid end to end along the dimension named above; an argument that names none is the same for every part.
All inputs are finite; a program needn't handle non-finite values.
Results may differ from the reference program's by a relative error of at most 0.00521982.
Values are sent between devices in bfloat16 or wider.
A program may use at most 1 GiB of HBM per device.

```python
import jax
import jax.numpy as jnp
from jax import lax

D_MODEL = 2048
FF_EXPERT = 768
FF_SHARED = 768
EXPERTS = 128
TOP_K = 8
TOK_DEV = 64
GROUP_DEV = 4
GROUP_TOK = GROUP_DEV * TOK_DEV
CAPACITY = GROUP_TOK * TOP_K // EXPERTS


def device_routing(dev_counts, rng_key):
    run_ends = jnp.cumsum(dev_counts)
    flat_ids = jnp.searchsorted(run_ends, jnp.arange(TOK_DEV * TOP_K), side='right')
    id_table = flat_ids.reshape(TOP_K, TOK_DEV).T
    key_order, key_turn = jax.random.split(rng_key)
    id_table = id_table[jax.random.permutation(key_order, TOK_DEV)]
    row_turn = jax.random.randint(key_turn, (TOK_DEV, 1), 0, TOP_K)
    col_index = (jnp.arange(TOP_K)[None, :] + row_turn) % TOP_K
    return jnp.take_along_axis(id_table, col_index, axis=1).astype(jnp.int32)


def draw_routing(rng_key):
    avg_load = TOK_DEV * TOP_K // EXPERTS
    spread = avg_load // 2
    half_experts = EXPERTS // 2
    key_bias, key_noise, key_perm, key_rows = jax.random.split(rng_key, 4)
    pair_bias = jax.random.randint(key_bias, (half_experts,), -spread, spread + 1)
    dev_noise = jax.random.randint(key_noise, (GROUP_DEV, half_experts), -spread, spread + 1)
    pair_shift = jnp.clip(pair_bias[None, :] + dev_noise, -avg_load, avg_load)
    forced = jnp.arange(half_experts)[None, :] == (jnp.arange(GROUP_DEV)[:, None] % half_experts)
    pair_shift = jnp.where(forced, avg_load, pair_shift)
    paired = jnp.stack([avg_load + pair_shift, avg_load - pair_shift], axis=-1).reshape(GROUP_DEV, EXPERTS)
    counts = paired[:, jax.random.permutation(key_perm, EXPERTS)]
    row_keys = jax.random.split(key_rows, GROUP_DEV)
    return jax.vmap(device_routing)(counts, row_keys).reshape(GROUP_TOK, TOP_K)


def setup_inputs(seed: int = 0, part: int = 0) -> dict:
    base_key = jax.random.key(seed)
    key_parts, key_weights = jax.random.split(base_key)
    part_key = jax.random.fold_in(key_parts, part)
    key_x, key_route, key_gate = jax.random.split(part_key, 3)
    key_w1, key_w2, key_s1, key_s2 = jax.random.split(key_weights, 4)
    tok_x = jax.random.normal(key_x, (GROUP_TOK, D_MODEL), jnp.float32).astype(jnp.bfloat16)
    route_ids = draw_routing(key_route)
    route_gate = jax.random.uniform(key_gate, (GROUP_TOK, TOP_K), jnp.float32, 0.5, 1.5) * TOP_K ** -0.5
    w_in = (jax.random.normal(key_w1, (EXPERTS, D_MODEL, FF_EXPERT), jnp.float32) * D_MODEL ** -0.5).astype(jnp.bfloat16)
    w_out = (jax.random.normal(key_w2, (EXPERTS, FF_EXPERT, D_MODEL), jnp.float32) * FF_EXPERT ** -0.5).astype(jnp.bfloat16)
    shared_in = (jax.random.normal(key_s1, (D_MODEL, FF_SHARED), jnp.float32) * D_MODEL ** -0.5).astype(jnp.bfloat16)
    shared_out = (jax.random.normal(key_s2, (FF_SHARED, D_MODEL), jnp.float32) * FF_SHARED ** -0.5).astype(jnp.bfloat16)
    return {'tok_x': tok_x, 'route_ids': route_ids, 'route_gate': route_gate, 'w_in': w_in, 'w_out': w_out, 'shared_in': shared_in, 'shared_out': shared_out}


def reference(tok_x, route_ids, route_gate, w_in, w_out, shared_in, shared_out):
    dev_ids = route_ids.reshape(GROUP_DEV, TOK_DEV * TOP_K)

    def count_step(offset, ids_dev):
        onehot = (ids_dev[:, None] == jnp.arange(EXPERTS)[None, :]).astype(jnp.int32)
        running = jnp.cumsum(onehot, axis=0)
        slot_dev = jnp.sum(running * onehot, axis=1) - 1 + offset[ids_dev]
        return offset + running[-1], slot_dev

    _, pair_slot = lax.scan(count_step, jnp.zeros((EXPERTS,), jnp.int32), dev_ids)
    pair_slot = pair_slot.reshape(-1)
    flat_ids = route_ids.reshape(-1)
    keep_pair = pair_slot < CAPACITY
    target = jnp.where(keep_pair, flat_ids * CAPACITY + pair_slot, EXPERTS * CAPACITY)
    pair_tok = jnp.arange(GROUP_TOK * TOP_K) // TOP_K
    tok_at = jnp.full((EXPERTS * CAPACITY,), GROUP_TOK, jnp.int32).at[target].set(pair_tok, mode='drop')
    gate_at = jnp.zeros((EXPERTS * CAPACITY,), jnp.float32).at[target].set(route_gate.reshape(-1), mode='drop')
    x_pad = jnp.concatenate([tok_x, jnp.zeros((1, D_MODEL), tok_x.dtype)], axis=0)

    def expert_step(moe_sum, inputs):
        tok_e, gate_e, w_first, w_second = inputs
        buffer = x_pad[tok_e]
        hidden = jax.nn.gelu(jnp.dot(buffer, w_first, preferred_element_type=jnp.float32)).astype(jnp.bfloat16)
        expert_out = jnp.dot(hidden, w_second, preferred_element_type=jnp.float32).astype(jnp.bfloat16)
        moe_sum = moe_sum.at[tok_e].add(gate_e[:, None] * expert_out.astype(jnp.float32), mode='drop')
        return moe_sum, None

    moe_sum, _ = lax.scan(expert_step, jnp.zeros((GROUP_TOK, D_MODEL), jnp.float32), (tok_at.reshape(EXPERTS, CAPACITY), gate_at.reshape(EXPERTS, CAPACITY), w_in, w_out))

    def shared_block(x_block):
        hidden = jax.nn.gelu(jnp.dot(x_block, shared_in, preferred_element_type=jnp.float32)).astype(jnp.bfloat16)
        return jnp.dot(hidden, shared_out, preferred_element_type=jnp.float32).astype(jnp.bfloat16)

    shared_y = lax.map(shared_block, tok_x.reshape(GROUP_DEV, TOK_DEV, D_MODEL)).reshape(GROUP_TOK, D_MODEL)
    return (tok_x.astype(jnp.float32) + shared_y.astype(jnp.float32) + moe_sum).astype(jnp.bfloat16)
```

```python
import functools

import jax
import jax.numpy as jnp
from jax import lax
from jax.experimental import pallas as pl
from jax.experimental.pallas import tpu as pltpu
from jax.sharding import PartitionSpec as P

F32 = jnp.float32
BF16 = jnp.bfloat16
MESH = pl.DeviceIdType.MESH

ROWS = 64
WIDTH = 2048
FF = 768
TOPK = 8
LOCAL = 16
CAP = 16
CK = 256
NCH = WIDTH // CK
EG = 4
KS = 512
NK = WIDTH // KS
NEG = LOCAL // EG
NA = 9
EB = 8
NB = 4
GROUP = 256
META = NCH


def dot(a, b):
    return jnp.dot(a, b, preferred_element_type=F32)


def tdot(a, b):
    return lax.dot_general(a, b, (((0,), (0,)), ((), ())), preferred_element_type=F32)


def bdot(a, b):
    return lax.dot_general(a, b, (((2,), (1,)), ((0,), (0,))), preferred_element_type=F32)


def kernel(x_ref, meta_ref, win_ref, wout_ref, sin_ref, sout_ref, o_ref,
           tok, meta, wa, wb, so, xs, hacc, hid, osc, disp, comb, ypart, r0, r1, r2, hs, ost,
           ld_sem, g1s, g1r, g2s, g2r, gds, gdr, a_sem, b_sem, sh_sem,
           t0s, t0r, t1s, t1r, t2s, t2r, o_sem):
    my_dp = lax.axis_index('dp')
    my_ep = lax.axis_index('ep')
    my_x = my_ep // 2
    my_c = my_ep % 2
    partner = (my_dp, my_x * 2 + (1 - my_c))
    x_nbr = (my_dp, (1 - my_x) * 2 + my_c)
    y_nbr = (1 - my_dp, my_ep)
    e_off = my_dp * LOCAL

    def a_copy(s):
        k, eg = divmod(s, NEG)
        return pltpu.make_async_copy(
            win_ref.at[pl.ds(e_off + eg * EG, EG), pl.ds(k * KS, KS), :], wa.at[s % NA], a_sem.at[s % NA])

    def b_copy(s):
        c, h = divmod(s, LOCAL // EB)
        return pltpu.make_async_copy(
            wout_ref.at[pl.ds(e_off + h * EB, EB), :, pl.ds(c * CK, CK)], wb.at[s % NB], b_sem.at[s % NB])

    def own(i):
        if i == META:
            return meta.at[my_c, my_dp, my_x]
        if i % 2 == 0:
            return tok.at[i, my_c, my_dp, my_x]
        return tok.at[i, my_c, my_x, my_dp]

    def own_pair(i):
        if i == META:
            return meta.at[my_c, my_dp]
        return tok.at[i, my_c, my_dp] if i % 2 == 0 else tok.at[i, my_c, my_x]

    def own_core(i):
        return meta.at[my_c] if i == META else tok.at[i, my_c]

    def load(i):
        src = meta_ref if i == META else x_ref.at[:, pl.ds(i * CK, CK)]
        return pltpu.make_async_copy(src, own(i), ld_sem.at[i])

    def remote(ref, ssem, rsem, i, dev, dst=None):
        return pltpu.make_async_remote_copy(
            src_ref=ref, dst_ref=ref if dst is None else dst, send_sem=ssem.at[i], recv_sem=rsem.at[i],
            device_id=dev, device_id_type=MESH)

    def gather1(i):
        return remote(own(i), g1s, g1r, i, y_nbr if i % 2 and i != META else x_nbr)

    def gather2(i):
        return remote(own_pair(i), g2s, g2r, i, x_nbr if i % 2 and i != META else y_nbr)

    def gatherd(i):
        return remote(own_core(i), gds, gdr, i, partner)

    items = [META] + list(range(NCH))

    for i in items:
        load(i).start()
    for s in range(NA):
        a_copy(s).start()
    for s in range(NB):
        b_copy(s).start()

    barrier = pltpu.get_barrier_semaphore()
    for dev in (partner, x_nbr, y_nbr):
        pl.semaphore_signal(barrier, inc=1, device_id=dev, device_id_type=MESH)
    pl.semaphore_wait(barrier, 3)

    for i in items:
        load(i).wait()
        gather1(i).start()
    for i in items:
        gather1(i).wait_recv()
        gather2(i).start()
    for i in (META, 0, 1):
        gather2(i).wait_recv()
        gatherd(i).start()
    gatherd(META).wait_recv()

    e_id = (lax.broadcasted_iota(jnp.int32, (LOCAL, GROUP), 0) + (my_ep * (2 * LOCAL) + e_off)).astype(F32)
    s_id = lax.broadcasted_iota(jnp.int32, (LOCAL, CAP, GROUP), 1).astype(F32)

    def true_pos(t):
        return ((t // 64) % 2) * 128 + (t // 128) * 64 + t % 64

    before = (true_pos(lax.broadcasted_iota(jnp.int32, (GROUP, GROUP), 0))
              < true_pos(lax.broadcasted_iota(jnp.int32, (GROUP, GROUP), 1)))
    before = jnp.where(before, 1.0, 0.0).astype(BF16)
    eye = (lax.broadcasted_iota(jnp.int32, (GROUP, GROUP), 0)
           == lax.broadcasted_iota(jnp.int32, (GROUP, GROUP), 1))
    eye = jnp.where(eye, 1.0, 0.0).astype(BF16)
    for g in range(2):
        table = jnp.concatenate([meta[0, g, 0] + meta[0, g, 1], meta[1, g, 0] + meta[1, g, 1]], axis=1)
        chosen = jnp.zeros((LOCAL, GROUP), F32)
        gate = jnp.zeros((LOCAL, GROUP), F32)
        for j in range(TOPK):
            hit = table[j:j + 1, :] == e_id
            chosen = jnp.where(hit, 1.0, chosen)
            gate = jnp.where(hit, table[TOPK + j:TOPK + j + 1, :], gate)
        slot = dot(chosen.astype(BF16), before)
        slot = jnp.where(chosen > 0.0, slot, -1.0)
        here = slot[:, None, :] == s_id
        disp[g] = jnp.where(here, 1.0, 0.0).reshape(LOCAL * CAP, GROUP).astype(BF16)
        weight = jnp.where(here, gate[:, None, :], 0.0).reshape(LOCAL * CAP, GROUP)
        for piece in range(3):
            part = weight.astype(BF16)
            comb[g, piece] = tdot(part, eye).astype(BF16)
            weight = weight - part.astype(F32)

    for k in range(NK):
        for h in range(2):
            i = 2 * k + h
            gatherd(i).wait_recv()
            for g in range(2):
                rows = tok[i, :, g] if i % 2 == 0 else tok[i, :, :, g]
                picked = dot(disp[g], rows.reshape(GROUP, CK)).astype(BF16)
                xs[:, pl.ds(g * CAP, CAP), pl.ds(h * CK, CK)] = picked.reshape(LOCAL, CAP, CK)
        for eg in range(NEG):
            s = k * NEG + eg
            a_copy(s).wait()
            batch = pl.ds(eg * EG, EG)
            acc = bdot(xs[batch], wa[s % NA])
            if k > 0:
                acc = acc + hacc[batch]
            if k < NK - 1:
                hacc[batch] = acc
            else:
                hid[batch] = jax.nn.gelu(acc).astype(BF16)
            if s + NA < NK * NEG:
                a_copy(s + NA).start()
            if eg == 1 and k < NK - 1:
                for i in (2 * k + 2, 2 * k + 3):
                    gather2(i).wait_recv()
                    gatherd(i).start()

    def dirs(c):
        if c % 2 == 0:
            return my_x, my_dp, x_nbr, y_nbr
        return my_dp, my_x, y_nbr, x_nbr

    def reduce0(c):
        return remote(ypart.at[c, 1 - my_c], t0s, t0r, c, partner, r0.at[c])

    def reduce1(c):
        a, _, dev, _ = dirs(c)
        return remote(ypart.at[c, my_c, 1 - a], t1s, t1r, c, dev, r1.at[c])

    def reduce2(c):
        a, b, _, dev = dirs(c)
        return remote(ypart.at[c, my_c, a, 1 - b], t2s, t2r, c, dev, r2.at[c])

    def stage1(c):
        a, _, _, _ = dirs(c)
        reduce0(c).wait_recv()
        ypart[c, my_c, 1 - a] = ypart[c, my_c, 1 - a] + r0[c, 1 - a]
        reduce1(c).start()
        ypart[c, my_c, a] = ypart[c, my_c, a] + r0[c, a]

    def stage2(c):
        a, b, _, _ = dirs(c)
        reduce1(c).wait_recv()
        ypart[c, my_c, a, 1 - b] = ypart[c, my_c, a, 1 - b] + r1[c, 1 - b]
        reduce2(c).start()

    def sh_in():
        return pltpu.make_async_copy(sin_ref, wa.at[(NK * NEG) % NA], sh_sem.at[0])

    def sh_out():
        return pltpu.make_async_copy(sout_ref, so, sh_sem.at[1])

    nsteps = NCH * (LOCAL // EB)
    for c in range(NCH):
        for h in range(LOCAL // EB):
            s = c * (LOCAL // EB) + h
            b_copy(s).wait()
            out = bdot(hid[pl.ds(h * EB, EB)], wb[s % NB]).astype(BF16)
            for g in range(2):
                osc[g, pl.ds(h * EB, EB)] = out[:, g * CAP:(g + 1) * CAP]
            if s + NB < nsteps:
                b_copy(s + NB).start()
            elif s + NB == nsteps:
                sh_in().start()
                sh_out().start()
        for g in range(2):
            rows = osc[g].reshape(LOCAL * CAP, CK)
            y = dot(comb[g, 0], rows) + dot(comb[g, 1], rows) + dot(comb[g, 2], rows)
            y = y.reshape(2, 2, ROWS, CK)
            for core in range(2):
                for x in range(2):
                    if c % 2 == 0:
                        ypart[c, core, x, g] = y[core, x]
                    else:
                        ypart[c, core, g, x] = y[core, x]
        reduce0(c).start()
        if c >= 1:
            stage1(c - 1)
        if c >= 3:
            stage2(c - 3)
    stage1(NCH - 1)
    stage2(NCH - 3)

    sh_in().wait()
    acc = jnp.zeros((ROWS, FF), F32)
    for k in range(NK):
        left = own(2 * k)[...]
        right = own(2 * k + 1)[...]
        acc = acc + dot(jnp.concatenate([left, right], axis=1), wa[(NK * NEG) % NA, k])
    hs[...] = jax.nn.gelu(acc).astype(BF16)
    stage2(NCH - 2)
    sh_out().wait()
    stage2(NCH - 1)
    for c in range(NCH):
        shared = dot(hs[...], so[:, pl.ds(c * CK, CK)]).astype(BF16).astype(F32)
        a, b, _, _ = dirs(c)
        reduce2(c).wait_recv()
        moe = ypart[c, my_c, a, b] + r1[c, b] + r2[c]
        ost[:, pl.ds(c * CK, CK)] = (own(c)[...].astype(F32) + shared + moe).astype(BF16)
    out = pltpu.make_async_copy(ost, o_ref, o_sem)
    out.start()
    for i in items:
        gather1(i).wait_send()
        gather2(i).wait_send()
        gatherd(i).wait_send()
    for c in range(NCH):
        reduce0(c).wait_send()
        reduce1(c).wait_send()
        reduce2(c).wait_send()
    out.wait()


def solution(mesh):
    def layer(tok_x, route_ids, route_gate, w_in, w_out, shared_in, shared_out):
        table = jnp.concatenate([route_ids.T.astype(F32), route_gate.T], axis=0)
        first = jnp.pad(table, ((0, 0), (0, 128 - ROWS)))
        second = jnp.pad(table, ((0, 0), (128 - ROWS, 0)))
        table = jnp.where(lax.axis_index('ep') // 2 == 0, first, second)
        hbm = pl.BlockSpec(memory_space=pl.ANY)
        dma = pltpu.SemaphoreType.DMA
        vmem = pltpu.VMEM
        return pl.pallas_call(
            kernel,
            out_shape=jax.ShapeDtypeStruct((ROWS, WIDTH), BF16),
            in_specs=[hbm] * 6,
            out_specs=hbm,
            scratch_shapes=[
                vmem((NCH, 2, 2, 2, ROWS, CK), BF16),
                vmem((2, 2, 2, 2 * TOPK, 128), F32),
                vmem((NA, EG, KS, FF), BF16),
                vmem((NB, EB, FF, CK), BF16),
                vmem((FF, WIDTH), BF16),
                vmem((LOCAL, 2 * CAP, KS), BF16),
                vmem((LOCAL, 2 * CAP, FF), F32),
                vmem((LOCAL, 2 * CAP, FF), BF16),
                vmem((2, LOCAL, CAP, CK), BF16),
                vmem((2, LOCAL * CAP, GROUP), BF16),
                vmem((2, 3, GROUP, LOCAL * CAP), BF16),
                vmem((NCH, 2, 2, 2, ROWS, CK), F32),
                vmem((NCH, 2, 2, ROWS, CK), F32),
                vmem((NCH, 2, ROWS, CK), F32),
                vmem((NCH, ROWS, CK), F32),
                vmem((ROWS, FF), BF16),
                vmem((ROWS, WIDTH), BF16),
                dma((NCH + 1,)),
                dma((NCH + 1,)), dma((NCH + 1,)),
                dma((NCH + 1,)), dma((NCH + 1,)),
                dma((NCH + 1,)), dma((NCH + 1,)),
                dma((NA,)), dma((NB,)), dma((2,)),
                dma((NCH,)), dma((NCH,)), dma((NCH,)), dma((NCH,)), dma((NCH,)), dma((NCH,)),
                dma,
            ],
            compiler_params=pltpu.CompilerParams(
                collective_id=0, has_side_effects=True, vmem_limit_bytes=66_000_000),
            name='moe_layer',
        )(tok_x, table, w_in, w_out, shared_in.reshape(NK, KS, FF), shared_out)

    row_spec = P(('dp', 'ep'), None)
    expert_spec = P('ep', None, None)
    whole_spec = P(None, None)
    return jax.shard_map(layer, mesh=mesh,
                         in_specs=(row_spec, row_spec, row_spec, expert_spec, expert_spec, whole_spec, whole_spec),
                         out_specs=row_spec, check_vma=False)
```

```python
import jax
import jax.numpy as jnp
from jax import lax
from jax.experimental import pallas as pl
from jax.experimental.pallas import tpu as pltpu
from jax.sharding import PartitionSpec as P

F32 = jnp.float32
BF16 = jnp.bfloat16
MESH = pl.DeviceIdType.MESH

ROWS = 64
WIDTH = 2048
FF = 768
TOPK = 8
LOCAL = 16
CAP = 16
T = 256
NCH = WIDTH // T
EG = 4
KS = 2 * T
NK = WIDTH // KS
NEG = LOCAL // EG
EB = 8
NHB = LOCAL // EB
NF = FF // T
GROUP = 256
NS = 15
A_STEPS = NK * NEG
B_STEPS = NCH * NHB
SH_IN = A_STEPS + B_STEPS
SH_OUT = SH_IN + 1
STEPS = SH_OUT + 1
LAG2 = 4


def dot(a, b):
    return jnp.dot(a, b, preferred_element_type=F32)


def tdot(a, b):
    return lax.dot_general(a, b, (((0,), (0,)), ((), ())), preferred_element_type=F32)


def bdot(a, b):
    return lax.dot_general(a, b, (((2,), (1,)), ((0,), (0,))), preferred_element_type=F32)


def kernel(x_ref, ids_ref, gates_ref, win_ref, wout_ref, sin_ref, sout_ref, o_ref,
           tok, mids, mgates, ring, xs, hacc, hid, osc, disp, comb, ypart, r0, r1, r2, hs, shy, ost,
           ld_sem, g1s, g1r, g2s, g2r, gds, gdr, w_sem, so_sem,
           t0s, t0r, t1s, t1r, t2s, t2r, o_sem):
    my_dp = lax.axis_index('dp')
    my_ep = lax.axis_index('ep')
    my_x = my_ep // 2
    my_c = my_ep % 2
    partner = (my_dp, my_x * 2 + (1 - my_c))
    x_nbr = (my_dp, (1 - my_x) * 2 + my_c)
    y_nbr = (1 - my_dp, my_ep)
    e_off = my_dp * LOCAL

    def w_copies(s):
        slot = s % NS
        if s == SH_OUT:
            return [pltpu.make_async_copy(
                sout_ref.at[:, :, pl.ds(c * T, T)], ring.at[slot, :, c // 2, c % 2], so_sem.at[c]) for c in range(NCH)]
        copies = []
        for n in range(NF):
            if s < A_STEPS:
                k, eg = divmod(s, NEG)
                src = win_ref.at[pl.ds(e_off + eg * EG, EG), pl.ds(2 * k, 2), :, pl.ds(n * T, T)]
            elif s < SH_IN:
                c, h = divmod(s - A_STEPS, NHB)
                src = wout_ref.at[pl.ds(e_off // 2 + h * (EB // 2), EB // 2), :, n, :, pl.ds(c * T, T)]
            else:
                src = sin_ref.at[:, :, :, pl.ds(n * T, T)]
            copies.append(pltpu.make_async_copy(src, ring.at[slot, n], w_sem.at[slot, n]))
        return copies

    def w_start(s):
        if s < STEPS:
            for copy in w_copies(s):
                copy.start()

    def w_wait(s):
        for copy in w_copies(s):
            copy.wait()

    IDS, GATES = NCH, NCH + 1

    def over_y(i):
        return i < NCH and i % 2 == 1

    def buffer(i):
        return mids if i == IDS else mgates if i == GATES else tok.at[i]

    def own_core(i):
        return buffer(i).at[my_c]

    def own_pair(i):
        return buffer(i).at[my_c, my_x if over_y(i) else my_dp]

    def own(i):
        return buffer(i).at[my_c, my_x, my_dp] if over_y(i) else buffer(i).at[my_c, my_dp, my_x]

    def load(i):
        src = ids_ref if i == IDS else gates_ref if i == GATES else x_ref.at[:, pl.ds(i * T, T)]
        return pltpu.make_async_copy(src, own(i), ld_sem.at[i])

    def remote(src, dst, ssem, rsem, dev):
        return pltpu.make_async_remote_copy(
            src_ref=src, dst_ref=dst, send_sem=ssem, recv_sem=rsem, device_id=dev, device_id_type=MESH)

    def gather1(i):
        return remote(own(i), own(i), g1s.at[i], g1r.at[i], y_nbr if over_y(i) else x_nbr)

    def gather2(i):
        return remote(own_pair(i), own_pair(i), g2s.at[i], g2r.at[i], x_nbr if over_y(i) else y_nbr)

    def gatherd(i):
        return remote(own_core(i), own_core(i), gds.at[i], gdr.at[i], partner)

    routing = [IDS, GATES]
    items = routing + list(range(NCH))

    barrier = pltpu.get_barrier_semaphore()
    for dev in (partner, x_nbr, y_nbr):
        pl.semaphore_signal(barrier, inc=1, device_id=dev, device_id_type=MESH)
    for i in items:
        load(i).start()
    for i in items:
        load(i).wait()
    for s in range(NS):
        w_start(s)
    pl.semaphore_wait(barrier, 3)
    for i in items:
        gather1(i).start()
    for i in items:
        gather1(i).wait_recv()
        gather2(i).start()
    for i in routing + [0, 1]:
        gather2(i).wait_recv()
        gatherd(i).start()
    for i in routing:
        gatherd(i).wait_recv()

    e_id = lax.broadcasted_iota(jnp.int32, (LOCAL, GROUP), 0) + (my_ep * (2 * LOCAL) + e_off)
    s_id = lax.broadcasted_iota(jnp.int32, (LOCAL, CAP, GROUP), 1).astype(F32)

    def true_pos(t):
        return ((t // 64) % 2) * 128 + (t // 128) * 64 + t % 64

    t_row = lax.broadcasted_iota(jnp.int32, (GROUP, GROUP), 0)
    t_col = lax.broadcasted_iota(jnp.int32, (GROUP, GROUP), 1)
    before = jnp.where(true_pos(t_row) < true_pos(t_col), 1.0, 0.0).astype(BF16)
    eye = jnp.where(t_row == t_col, 1.0, 0.0).astype(BF16)
    for g in range(2):
        ids = jnp.concatenate([mids[c, g, x] for c in range(2) for x in range(2)], axis=1)
        gates = jnp.concatenate([mgates[c, g, x] for c in range(2) for x in range(2)], axis=1)
        chosen = jnp.zeros((LOCAL, GROUP), F32)
        gate = jnp.zeros((LOCAL, GROUP), F32)
        for j in range(TOPK):
            hit = ids[j:j + 1, :] == e_id
            chosen = jnp.where(hit, 1.0, chosen)
            gate = jnp.where(hit, gates[j:j + 1, :], gate)
        slot = dot(chosen.astype(BF16), before)
        slot = jnp.where(chosen > 0.0, slot, -1.0)
        here = slot[:, None, :] == s_id
        disp[g] = jnp.where(here, 1.0, 0.0).reshape(LOCAL * CAP, GROUP).astype(BF16)
        weight = jnp.where(here, gate[:, None, :], 0.0).reshape(LOCAL * CAP, GROUP)
        for piece in range(3):
            part = weight.astype(BF16)
            comb[g, piece] = tdot(part, eye).astype(BF16)
            weight = weight - part.astype(F32)

    for k in range(NK):
        for h in range(2):
            gatherd(2 * k + h).wait_recv()
        for h in range(2):
            i = 2 * k + h
            for g in range(2):
                rows = tok[i, :, :, g] if over_y(i) else tok[i, :, g]
                picked = dot(disp[g], rows.reshape(GROUP, T)).astype(BF16)
                xs[:, pl.ds(g * CAP, CAP), pl.ds(h * T, T)] = picked.reshape(LOCAL, CAP, T)
        for eg in range(NEG):
            s = k * NEG + eg
            batch = pl.ds(eg * EG, EG)
            w_wait(s)
            for n in range(NF):
                cols = pl.ds(n * T, T)
                acc = bdot(xs[batch], ring[s % NS, n].reshape(EG, KS, T))
                if k > 0:
                    acc = acc + hacc[batch, :, cols]
                if k < NK - 1:
                    hacc[batch, :, cols] = acc
                else:
                    hid[batch, :, cols] = jax.nn.gelu(acc).astype(BF16)
            w_start(s + NS)
            if eg == 1 and k < NK - 1:
                for i in (2 * k + 2, 2 * k + 3):
                    gather2(i).wait_recv()
                    gatherd(i).start()

    def dirs(c):
        if c % 2 == 0:
            return my_x, my_dp, x_nbr, y_nbr
        return my_dp, my_x, y_nbr, x_nbr

    def reduce0(c):
        return remote(ypart.at[c, 1 - my_c], r0.at[c], t0s.at[c], t0r.at[c], partner)

    def reduce1(c, last):
        a, b, dev, _ = dirs(c)
        side = b if last else 1 - b
        return remote(ypart.at[c, my_c, 1 - a, side], r1.at[c, side], t1s.at[c, last], t1r.at[c, last], dev)

    def reduce2(c):
        a, b, _, dev = dirs(c)
        return remote(ypart.at[c, my_c, a, 1 - b], r2.at[c], t2s.at[c], t2r.at[c], dev)

    def stage1(c):
        a, b, _, _ = dirs(c)
        reduce0(c).wait_recv()
        ypart[c, my_c, 1 - a] = ypart[c, my_c, 1 - a] + r0[c, 1 - a]
        reduce1(c, 0).start()
        reduce1(c, 1).start()
        ypart[c, my_c, a] = ypart[c, my_c, a] + r0[c, a]

    def stage2(c):
        a, b, _, _ = dirs(c)
        reduce1(c, 0).wait_recv()
        ypart[c, my_c, a, 1 - b] = ypart[c, my_c, a, 1 - b] + r1[c, 1 - b]
        reduce2(c).start()

    def write(c):
        return pltpu.make_async_copy(ost.at[c], o_ref.at[:, pl.ds(c * T, T)], o_sem.at[c])

    def final(c):
        a, b, _, _ = dirs(c)
        reduce1(c, 1).wait_recv()
        reduce2(c).wait_recv()
        moe = ypart[c, my_c, a, b] + r1[c, b] + r2[c]
        ost[c] = (own(c)[...].astype(F32) + shy[:, pl.ds(c * T, T)].astype(F32) + moe).astype(BF16)
        write(c).start()

    for c in range(NCH):
        for h in range(NHB):
            s = A_STEPS + c * NHB + h
            batch = pl.ds(h * EB, EB)
            w_wait(s)
            out = bdot(hid[batch, :, pl.ds(0, T)], ring[s % NS, 0].reshape(EB, T, T))
            for j in range(1, NF):
                out = out + bdot(hid[batch, :, pl.ds(j * T, T)], ring[s % NS, j].reshape(EB, T, T))
            out = out.astype(BF16)
            for g in range(2):
                osc[g, batch] = out[:, g * CAP:(g + 1) * CAP]
            w_start(s + NS)
        for g in range(2):
            rows = osc[g].reshape(LOCAL * CAP, T)
            y = dot(comb[g, 0], rows) + dot(comb[g, 1], rows) + dot(comb[g, 2], rows)
            y = y.reshape(2, 2, ROWS, T)
            for core in range(2):
                for x in range(2):
                    if c % 2 == 0:
                        ypart[c, core, x, g] = y[core, x]
                    else:
                        ypart[c, core, g, x] = y[core, x]
        reduce0(c).start()
        if c >= 1:
            stage1(c - 1)
        if c >= LAG2:
            stage2(c - LAG2)
    stage1(NCH - 1)

    stage2(NCH - LAG2)
    w_wait(SH_IN)
    for n in range(NF):
        acc = jnp.zeros((ROWS, T), F32)
        weights = ring[SH_IN % NS, n].reshape(NCH, T, T)
        for k in range(NCH):
            acc = acc + dot(own(k)[...], weights[k])
        hs[:, pl.ds(n * T, T)] = jax.nn.gelu(acc).astype(BF16)
    stage2(NCH - LAG2 + 1)
    w_wait(SH_OUT)
    for c in range(NCH):
        acc = jnp.zeros((ROWS, T), F32)
        for j in range(NF):
            acc = acc + dot(hs[:, pl.ds(j * T, T)], ring[SH_OUT % NS, j, c // 2, c % 2])
        shy[:, pl.ds(c * T, T)] = acc.astype(BF16)
    stage2(NCH - 2)
    stage2(NCH - 1)
    for c in range(NCH):
        final(c)
    for i in items:
        gather1(i).wait_send()
        gather2(i).wait_send()
        gatherd(i).wait_send()
    for c in range(NCH):
        reduce0(c).wait_send()
        reduce1(c, 0).wait_send()
        reduce1(c, 1).wait_send()
        reduce2(c).wait_send()
        write(c).wait()


def solution(mesh):
    def layer(tok_x, route_ids, route_gate, w_in, w_out, shared_in, shared_out):
        local = w_in.shape[0]
        any_space = pl.BlockSpec(memory_space=pl.ANY)
        dma = pltpu.SemaphoreType.DMA
        vmem = pltpu.VMEM
        return pl.pallas_call(
            kernel,
            out_shape=jax.ShapeDtypeStruct((ROWS, WIDTH), BF16),
            in_specs=[any_space] * 7,
            out_specs=any_space,
            scratch_shapes=[
                vmem((NCH, 2, 2, 2, ROWS, T), BF16),
                vmem((2, 2, 2, TOPK, ROWS), jnp.int32),
                vmem((2, 2, 2, TOPK, ROWS), F32),
                vmem((NS, NF, EG, 2, T, T), BF16),
                vmem((LOCAL, 2 * CAP, KS), BF16),
                vmem((LOCAL, 2 * CAP, FF), F32),
                vmem((LOCAL, 2 * CAP, FF), BF16),
                vmem((2, LOCAL, CAP, T), BF16),
                vmem((2, LOCAL * CAP, GROUP), BF16),
                vmem((2, 3, GROUP, LOCAL * CAP), BF16),
                vmem((NCH, 2, 2, 2, ROWS, T), F32),
                vmem((NCH, 2, 2, ROWS, T), F32),
                vmem((NCH, 2, ROWS, T), F32),
                vmem((NCH, ROWS, T), F32),
                vmem((ROWS, FF), BF16),
                vmem((ROWS, WIDTH), BF16),
                vmem((NCH, ROWS, T), BF16),
                dma((NCH + 2,)),
                dma((NCH + 2,)), dma((NCH + 2,)),
                dma((NCH + 2,)), dma((NCH + 2,)),
                dma((NCH + 2,)), dma((NCH + 2,)),
                dma((NS, NF)), dma((NCH,)),
                dma((NCH,)), dma((NCH,)), dma((NCH, 2)), dma((NCH, 2)), dma((NCH,)), dma((NCH,)),
                dma((NCH,)),
            ],
            compiler_params=pltpu.CompilerParams(
                collective_id=0, has_side_effects=True, vmem_limit_bytes=67_000_000),
            name='moe_layer',
        )(tok_x, route_ids.T, route_gate.T,
          w_in.reshape(local, WIDTH // T, T, FF), w_out.reshape(local // 2, 2, NF, T, WIDTH),
          shared_in.reshape(EG, 2, T, FF), shared_out.reshape(NF, T, WIDTH))

    row_spec = P(('dp', 'ep'), None)
    expert_spec = P('ep', None, None)
    whole_spec = P(None, None)
    return jax.shard_map(layer, mesh=mesh,
                         in_specs=(row_spec, row_spec, row_spec, expert_spec, expert_spec, whole_spec, whole_spec),
                         out_specs=row_spec, check_vma=False)
```

```python
import jax
import jax.numpy as jnp
from jax import lax
from jax.experimental import pallas as pl
from jax.experimental.pallas import tpu as pltpu
from jax.sharding import PartitionSpec as P

F32 = jnp.float32
BF16 = jnp.bfloat16
MESH = pl.DeviceIdType.MESH

ROWS = 64
WIDTH = 2048
FF = 768
TOPK = 8
LOCAL = 16
CAP = 16
T = 256
NCH = WIDTH // T
EG = 4
KS = 2 * T
NK = WIDTH // KS
NEG = LOCAL // EG
EB = 8
NHB = LOCAL // EB
NF = FF // T
GROUP = 256
NS = 15
A_STEPS = NK * NEG
B_STEPS = NCH * NHB
SH_IN = A_STEPS + B_STEPS
SH_OUT = SH_IN + 1
STEPS = SH_OUT + 1
LAG2 = 4


def dot(a, b):
    return jnp.dot(a, b, preferred_element_type=F32)


class Mark:
    def __init__(self):
        self.cm = None

    def __call__(self, name):
        if self.cm is not None:
            self.cm.__exit__(None, None, None)
            self.cm = None
        if name:
            self.cm = jax.named_scope(name)
            self.cm.__enter__()


MARK = Mark()


def tdot(a, b):
    return lax.dot_general(a, b, (((0,), (0,)), ((), ())), preferred_element_type=F32)


def bdot(a, b):
    return lax.dot_general(a, b, (((2,), (1,)), ((0,), (0,))), preferred_element_type=F32)


def kernel(x_ref, ids_ref, gates_ref, win_ref, wout_ref, wpair_ref, sin_ref, sout_ref, o_ref,
           tok, mids, mgates, ring, xs, hacc, hid, hid3, osc, disp, comb, comb3, ypart, r0, r1, r2, hs, shy, ost,
           ld_sem, g1s, g1r, g2s, g2r, gds, gdr, w_sem, so_sem,
           t0s, t0r, t1s, t1r, t2s, t2r, o_sem):
    my_dp = lax.axis_index('dp')
    my_ep = lax.axis_index('ep')
    my_x = my_ep // 2
    my_c = my_ep % 2
    partner = (my_dp, my_x * 2 + (1 - my_c))
    x_nbr = (my_dp, (1 - my_x) * 2 + my_c)
    y_nbr = (1 - my_dp, my_ep)
    e_off = my_dp * LOCAL

    def w_copies(s):
        slot = s % NS
        if s == SH_OUT:
            return [pltpu.make_async_copy(
                sout_ref.at[:, :, pl.ds(c * T, T)], ring.at[slot, :, c // 2, c % 2], so_sem.at[c]) for c in range(NCH)]
        copies = []
        for n in range(NF):
            if s < A_STEPS:
                k, eg = divmod(s, NEG)
                src = win_ref.at[pl.ds(e_off + eg * EG, EG), pl.ds(2 * k, 2), :, pl.ds(n * T, T)]
            elif s < SH_IN:
                c, h = divmod(s - A_STEPS, NHB)
                if n < 2:
                    src = wout_ref.at[pl.ds(e_off + h * EB + n * EG, EG), pl.ds(0, 2), :, pl.ds(c * T, T)]
                else:
                    src = wpair_ref.at[pl.ds(e_off // 2 + h * EG, EG), :, 2, :, pl.ds(c * T, T)]
            else:
                src = sin_ref.at[:, :, :, pl.ds(n * T, T)]
            copies.append(pltpu.make_async_copy(src, ring.at[slot, n], w_sem.at[slot, n]))
        return copies

    def w_start(s):
        if s < STEPS:
            for copy in w_copies(s):
                copy.start()

    def w_wait(s):
        for copy in w_copies(s):
            copy.wait()

    IDS, GATES = NCH, NCH + 1

    def over_y(i):
        return i < NCH and i % 2 == 1

    def buffer(i):
        return mids if i == IDS else mgates if i == GATES else tok.at[i]

    def own_core(i):
        return buffer(i).at[my_c]

    def own_pair(i):
        return buffer(i).at[my_c, my_x if over_y(i) else my_dp]

    def own(i):
        return buffer(i).at[my_c, my_x, my_dp] if over_y(i) else buffer(i).at[my_c, my_dp, my_x]

    def load(i):
        src = ids_ref if i == IDS else gates_ref if i == GATES else x_ref.at[:, pl.ds(i * T, T)]
        return pltpu.make_async_copy(src, own(i), ld_sem.at[i])

    def remote(src, dst, ssem, rsem, dev):
        return pltpu.make_async_remote_copy(
            src_ref=src, dst_ref=dst, send_sem=ssem, recv_sem=rsem, device_id=dev, device_id_type=MESH)

    def gather1(i):
        return remote(own(i), own(i), g1s.at[i], g1r.at[i], y_nbr if over_y(i) else x_nbr)

    def gather2(i):
        return remote(own_pair(i), own_pair(i), g2s.at[i], g2r.at[i], x_nbr if over_y(i) else y_nbr)

    def gatherd(i):
        return remote(own_core(i), own_core(i), gds.at[i], gdr.at[i], partner)

    routing = [IDS, GATES]
    items = routing + list(range(NCH))

    MARK('sig')
    barrier = pltpu.get_barrier_semaphore()
    for dev in (partner, x_nbr, y_nbr):
        pl.semaphore_signal(barrier, inc=1, device_id=dev, device_id_type=MESH)
    for i in items:
        load(i).start()
    hid3[...] = jnp.zeros_like(hid3)
    MARK('ld')
    for i in items:
        load(i).wait()
    MARK('ws')
    for s in range(NS):
        w_start(s)
    MARK('barrier')
    pl.semaphore_wait(barrier, 3)

    def send_on(i):
        gather1(i).wait_recv()
        gather2(i).start()

    def share(i):
        gather2(i).wait_recv()
        gatherd(i).start()

    MARK('g1')
    for i in items[:6]:
        gather1(i).start()
    MARK('g2a')
    for i in items[:4]:
        send_on(i)
    for i in items[6:]:
        gather1(i).start()
    MARK('g2b')
    for i in items[4:6]:
        send_on(i)
    MARK('gdr')
    for i in routing:
        share(i)
    MARK('g2c')
    for i in items[6:8]:
        send_on(i)
    MARK('gdw')
    for i in routing:
        gatherd(i).wait_recv()

    MARK('route')
    e_id = lax.broadcasted_iota(jnp.int32, (LOCAL, GROUP), 0) + (my_ep * (2 * LOCAL) + e_off)
    s_id = lax.broadcasted_iota(jnp.int32, (LOCAL, CAP, GROUP), 1).astype(F32)

    def true_pos(t):
        return ((t // 64) % 2) * 128 + (t // 128) * 64 + t % 64

    t_row = lax.broadcasted_iota(jnp.int32, (GROUP, GROUP), 0)
    t_col = lax.broadcasted_iota(jnp.int32, (GROUP, GROUP), 1)
    before = jnp.where(true_pos(t_row) < true_pos(t_col), 1.0, 0.0).astype(BF16)
    eye = jnp.where(t_row == t_col, 1.0, 0.0).astype(BF16)
    for g in range(2):
        ids = jnp.concatenate([mids[c, g, x] for c in range(2) for x in range(2)], axis=1)
        gates = jnp.concatenate([mgates[c, g, x] for c in range(2) for x in range(2)], axis=1)
        chosen = jnp.zeros((LOCAL, GROUP), F32)
        gate = jnp.zeros((LOCAL, GROUP), F32)
        for j in range(TOPK):
            hit = ids[j:j + 1, :] == e_id
            chosen = jnp.where(hit, 1.0, chosen)
            gate = jnp.where(hit, gates[j:j + 1, :], gate)
        slot = dot(chosen.astype(BF16), before)
        slot = jnp.where(chosen > 0.0, slot, -1.0)
        here = slot[:, None, :] == s_id
        disp[g] = jnp.where(here, 1.0, 0.0).reshape(LOCAL * CAP, GROUP).astype(BF16)
        weight = jnp.where(here, gate[:, None, :], 0.0).reshape(LOCAL * CAP, GROUP)
        for piece in range(3):
            part = weight.astype(BF16)
            turned = tdot(part, eye).astype(BF16)
            if piece < 2:
                comb[g, :, pl.ds(piece * GROUP, GROUP)] = turned
            else:
                comb3[g] = turned
            weight = weight - part.astype(F32)

    MARK('share0')
    for i in (0, 1):
        share(i)
    MARK('g2d')
    for i in items[8:]:
        send_on(i)
    for k in range(NK):
        MARK(f'gw{k}')
        for h in range(2):
            gatherd(2 * k + h).wait_recv()
        MARK(f'dsp{k}')
        for h in range(2):
            i = 2 * k + h
            for g in range(2):
                rows = tok[i, :, :, g] if over_y(i) else tok[i, :, g]
                picked = dot(disp[g], rows.reshape(GROUP, T)).astype(BF16)
                xs[:, pl.ds(g * CAP, CAP), pl.ds(h * T, T)] = picked.reshape(LOCAL, CAP, T)
        for half in range(2):
            steps = [k * NEG + half * 2 + q for q in range(2)]
            MARK(f'aw{k}{half}')
            for s in steps:
                w_wait(s)
            MARK(f'a{k}{half}')
            for s in steps:
                eg = s % NEG
                batch = pl.ds(eg * EG, EG)
                for n in range(NF):
                    cols = pl.ds(n * T, T)
                    acc = bdot(xs[batch], ring[s % NS, n].reshape(EG, KS, T))
                    if k > 0:
                        acc = acc + hacc[batch, :, cols]
                    if k < NK - 1:
                        hacc[batch, :, cols] = acc
                        continue
                    act = jax.nn.gelu(acc).astype(BF16)
                    if n < 2:
                        hid[batch, :, cols] = act
                    else:
                        act = act.reshape(EG // 2, 2, 2 * CAP, T)
                        for m in range(2):
                            hid3[pl.ds(eg * EG // 2, EG // 2), pl.ds(m * 2 * CAP, 2 * CAP), pl.ds(m * T, T)] = act[:, m]
            for s in steps:
                w_start(s + NS)
            MARK(f'fw{k}')
            if half == 0 and k < NK - 1:
                for i in (2 * k + 2, 2 * k + 3):
                    share(i)

    def dirs(c):
        if c % 2 == 0:
            return my_x, my_dp, x_nbr, y_nbr
        return my_dp, my_x, y_nbr, x_nbr

    def reduce0(c):
        return remote(ypart.at[c, 1 - my_c], r0.at[c], t0s.at[c], t0r.at[c], partner)

    def reduce1(c, last):
        a, b, dev, _ = dirs(c)
        side = b if last else 1 - b
        return remote(ypart.at[c, my_c, 1 - a, side], r1.at[c, side], t1s.at[c, last], t1r.at[c, last], dev)

    def reduce2(c):
        a, b, _, dev = dirs(c)
        return remote(ypart.at[c, my_c, a, 1 - b], r2.at[c], t2s.at[c], t2r.at[c], dev)

    def stage1(c):
        a, b, _, _ = dirs(c)
        MARK(f's1_{c}')
        reduce0(c).wait_recv()
        ypart[c, my_c, 1 - a] = ypart[c, my_c, 1 - a] + r0[c, 1 - a]
        reduce1(c, 0).start()
        reduce1(c, 1).start()
        ypart[c, my_c, a] = ypart[c, my_c, a] + r0[c, a]

    def stage2(c):
        a, b, _, _ = dirs(c)
        MARK(f's2_{c}')
        reduce1(c, 0).wait_recv()
        ypart[c, my_c, a, 1 - b] = ypart[c, my_c, a, 1 - b] + r1[c, 1 - b]
        reduce2(c).start()

    def write(c):
        return pltpu.make_async_copy(ost.at[c], o_ref.at[:, pl.ds(c * T, T)], o_sem.at[c])

    def final(c):
        a, b, _, _ = dirs(c)
        MARK(f'fin{c}')
        reduce1(c, 1).wait_recv()
        reduce2(c).wait_recv()
        moe = ypart[c, my_c, a, b] + r1[c, b] + r2[c]
        ost[c] = (own(c)[...].astype(F32) + shy[:, pl.ds(c * T, T)].astype(F32) + moe).astype(BF16)
        write(c).start()

    for c in range(NCH):
        for h in range(NHB):
            s = A_STEPS + c * NHB + h
            MARK(f'bw{s}')
            w_wait(s)
            MARK(f'b{s}')
            third = bdot(hid3[pl.ds(h * EG, EG)], ring[s % NS, 2].reshape(EG, 2 * T, T)).reshape(EB, 2 * CAP, T)
            for q in range(2):
                first = h * EB + q * EG
                out = bdot(hid[pl.ds(first, EG)], ring[s % NS, q].reshape(EG, 2 * T, T))
                out = (out + third[q * EG:(q + 1) * EG]).astype(BF16)
                for g in range(2):
                    for copy in range(2):
                        osc[g, copy, pl.ds(first, EG)] = out[:, g * CAP:(g + 1) * CAP]
            w_start(s + NS)
        MARK(f'cmb{c}')
        for g in range(2):
            y = dot(comb[g], osc[g].reshape(2 * GROUP, T)) + dot(comb3[g], osc[g, 0].reshape(GROUP, T))
            y = y.reshape(2, 2, ROWS, T)
            for core in range(2):
                for x in range(2):
                    if c % 2 == 0:
                        ypart[c, core, x, g] = y[core, x]
                    else:
                        ypart[c, core, g, x] = y[core, x]
        MARK(f'r0_{c}')
        reduce0(c).start()
        if c >= 1:
            stage1(c - 1)
        if c >= LAG2:
            stage2(c - LAG2)
    stage1(NCH - 1)

    stage2(NCH - LAG2)
    MARK('shw')
    w_wait(SH_IN)
    MARK('sh')
    for n in range(NF):
        acc = jnp.zeros((ROWS, T), F32)
        weights = ring[SH_IN % NS, n].reshape(NCH, T, T)
        for k in range(NCH):
            acc = acc + dot(own(k)[...], weights[k])
        hs[:, pl.ds(n * T, T)] = jax.nn.gelu(acc).astype(BF16)
    stage2(NCH - LAG2 + 1)
    MARK('show')
    w_wait(SH_OUT)
    MARK('so')
    for c in range(NCH):
        acc = jnp.zeros((ROWS, T), F32)
        for j in range(NF):
            acc = acc + dot(hs[:, pl.ds(j * T, T)], ring[SH_OUT % NS, j, c // 2, c % 2])
        shy[:, pl.ds(c * T, T)] = acc.astype(BF16)
    stage2(NCH - 2)
    stage2(NCH - 1)
    for c in range(NCH):
        final(c)
    MARK('drain')
    for i in items:
        gather1(i).wait_send()
        gather2(i).wait_send()
        gatherd(i).wait_send()
    for c in range(NCH):
        reduce0(c).wait_send()
        reduce1(c, 0).wait_send()
        reduce1(c, 1).wait_send()
        reduce2(c).wait_send()
        write(c).wait()
    MARK(None)


def solution(mesh):
    def layer(tok_x, route_ids, route_gate, w_in, w_out, shared_in, shared_out):
        local = w_in.shape[0]
        any_space = pl.BlockSpec(memory_space=pl.ANY)
        dma = pltpu.SemaphoreType.DMA
        vmem = pltpu.VMEM
        return pl.pallas_call(
            kernel,
            out_shape=jax.ShapeDtypeStruct((ROWS, WIDTH), BF16),
            in_specs=[any_space] * 8,
            out_specs=any_space,
            scratch_shapes=[
                vmem((NCH, 2, 2, 2, ROWS, T), BF16),
                vmem((2, 2, 2, TOPK, ROWS), jnp.int32),
                vmem((2, 2, 2, TOPK, ROWS), F32),
                vmem((NS, NF, EG, 2, T, T), BF16),
                vmem((LOCAL, 2 * CAP, KS), BF16),
                vmem((LOCAL, 2 * CAP, FF), F32),
                vmem((LOCAL, 2 * CAP, 2 * T), BF16),
                vmem((LOCAL // 2, 4 * CAP, 2 * T), BF16),
                vmem((2, 2, LOCAL, CAP, T), BF16),
                vmem((2, LOCAL * CAP, GROUP), BF16),
                vmem((2, GROUP, 2 * GROUP), BF16),
                vmem((2, GROUP, GROUP), BF16),
                vmem((NCH, 2, 2, 2, ROWS, T), F32),
                vmem((NCH, 2, 2, ROWS, T), F32),
                vmem((NCH, 2, ROWS, T), F32),
                vmem((NCH, ROWS, T), F32),
                vmem((ROWS, FF), BF16),
                vmem((ROWS, WIDTH), BF16),
                vmem((NCH, ROWS, T), BF16),
                dma((NCH + 2,)),
                dma((NCH + 2,)), dma((NCH + 2,)),
                dma((NCH + 2,)), dma((NCH + 2,)),
                dma((NCH + 2,)), dma((NCH + 2,)),
                dma((NS, NF)), dma((NCH,)),
                dma((NCH,)), dma((NCH,)), dma((NCH, 2)), dma((NCH, 2)), dma((NCH,)), dma((NCH,)),
                dma((NCH,)),
            ],
            compiler_params=pltpu.CompilerParams(
                collective_id=0, has_side_effects=True, vmem_limit_bytes=67_000_000),
            name='moe_layer',
        )(tok_x, route_ids.T, route_gate.T,
          w_in.reshape(local, WIDTH // T, T, FF), w_out.reshape(local, NF, T, WIDTH),
          w_out.reshape(local // 2, 2, NF, T, WIDTH),
          shared_in.reshape(EG, 2, T, FF), shared_out.reshape(NF, T, WIDTH))

    row_spec = P(('dp', 'ep'), None)
    expert_spec = P('ep', None, None)
    whole_spec = P(None, None)
    return jax.shard_map(layer, mesh=mesh,
                         in_specs=(row_spec, row_spec, row_spec, expert_spec, expert_spec, whole_spec, whole_spec),
                         out_specs=row_spec, check_vma=False)
```

```python
import jax
import jax.numpy as jnp
from jax import lax
from jax.experimental import pallas as pl
from jax.experimental.pallas import tpu as pltpu
from jax.sharding import PartitionSpec as P

F32 = jnp.float32
BF16 = jnp.bfloat16
MESH = pl.DeviceIdType.MESH

ROWS = 64
WIDTH = 2048
FF = 768
TOPK = 8
LOCAL = 16
CAP = 16
H = 128
T = 256
NCH = WIDTH // T
EG = 4
KS = 2 * T
NK = WIDTH // KS
NEG = LOCAL // EG
EB = 8
NHB = LOCAL // EB
NF = FF // T
GROUP = 256
NS = 15
A_STEPS = NK * NEG
B_STEPS = NCH * NHB
SH_IN = A_STEPS + B_STEPS
SH_OUT = SH_IN + 1
STEPS = SH_OUT + 1
LAG2 = 3


def dot(a, b):
    return jnp.dot(a, b, preferred_element_type=F32)


class Mark:
    def __init__(self):
        self.cm = None

    def __call__(self, name):
        if self.cm is not None:
            self.cm.__exit__(None, None, None)
            self.cm = None
        if name:
            self.cm = jax.named_scope(name)
            self.cm.__enter__()


MARK = Mark()


def tdot(a, b):
    return lax.dot_general(a, b, (((0,), (0,)), ((), ())), preferred_element_type=F32)


def bdot(a, b):
    return lax.dot_general(a, b, (((2,), (1,)), ((0,), (0,))), preferred_element_type=F32)


def kernel(x_ref, ids_ref, gates_ref, win_ref, wout_ref, wpair_ref, sin_ref, sout_ref, o_ref,
           tok, mids, mgates, ring, xs, hacc, hid, hid3, osc, disp, comb, comb3, ypart, r0, r1, r2, hs, shy, ost,
           ld_sem, rts, rtr, g1s, g1r, g2s, g2r, gds, gdr, w_sem, so_sem,
           t0s, t0r, t1s, t1r, t2s, t2r, o_sem):
    my_dp = lax.axis_index('dp')
    my_ep = lax.axis_index('ep')
    my_x = my_ep // 2
    my_c = my_ep % 2
    partner = (my_dp, my_x * 2 + (1 - my_c))
    x_nbr = (my_dp, (1 - my_x) * 2 + my_c)
    y_nbr = (1 - my_dp, my_ep)
    e_off = my_dp * LOCAL

    def w_copies(s):
        slot = s % NS
        if s == SH_OUT:
            return [pltpu.make_async_copy(
                sout_ref.at[:, :, pl.ds(c * T, T)], ring.at[slot, :, c // 2, c % 2], so_sem.at[c]) for c in range(NCH)]
        copies = []
        for n in range(NF):
            if s < A_STEPS:
                k, eg = divmod(s, NEG)
                src = win_ref.at[pl.ds(e_off + eg * EG, EG), pl.ds(2 * k, 2), :, pl.ds(n * T, T)]
            elif s < SH_IN:
                c, h = divmod(s - A_STEPS, NHB)
                if n < 2:
                    src = wout_ref.at[pl.ds(e_off + h * EB + n * EG, EG), pl.ds(0, 2), :, pl.ds(c * T, T)]
                else:
                    src = wpair_ref.at[pl.ds(e_off // 2 + h * EG, EG), :, 2, :, pl.ds(c * T, T)]
            else:
                src = sin_ref.at[:, :, :, pl.ds(n * T, T)]
            copies.append(pltpu.make_async_copy(src, ring.at[slot, n], w_sem.at[slot, n]))
        return copies

    def w_start(s):
        if s < STEPS:
            for copy in w_copies(s):
                copy.start()

    def w_wait(s):
        for copy in w_copies(s):
            copy.wait()

    IDS, GATES = NCH, NCH + 1

    def over_y(i):
        return i < NCH and i % 2 == 1

    def buffer(i):
        return mids if i == IDS else mgates if i == GATES else tok.at[i]

    def own_core(i):
        return buffer(i).at[my_c]

    def own_pair(i):
        return buffer(i).at[my_c, my_x if over_y(i) else my_dp]

    def own(i):
        return buffer(i).at[my_c, my_x, my_dp] if over_y(i) else buffer(i).at[my_c, my_dp, my_x]

    def load(i):
        src = ids_ref if i == IDS else gates_ref if i == GATES else x_ref.at[:, pl.ds(i * T, T)]
        return pltpu.make_async_copy(src, own(i), ld_sem.at[i])

    def remote(src, dst, ssem, rsem, dev):
        return pltpu.make_async_remote_copy(
            src_ref=src, dst_ref=dst, send_sem=ssem, recv_sem=rsem, device_id=dev, device_id_type=MESH)

    def gather1(i):
        return remote(own(i), own(i), g1s.at[i], g1r.at[i], y_nbr if over_y(i) else x_nbr)

    def gather2(i):
        return remote(own_pair(i), own_pair(i), g2s.at[i], g2r.at[i], x_nbr if over_y(i) else y_nbr)

    def gatherd(i):
        return remote(own_core(i), own_core(i), gds.at[i], gdr.at[i], partner)

    routing = [IDS, GATES]
    items = routing + list(range(NCH))

    def peer(r):
        dp = 1 - my_dp if r & 1 else my_dp
        x = 1 - my_x if r & 2 else my_x
        c = 1 - my_c if r & 4 else my_c
        return dp, x * 2 + c

    def tell(i, r):
        return remote(own(i), own(i), rts.at[i - NCH, r], rtr.at[i - NCH, r], peer(r))

    MARK('sig')
    barrier = pltpu.get_barrier_semaphore()
    for r in range(1, 8):
        pl.semaphore_signal(barrier, inc=1, device_id=peer(r), device_id_type=MESH)
    for i in items:
        load(i).start()
    hid3[...] = jnp.zeros_like(hid3)
    MARK('ld')
    for i in items:
        load(i).wait()
    MARK('ws')
    for s in range(NS):
        w_start(s)
    MARK('barrier')
    pl.semaphore_wait(barrier, 7)

    def send_on(i):
        gather1(i).wait_recv()
        gather2(i).start()

    def share(i):
        gather2(i).wait_recv()
        gatherd(i).start()

    MARK('g1')
    for i in routing:
        for r in (3, 7, 1, 2, 5, 6, 4):
            tell(i, r).start()
    for i in range(4):
        gather1(i).start()
    MARK('g2a')
    for i in range(2):
        send_on(i)
    for i in range(4, NCH):
        gather1(i).start()
    MARK('rtw')
    for i in routing:
        for r in range(1, 8):
            tell(i, r).wait_recv()

    MARK('route')
    e_id = lax.broadcasted_iota(jnp.int32, (LOCAL, GROUP), 0) + (my_ep * (2 * LOCAL) + e_off)
    s_id = lax.broadcasted_iota(jnp.int32, (LOCAL, CAP, GROUP), 1).astype(F32)

    def true_pos(t):
        return ((t // 64) % 2) * 128 + (t // 128) * 64 + t % 64

    t_row = lax.broadcasted_iota(jnp.int32, (GROUP, GROUP), 0)
    t_col = lax.broadcasted_iota(jnp.int32, (GROUP, GROUP), 1)
    before = jnp.where(true_pos(t_row) < true_pos(t_col), 1.0, 0.0).astype(BF16)
    eye = jnp.where(t_row == t_col, 1.0, 0.0).astype(BF16)
    for g in range(2):
        ids = jnp.concatenate([mids[c, g, x] for c in range(2) for x in range(2)], axis=1)
        gates = jnp.concatenate([mgates[c, g, x] for c in range(2) for x in range(2)], axis=1)
        chosen = jnp.zeros((LOCAL, GROUP), F32)
        gate = jnp.zeros((LOCAL, GROUP), F32)
        for j in range(TOPK):
            hit = ids[j:j + 1, :] == e_id
            chosen = jnp.where(hit, 1.0, chosen)
            gate = jnp.where(hit, gates[j:j + 1, :], gate)
        slot = dot(chosen.astype(BF16), before)
        slot = jnp.where(chosen > 0.0, slot, -1.0)
        here = slot[:, None, :] == s_id
        disp[g] = jnp.where(here, 1.0, 0.0).reshape(LOCAL * CAP, GROUP).astype(BF16)
        weight = jnp.where(here, gate[:, None, :], 0.0).reshape(LOCAL * CAP, GROUP)
        for piece in range(3):
            part = weight.astype(BF16)
            turned = tdot(part, eye).astype(BF16)
            if piece < 2:
                comb[g, :, pl.ds(piece * GROUP, GROUP)] = turned
            else:
                comb3[g] = turned
            weight = weight - part.astype(F32)

    MARK('g2b')
    for i in (2, 3):
        send_on(i)
    MARK('share0')
    for i in (0, 1):
        share(i)
    MARK('g2c')
    for i in (4, 5):
        send_on(i)
    for k in range(NK):
        MARK(f'gw{k}')
        for h in range(2):
            gatherd(2 * k + h).wait_recv()
        MARK(f'dsp{k}')
        for h in range(2):
            i = 2 * k + h
            for g in range(2):
                rows = tok[i, :, :, g] if over_y(i) else tok[i, :, g]
                picked = dot(disp[g], rows.reshape(GROUP, T)).astype(BF16)
                xs[:, pl.ds(g * CAP, CAP), pl.ds(h * T, T)] = picked.reshape(LOCAL, CAP, T)
        for half in range(2):
            steps = [k * NEG + half * 2 + q for q in range(2)]
            MARK(f'aw{k}{half}')
            for s in steps:
                w_wait(s)
            MARK(f'a{k}{half}')
            for s in steps:
                eg = s % NEG
                batch = pl.ds(eg * EG, EG)
                for n in range(NF):
                    cols = pl.ds(n * T, T)
                    acc = bdot(xs[batch], ring[s % NS, n].reshape(EG, KS, T))
                    if k > 0:
                        acc = acc + hacc[batch, :, cols]
                    if k < NK - 1:
                        hacc[batch, :, cols] = acc
                        continue
                    act = jax.nn.gelu(acc).astype(BF16)
                    if n < 2:
                        hid[batch, :, cols] = act
                    else:
                        act = act.reshape(EG // 2, 2, 2 * CAP, T)
                        for m in range(2):
                            hid3[pl.ds(eg * EG // 2, EG // 2), pl.ds(m * 2 * CAP, 2 * CAP), pl.ds(m * T, T)] = act[:, m]
            for s in steps:
                w_start(s + NS)
            MARK(f'fw{k}')
            if half == 0 and k < NK - 1:
                if k == 0:
                    for i in (6, 7):
                        send_on(i)
                for i in (2 * k + 2, 2 * k + 3):
                    share(i)

    def route(d):
        if d == 0:
            return my_x, my_dp, x_nbr, y_nbr
        return my_dp, my_x, y_nbr, x_nbr

    def reduce0(c):
        return remote(ypart.at[c, 1 - my_c], r0.at[c], t0s.at[c], t0r.at[c], partner)

    def reduce1(c, d, last):
        a, b, dev, _ = route(d)
        side = b if last else 1 - b
        return remote(ypart.at[c, my_c, d, 1 - a, side], r1.at[c, d, side], t1s.at[c, d, last], t1r.at[c, d, last], dev)

    def reduce2(c, d):
        a, b, _, dev = route(d)
        return remote(ypart.at[c, my_c, d, a, 1 - b], r2.at[c, d], t2s.at[c, d], t2r.at[c, d], dev)

    def stage1(c):
        MARK(f's1_{c}')
        reduce0(c).wait_recv()
        for last in range(2):
            for d in range(2):
                a, b, _, _ = route(d)
                side = b if last else 1 - b
                ypart[c, my_c, d, 1 - a, side] = ypart[c, my_c, d, 1 - a, side] + r0[c, d, 1 - a, side]
        for last in range(2):
            for d in range(2):
                reduce1(c, d, last).start()
        for d in range(2):
            a, _, _, _ = route(d)
            ypart[c, my_c, d, a] = ypart[c, my_c, d, a] + r0[c, d, a]

    def stage2(c):
        MARK(f's2_{c}')
        for d in range(2):
            a, b, _, _ = route(d)
            reduce1(c, d, 0).wait_recv()
            ypart[c, my_c, d, a, 1 - b] = ypart[c, my_c, d, a, 1 - b] + r1[c, d, 1 - b]
        for d in range(2):
            reduce2(c, d).start()

    def write(c):
        return pltpu.make_async_copy(ost.at[c], o_ref.at[:, pl.ds(c * T, T)], o_sem.at[c])

    def final(c):
        MARK(f'fin{c}')
        for d in range(2):
            a, b, _, _ = route(d)
            reduce1(c, d, 1).wait_recv()
            reduce2(c, d).wait_recv()
            moe = ypart[c, my_c, d, a, b] + r1[c, d, b] + r2[c, d]
            x_own = own(c)[:, pl.ds(d * H, H)].astype(F32)
            shared = shy[:, pl.ds(c * T + d * H, H)].astype(F32)
            ost[c, :, pl.ds(d * H, H)] = (x_own + shared + moe).astype(BF16)
        write(c).start()

    for c in range(NCH):
        for h in range(NHB):
            s = A_STEPS + c * NHB + h
            MARK(f'bw{s}')
            w_wait(s)
            MARK(f'b{s}')
            third = bdot(hid3[pl.ds(h * EG, EG)], ring[s % NS, 2].reshape(EG, 2 * T, T)).reshape(EB, 2 * CAP, T)
            for q in range(2):
                first = h * EB + q * EG
                out = bdot(hid[pl.ds(first, EG)], ring[s % NS, q].reshape(EG, 2 * T, T))
                out = (out + third[q * EG:(q + 1) * EG]).astype(BF16)
                for g in range(2):
                    for copy in range(2):
                        osc[g, copy, pl.ds(first, EG)] = out[:, g * CAP:(g + 1) * CAP]
            w_start(s + NS)
        if c >= 1:
            stage1(c - 1)
        MARK(f'cmb{c}')
        for g in range(2):
            y = dot(comb[g], osc[g].reshape(2 * GROUP, T)) + dot(comb3[g], osc[g, 0].reshape(GROUP, T))
            y = y.reshape(2, 2, ROWS, T)
            for core in range(2):
                for x in range(2):
                    ypart[c, core, 0, x, g] = y[core, x, :, :H]
                    ypart[c, core, 1, g, x] = y[core, x, :, H:]
        MARK(f'r0_{c}')
        reduce0(c).start()
        if c >= LAG2:
            stage2(c - LAG2)

    MARK('shw')
    w_wait(SH_IN)
    MARK('sh')
    for n in range(NF):
        acc = jnp.zeros((ROWS, T), F32)
        weights = ring[SH_IN % NS, n].reshape(NCH, T, T)
        for k in range(NCH):
            acc = acc + dot(own(k)[...], weights[k])
        hs[:, pl.ds(n * T, T)] = jax.nn.gelu(acc).astype(BF16)
    stage1(NCH - 1)
    stage2(NCH - 3)
    MARK('show')
    w_wait(SH_OUT)
    MARK('so')
    for c in range(NCH):
        acc = jnp.zeros((ROWS, T), F32)
        for j in range(NF):
            acc = acc + dot(hs[:, pl.ds(j * T, T)], ring[SH_OUT % NS, j, c // 2, c % 2])
        shy[:, pl.ds(c * T, T)] = acc.astype(BF16)
    stage2(NCH - 2)
    stage2(NCH - 1)
    for c in range(NCH):
        final(c)
    MARK('drain')
    for i in routing:
        for r in range(1, 8):
            tell(i, r).wait_send()
    for i in range(NCH):
        gather1(i).wait_send()
        gather2(i).wait_send()
        gatherd(i).wait_send()
    for c in range(NCH):
        reduce0(c).wait_send()
        for d in range(2):
            reduce1(c, d, 0).wait_send()
            reduce1(c, d, 1).wait_send()
            reduce2(c, d).wait_send()
        write(c).wait()
    MARK(None)


def solution(mesh):
    def layer(tok_x, route_ids, route_gate, w_in, w_out, shared_in, shared_out):
        local = w_in.shape[0]
        any_space = pl.BlockSpec(memory_space=pl.ANY)
        dma = pltpu.SemaphoreType.DMA
        vmem = pltpu.VMEM
        return pl.pallas_call(
            kernel,
            out_shape=jax.ShapeDtypeStruct((ROWS, WIDTH), BF16),
            in_specs=[any_space] * 8,
            out_specs=any_space,
            scratch_shapes=[
                vmem((NCH, 2, 2, 2, ROWS, T), BF16),
                vmem((2, 2, 2, TOPK, ROWS), jnp.int32),
                vmem((2, 2, 2, TOPK, ROWS), F32),
                vmem((NS, NF, EG, 2, T, T), BF16),
                vmem((LOCAL, 2 * CAP, KS), BF16),
                vmem((LOCAL, 2 * CAP, FF), F32),
                vmem((LOCAL, 2 * CAP, 2 * T), BF16),
                vmem((LOCAL // 2, 4 * CAP, 2 * T), BF16),
                vmem((2, 2, LOCAL, CAP, T), BF16),
                vmem((2, LOCAL * CAP, GROUP), BF16),
                vmem((2, GROUP, 2 * GROUP), BF16),
                vmem((2, GROUP, GROUP), BF16),
                vmem((NCH, 2, 2, 2, 2, ROWS, H), F32),
                vmem((NCH, 2, 2, 2, ROWS, H), F32),
                vmem((NCH, 2, 2, ROWS, H), F32),
                vmem((NCH, 2, ROWS, H), F32),
                vmem((ROWS, FF), BF16),
                vmem((ROWS, WIDTH), BF16),
                vmem((NCH, ROWS, T), BF16),
                dma((NCH + 2,)),
                dma((2, 8)), dma((2, 8)),
                dma((NCH,)), dma((NCH,)),
                dma((NCH,)), dma((NCH,)),
                dma((NCH,)), dma((NCH,)),
                dma((NS, NF)), dma((NCH,)),
                dma((NCH,)), dma((NCH,)), dma((NCH, 2, 2)), dma((NCH, 2, 2)), dma((NCH, 2)), dma((NCH, 2)),
                dma((NCH,)),
            ],
            compiler_params=pltpu.CompilerParams(
                collective_id=0, has_side_effects=True, vmem_limit_bytes=67_000_000),
            name='moe_layer',
        )(tok_x, route_ids.T, route_gate.T,
          w_in.reshape(local, WIDTH // T, T, FF), w_out.reshape(local, NF, T, WIDTH),
          w_out.reshape(local // 2, 2, NF, T, WIDTH),
          shared_in.reshape(EG, 2, T, FF), shared_out.reshape(NF, T, WIDTH))

    row_spec = P(('dp', 'ep'), None)
    expert_spec = P('ep', None, None)
    whole_spec = P(None, None)
    return jax.shard_map(layer, mesh=mesh,
                         in_specs=(row_spec, row_spec, row_spec, expert_spec, expert_spec, whole_spec, whole_spec),
                         out_specs=row_spec, check_vma=False)
```

```python
import jax
import jax.numpy as jnp
from jax import lax
from jax.experimental import pallas as pl
from jax.experimental.pallas import tpu as pltpu
from jax.sharding import PartitionSpec as P

F32 = jnp.float32
BF16 = jnp.bfloat16
MESH = pl.DeviceIdType.MESH

ROWS = 64
WIDTH = 2048
FF = 768
TOPK = 8
LOCAL = 16
CAP = 16
H = 128
T = 256
NCH = WIDTH // T
EG = 4
KS = 2 * T
NK = WIDTH // KS
NEG = LOCAL // EG
EB = 8
NHB = LOCAL // EB
NF = FF // T
GROUP = 256
NS = 15
A_STEPS = NK * NEG
B_STEPS = NCH * NHB
SH_IN = A_STEPS + B_STEPS
SH_OUT = SH_IN + 1
STEPS = SH_OUT + 1
LAG2 = 3


def dot(a, b):
    return jnp.dot(a, b, preferred_element_type=F32)


class Mark:
    def __init__(self):
        self.cm = None

    def __call__(self, name):
        if self.cm is not None:
            self.cm.__exit__(None, None, None)
            self.cm = None
        if name:
            self.cm = jax.named_scope(name)
            self.cm.__enter__()


MARK = Mark()


def tdot(a, b):
    return lax.dot_general(a, b, (((0,), (0,)), ((), ())), preferred_element_type=F32)


def bdot(a, b):
    return lax.dot_general(a, b, (((2,), (1,)), ((0,), (0,))), preferred_element_type=F32)


def kernel(x_ref, ids_ref, gates_ref, win_ref, wout_ref, wpair_ref, sin_ref, sout_ref, o_ref,
           tok, mids, mgates, ring, xs, hacc, hid, hid3, osc, disp, comb, comb3, ypart, r0, r1, r2, hs, shy, ost,
           ld_sem, rts, rtr, g1s, g1r, g2s, g2r, gds, gdr, w_sem, t0s, t0r, t1s, t1r, t2s, fin, o_sem):
    my_dp = lax.axis_index('dp')
    my_ep = lax.axis_index('ep')
    my_x = my_ep // 2
    my_c = my_ep % 2
    my_pos = my_c * 4 + my_dp * 2 + my_x
    partner = (my_dp, my_x * 2 + (1 - my_c))
    x_nbr = (my_dp, (1 - my_x) * 2 + my_c)
    y_nbr = (1 - my_dp, my_ep)
    e_off = my_dp * LOCAL

    def wait_all(ref, sem):
        pltpu.make_async_copy(ref, ref, sem).wait()

    def w_copies(s):
        slot = s % NS
        if s == SH_OUT:
            return [pltpu.make_async_copy(
                sout_ref.at[:, :, pl.ds(c * T, T)], ring.at[slot, :, c // 2, c % 2], w_sem.at[slot]) for c in range(NCH)]
        copies = []
        for n in range(NF):
            if s < A_STEPS:
                k, eg = divmod(s, NEG)
                src = win_ref.at[pl.ds(e_off + eg * EG, EG), pl.ds(2 * k, 2), :, pl.ds(n * T, T)]
            elif s < SH_IN:
                c, h = divmod(s - A_STEPS, NHB)
                if n < 2:
                    src = wout_ref.at[pl.ds(e_off + h * EB + n * EG, EG), pl.ds(0, 2), :, pl.ds(c * T, T)]
                else:
                    src = wpair_ref.at[pl.ds(e_off // 2 + h * EG, EG), :, 2, :, pl.ds(c * T, T)]
            else:
                src = sin_ref.at[:, :, :, pl.ds(n * T, T)]
            copies.append(pltpu.make_async_copy(src, ring.at[slot, n], w_sem.at[slot]))
        return copies

    def w_start(s):
        if s < STEPS:
            for copy in w_copies(s):
                copy.start()

    def w_wait(s):
        wait_all(ring.at[s % NS], w_sem.at[s % NS])

    IDS, GATES = NCH, NCH + 1

    def over_y(i):
        return i % 2 == 1

    def own_core(i):
        return tok.at[i, my_c]

    def own_pair(i):
        return tok.at[i, my_c, my_x if over_y(i) else my_dp]

    def own(i):
        if i == IDS:
            return mids.at[my_pos]
        if i == GATES:
            return mgates.at[my_pos]
        return tok.at[i, my_c, my_x, my_dp] if over_y(i) else tok.at[i, my_c, my_dp, my_x]

    def load(i):
        src = ids_ref if i == IDS else gates_ref if i == GATES else x_ref.at[:, pl.ds(i * T, T)]
        return pltpu.make_async_copy(src, own(i), ld_sem.at[max(0, i - NCH + 1)])

    def remote(src, dst, ssem, rsem, dev):
        return pltpu.make_async_remote_copy(
            src_ref=src, dst_ref=dst, send_sem=ssem, recv_sem=rsem, device_id=dev, device_id_type=MESH)

    def gather1(i):
        return remote(own(i), own(i), g1s, g1r.at[i // 2], y_nbr if over_y(i) else x_nbr)

    def gather2(i):
        return remote(own_pair(i), own_pair(i), g2s, g2r.at[i // 2], x_nbr if over_y(i) else y_nbr)

    def gatherd(i):
        return remote(own_core(i), own_core(i), gds, gdr.at[i // 2], partner)

    routing = [IDS, GATES]
    items = routing + list(range(NCH))

    def peer(r):
        dp = 1 - my_dp if r & 1 else my_dp
        x = 1 - my_x if r & 2 else my_x
        c = 1 - my_c if r & 4 else my_c
        return dp, x * 2 + c

    def tell(i, r):
        return remote(own(i), own(i), rts.at[i - NCH], rtr.at[i - NCH], peer(r))

    MARK('sig')
    barrier = pltpu.get_barrier_semaphore()
    for r in range(1, 8):
        pl.semaphore_signal(barrier, inc=1, device_id=peer(r), device_id_type=MESH)
    for i in items:
        load(i).start()
    hid3[...] = jnp.zeros_like(hid3)
    MARK('ld')
    wait_all(ost, ld_sem.at[0])
    for i in routing:
        load(i).wait()
    MARK('ws')
    for s in range(NS):
        w_start(s)
    MARK('barrier')
    pl.semaphore_wait(barrier, 7)

    def send(p):
        for i in (2 * p, 2 * p + 1):
            gather1(i).start()

    def send_on(p):
        wait_all(tok.at[2 * p, 0, 0], g1r.at[p])
        for i in (2 * p, 2 * p + 1):
            gather2(i).start()

    def share(p):
        wait_all(tok.at[2 * p, 0], g2r.at[p])
        for i in (2 * p, 2 * p + 1):
            gatherd(i).start()

    MARK('g1')
    send(0)
    for i in routing:
        for r in (3, 7, 1, 2, 5, 6, 4):
            tell(i, r).start()
    MARK('g2a')
    send_on(0)
    send(1)
    MARK('rtw')
    wait_all(mids.at[pl.ds(0, 7)], rtr.at[0])
    wait_all(mgates.at[pl.ds(0, 7)], rtr.at[1])

    MARK('route')
    e_id = lax.broadcasted_iota(jnp.int32, (LOCAL, GROUP), 0) + (my_ep * (2 * LOCAL) + e_off)
    s_id = lax.broadcasted_iota(jnp.int32, (LOCAL, CAP, GROUP), 1).astype(F32)

    def true_pos(t):
        return ((t // 64) % 2) * 128 + (t // 128) * 64 + t % 64

    t_row = lax.broadcasted_iota(jnp.int32, (GROUP, GROUP), 0)
    t_col = lax.broadcasted_iota(jnp.int32, (GROUP, GROUP), 1)
    before = jnp.where(true_pos(t_row) < true_pos(t_col), 1.0, 0.0).astype(BF16)
    eye = jnp.where(t_row == t_col, 1.0, 0.0).astype(BF16)
    for g in range(2):
        ids = jnp.concatenate([mids[c * 4 + g * 2 + x] for c in range(2) for x in range(2)], axis=1)
        gates = jnp.concatenate([mgates[c * 4 + g * 2 + x] for c in range(2) for x in range(2)], axis=1)
        chosen = jnp.zeros((LOCAL, GROUP), F32)
        gate = jnp.zeros((LOCAL, GROUP), F32)
        for j in range(TOPK):
            hit = ids[j:j + 1, :] == e_id
            chosen = jnp.where(hit, 1.0, chosen)
            gate = jnp.where(hit, gates[j:j + 1, :], gate)
        slot = dot(chosen.astype(BF16), before)
        slot = jnp.where(chosen > 0.0, slot, -1.0)
        here = slot[:, None, :] == s_id
        disp[g] = jnp.where(here, 1.0, 0.0).reshape(LOCAL * CAP, GROUP).astype(BF16)
        weight = jnp.where(here, gate[:, None, :], 0.0).reshape(LOCAL * CAP, GROUP)
        for piece in range(3):
            part = weight.astype(BF16)
            turned = tdot(part, eye).astype(BF16)
            if piece < 2:
                comb[g, :, pl.ds(piece * GROUP, GROUP)] = turned
            else:
                comb3[g] = turned
            weight = weight - part.astype(F32)

    MARK('g2b')
    send_on(1)
    send(2)
    send(3)
    MARK('share0')
    share(0)
    for k in range(NK):
        MARK(f'gw{k}')
        wait_all(tok.at[2 * k], gdr.at[k])
        MARK(f'dsp{k}')
        for h in range(2):
            i = 2 * k + h
            for g in range(2):
                rows = tok[i, :, :, g] if over_y(i) else tok[i, :, g]
                picked = dot(disp[g], rows.reshape(GROUP, T)).astype(BF16)
                xs[:, pl.ds(g * CAP, CAP), pl.ds(h * T, T)] = picked.reshape(LOCAL, CAP, T)
        for half in range(2):
            steps = [k * NEG + half * 2 + q for q in range(2)]
            MARK(f'aw{k}{half}')
            for s in steps:
                w_wait(s)
            MARK(f'a{k}{half}')
            for s in steps:
                eg = s % NEG
                batch = pl.ds(eg * EG, EG)
                for n in range(NF):
                    cols = pl.ds(n * T, T)
                    acc = bdot(xs[batch], ring[s % NS, n].reshape(EG, KS, T))
                    if k > 0:
                        acc = acc + hacc[batch, :, cols]
                    if k < NK - 1:
                        hacc[batch, :, cols] = acc
                        continue
                    act = jax.nn.gelu(acc).astype(BF16)
                    if n < 2:
                        hid[batch, :, cols] = act
                    else:
                        act = act.reshape(EG // 2, 2, 2 * CAP, T)
                        for m in range(2):
                            hid3[pl.ds(eg * EG // 2, EG // 2), pl.ds(m * 2 * CAP, 2 * CAP), pl.ds(m * T, T)] = act[:, m]
            for s in steps:
                w_start(s + NS)
            MARK(f'fw{k}')
            if half == 0 and k < NK - 1:
                if k == 0:
                    send_on(2)
                    send_on(3)
                share(k + 1)

    def route(d):
        if d == 0:
            return my_x, my_dp, x_nbr, y_nbr
        return my_dp, my_x, y_nbr, x_nbr

    def reduce0(c):
        return remote(ypart.at[c, 1 - my_c], r0.at[c], t0s, t0r.at[c], partner)

    def reduce1(c, d, last):
        a, b, dev, _ = route(d)
        side = b if last else 1 - b
        return remote(ypart.at[c, my_c, d, 1 - a, side], r1.at[c, d, side], t1s, fin.at[c] if last else t1r.at[c], dev)

    def reduce2(c, d):
        a, b, _, dev = route(d)
        return remote(ypart.at[c, my_c, d, a, 1 - b], r2.at[c, d], t2s, fin.at[c], dev)

    def stage1(c):
        MARK(f's1_{c}')
        reduce0(c).wait_recv()
        for last in range(2):
            for d in range(2):
                a, b, _, _ = route(d)
                side = b if last else 1 - b
                ypart[c, my_c, d, 1 - a, side] = ypart[c, my_c, d, 1 - a, side] + r0[c, d, 1 - a, side]
        for last in range(2):
            for d in range(2):
                reduce1(c, d, last).start()
        for d in range(2):
            a, _, _, _ = route(d)
            ypart[c, my_c, d, a] = ypart[c, my_c, d, a] + r0[c, d, a]

    def stage2(c):
        MARK(f's2_{c}')
        wait_all(r1.at[c, 0], t1r.at[c])
        for d in range(2):
            a, b, _, _ = route(d)
            ypart[c, my_c, d, a, 1 - b] = ypart[c, my_c, d, a, 1 - b] + r1[c, d, 1 - b]
        for d in range(2):
            reduce2(c, d).start()

    def write(c):
        return pltpu.make_async_copy(ost.at[c], o_ref.at[:, pl.ds(c * T, T)], o_sem)

    def final(c):
        MARK(f'fin{c}')
        wait_all(r0.at[c, 0], fin.at[c])
        for d in range(2):
            a, b, _, _ = route(d)
            moe = ypart[c, my_c, d, a, b] + r1[c, d, b] + r2[c, d]
            x_own = own(c)[:, pl.ds(d * H, H)].astype(F32)
            shared = shy[:, pl.ds(c * T + d * H, H)].astype(F32)
            ost[c, :, pl.ds(d * H, H)] = (x_own + shared + moe).astype(BF16)
        write(c).start()

    for c in range(NCH):
        for h in range(NHB):
            s = A_STEPS + c * NHB + h
            MARK(f'bw{s}')
            w_wait(s)
            MARK(f'b{s}')
            third = bdot(hid3[pl.ds(h * EG, EG)], ring[s % NS, 2].reshape(EG, 2 * T, T)).reshape(EB, 2 * CAP, T)
            for q in range(2):
                first = h * EB + q * EG
                out = bdot(hid[pl.ds(first, EG)], ring[s % NS, q].reshape(EG, 2 * T, T))
                out = (out + third[q * EG:(q + 1) * EG]).astype(BF16)
                for g in range(2):
                    for copy in range(2):
                        osc[g, copy, pl.ds(first, EG)] = out[:, g * CAP:(g + 1) * CAP]
            w_start(s + NS)
        if c >= 1:
            stage1(c - 1)
        MARK(f'cmb{c}')
        for g in range(2):
            y = dot(comb[g], osc[g].reshape(2 * GROUP, T)) + dot(comb3[g], osc[g, 0].reshape(GROUP, T))
            y = y.reshape(2, 2, ROWS, T)
            for core in range(2):
                for x in range(2):
                    ypart[c, core, 0, x, g] = y[core, x, :, :H]
                    ypart[c, core, 1, g, x] = y[core, x, :, H:]
        MARK(f'r0_{c}')
        reduce0(c).start()
        if c >= LAG2:
            stage2(c - LAG2)

    MARK('shw')
    w_wait(SH_IN)
    MARK('sh')
    for n in range(NF):
        acc = jnp.zeros((ROWS, T), F32)
        weights = ring[SH_IN % NS, n].reshape(NCH, T, T)
        for k in range(NCH):
            acc = acc + dot(own(k)[...], weights[k])
        hs[:, pl.ds(n * T, T)] = jax.nn.gelu(acc).astype(BF16)
    stage1(NCH - 1)
    stage2(NCH - 3)
    MARK('show')
    w_wait(SH_OUT)
    MARK('so')
    for c in range(NCH):
        acc = jnp.zeros((ROWS, T), F32)
        for j in range(NF):
            acc = acc + dot(hs[:, pl.ds(j * T, T)], ring[SH_OUT % NS, j, c // 2, c % 2])
        shy[:, pl.ds(c * T, T)] = acc.astype(BF16)
    stage2(NCH - 2)
    stage2(NCH - 1)
    for c in range(NCH):
        final(c)
    MARK('drain')
    wait_all(mids.at[pl.ds(0, 7)], rts.at[0])
    wait_all(mgates.at[pl.ds(0, 7)], rts.at[1])
    wait_all(ost, g1s)
    wait_all(tok.at[pl.ds(0, 2)], g2s)
    wait_all(tok.at[pl.ds(0, 4)], gds)
    wait_all(r0, t0s)
    wait_all(r1, t1s)
    wait_all(r2, t2s)
    wait_all(ost, o_sem)
    MARK(None)


def solution(mesh):
    def layer(tok_x, route_ids, route_gate, w_in, w_out, shared_in, shared_out):
        local = w_in.shape[0]
        any_space = pl.BlockSpec(memory_space=pl.ANY)
        dma = pltpu.SemaphoreType.DMA
        vmem = pltpu.VMEM
        return pl.pallas_call(
            kernel,
            out_shape=jax.ShapeDtypeStruct((ROWS, WIDTH), BF16),
            in_specs=[any_space] * 8,
            out_specs=any_space,
            scratch_shapes=[
                vmem((NCH, 2, 2, 2, ROWS, T), BF16),
                vmem((8, TOPK, ROWS), jnp.int32),
                vmem((8, TOPK, ROWS), F32),
                vmem((NS, NF, EG, 2, T, T), BF16),
                vmem((LOCAL, 2 * CAP, KS), BF16),
                vmem((LOCAL, 2 * CAP, FF), F32),
                vmem((LOCAL, 2 * CAP, 2 * T), BF16),
                vmem((LOCAL // 2, 4 * CAP, 2 * T), BF16),
                vmem((2, 2, LOCAL, CAP, T), BF16),
                vmem((2, LOCAL * CAP, GROUP), BF16),
                vmem((2, GROUP, 2 * GROUP), BF16),
                vmem((2, GROUP, GROUP), BF16),
                vmem((NCH, 2, 2, 2, 2, ROWS, H), F32),
                vmem((NCH, 2, 2, 2, ROWS, H), F32),
                vmem((NCH, 2, 2, ROWS, H), F32),
                vmem((NCH, 2, ROWS, H), F32),
                vmem((ROWS, FF), BF16),
                vmem((ROWS, WIDTH), BF16),
                vmem((NCH, ROWS, T), BF16),
                dma((3,)), dma((2,)), dma((2,)),
                dma, dma((NK,)), dma, dma((NK,)), dma, dma((NK,)),
                dma((NS,)),
                dma, dma((NCH,)), dma, dma((NCH,)), dma, dma((NCH,)), dma,
            ],
            compiler_params=pltpu.CompilerParams(
                collective_id=0, has_side_effects=True, vmem_limit_bytes=67_000_000),
            name='moe_layer',
        )(tok_x, route_ids.T, route_gate.T,
          w_in.reshape(local, WIDTH // T, T, FF), w_out.reshape(local, NF, T, WIDTH),
          w_out.reshape(local // 2, 2, NF, T, WIDTH),
          shared_in.reshape(EG, 2, T, FF), shared_out.reshape(NF, T, WIDTH))

    row_spec = P(('dp', 'ep'), None)
    expert_spec = P('ep', None, None)
    whole_spec = P(None, None)
    return jax.shard_map(layer, mesh=mesh,
                         in_specs=(row_spec, row_spec, row_spec, expert_spec, expert_spec, whole_spec, whole_spec),
                         out_specs=row_spec, check_vma=False)
```

```python
import jax
import jax.numpy as jnp
from jax import lax
from jax.experimental import pallas as pl
from jax.experimental.pallas import tpu as pltpu
from jax.sharding import PartitionSpec as P

F32 = jnp.float32
BF16 = jnp.bfloat16
MESH = pl.DeviceIdType.MESH

ROWS = 64
WIDTH = 2048
FF = 768
TOPK = 8
LOCAL = 16
CAP = 16
H = 128
T = 256
NCH = WIDTH // T
EG = 4
KS = 2 * T
NK = WIDTH // KS
NEG = LOCAL // EG
EB = 8
NHB = LOCAL // EB
NF = FF // T
GROUP = 256
NS = 13
A_STEPS = NK * NEG
B_STEPS = NCH * NHB
SH_IN = A_STEPS + B_STEPS
SH_OUT = SH_IN + 1
STEPS = SH_OUT + 1
DEFER = 2
LAG2 = 3


def dot(a, b):
    return jnp.dot(a, b, preferred_element_type=F32)


class Mark:
    def __init__(self):
        self.cm = None

    def __call__(self, name):
        if self.cm is not None:
            self.cm.__exit__(None, None, None)
            self.cm = None
        if name:
            self.cm = jax.named_scope(name)
            self.cm.__enter__()


MARK = Mark()


def tdot(a, b):
    return lax.dot_general(a, b, (((0,), (0,)), ((), ())), preferred_element_type=F32)


def bdot(a, b):
    return lax.dot_general(a, b, (((2,), (1,)), ((0,), (0,))), preferred_element_type=F32)


def kernel(x_ref, ids_ref, gates_ref, win_ref, wout_ref, wpair_ref, sin_ref, sout_ref, o_ref,
           tok, mids, mgates, ring, xs, hacc, hid, hid3, osc, disp, comb, comb3, ypart, r0, r1, r2, hs, shy,
           ld_sem, rts, rtr, g1s, g1r, g2s, g2r, gds, gdr, w_sem, t0s, t0r, t1s, t1r, t2s, fin):
    my_dp = lax.axis_index('dp')
    my_ep = lax.axis_index('ep')
    my_x = my_ep // 2
    my_c = my_ep % 2
    my_pos = my_c * 4 + my_dp * 2 + my_x
    partner = (my_dp, my_x * 2 + (1 - my_c))
    x_nbr = (my_dp, (1 - my_x) * 2 + my_c)
    y_nbr = (1 - my_dp, my_ep)
    e_off = my_dp * LOCAL

    def wait_all(ref, sem):
        pltpu.make_async_copy(ref, ref, sem).wait()

    def w_copies(s):
        slot = s % NS
        if s == SH_OUT:
            return [pltpu.make_async_copy(
                sout_ref.at[:, :, pl.ds(c * T, T)], ring.at[slot, :, c // 2, c % 2], w_sem.at[slot]) for c in range(NCH)]
        copies = []
        for n in range(NF):
            if s < A_STEPS:
                k, eg = divmod(s, NEG)
                src = win_ref.at[pl.ds(e_off + eg * EG, EG), pl.ds(2 * k, 2), :, pl.ds(n * T, T)]
            elif s < SH_IN:
                c, h = divmod(s - A_STEPS, NHB)
                if n < 2:
                    src = wout_ref.at[pl.ds(e_off + h * EB + n * EG, EG), pl.ds(0, 2), :, pl.ds(c * T, T)]
                else:
                    src = wpair_ref.at[pl.ds(e_off // 2 + h * EG, EG), :, 2, :, pl.ds(c * T, T)]
            else:
                src = sin_ref.at[:, :, :, pl.ds(n * T, T)]
            copies.append(pltpu.make_async_copy(src, ring.at[slot, n], w_sem.at[slot]))
        return copies

    def w_start(s):
        if s < STEPS:
            for copy in w_copies(s):
                copy.start()

    def w_wait(s):
        wait_all(ring.at[s % NS], w_sem.at[s % NS])

    IDS, GATES = NCH, NCH + 1

    def over_y(i):
        return i % 2 == 1

    def own_core(i):
        return tok.at[i, my_c]

    def own_pair(i):
        return tok.at[i, my_c, my_x if over_y(i) else my_dp]

    def own(i):
        if i == IDS:
            return mids.at[my_pos]
        if i == GATES:
            return mgates.at[my_pos]
        return tok.at[i, my_c, my_x, my_dp] if over_y(i) else tok.at[i, my_c, my_dp, my_x]

    def load(i):
        src = ids_ref if i == IDS else gates_ref if i == GATES else x_ref.at[:, pl.ds(i * T, T)]
        return pltpu.make_async_copy(src, own(i), ld_sem.at[max(0, i - NCH + 1)])

    def remote(src, dst, ssem, rsem, dev):
        return pltpu.make_async_remote_copy(
            src_ref=src, dst_ref=dst, send_sem=ssem, recv_sem=rsem, device_id=dev, device_id_type=MESH)

    def gather1(i):
        return remote(own(i), own(i), g1s, g1r.at[i // 2], y_nbr if over_y(i) else x_nbr)

    def gather2(i):
        return remote(own_pair(i), own_pair(i), g2s, g2r.at[i // 2], x_nbr if over_y(i) else y_nbr)

    def gatherd(i):
        return remote(own_core(i), own_core(i), gds, gdr.at[i // 2], partner)

    routing = [IDS, GATES]
    items = routing + list(range(NCH))

    def peer(r):
        dp = 1 - my_dp if r & 1 else my_dp
        x = 1 - my_x if r & 2 else my_x
        c = 1 - my_c if r & 4 else my_c
        return dp, x * 2 + c

    def tell(i, r):
        return remote(own(i), own(i), rts.at[i - NCH], rtr.at[i - NCH], peer(r))

    MARK('sig')
    barrier = pltpu.get_barrier_semaphore()
    for r in range(1, 8):
        pl.semaphore_signal(barrier, inc=1, device_id=peer(r), device_id_type=MESH)
    for i in items:
        load(i).start()
    hid3[...] = jnp.zeros_like(hid3)
    MARK('ld')
    wait_all(tok.at[0], ld_sem.at[0])
    for i in routing:
        load(i).wait()
    MARK('ws')
    for s in range(NS):
        w_start(s)
    MARK('barrier')
    pl.semaphore_wait(barrier, 7)

    def direct(i, r):
        return remote(own(i), own(i), g1s, g2r.at[0], peer(r))

    def send(p):
        for i in (2 * p, 2 * p + 1):
            gather1(i).start()

    def send_on(p):
        wait_all(tok.at[2 * p, 0, 0], g1r.at[p])
        for i in (2 * p, 2 * p + 1):
            gather2(i).start()

    def share(p):
        wait_all(tok.at[pl.ds(0, 3), 0, 0] if p == 0 else tok.at[2 * p, 0], g2r.at[p])
        for i in (2 * p, 2 * p + 1):
            gatherd(i).start()

    MARK('g1')
    for r in (3, 2, 1):
        for i in (0, 1):
            direct(i, r).start()
    for i in routing:
        for r in (3, 7, 1, 2, 5, 6, 4):
            tell(i, r).start()
    send(1)
    MARK('rtw')
    wait_all(mids.at[pl.ds(0, 7)], rtr.at[0])
    wait_all(mgates.at[pl.ds(0, 7)], rtr.at[1])
    send(2)
    send(3)

    MARK('route')
    e_id = lax.broadcasted_iota(jnp.int32, (LOCAL, GROUP), 0) + (my_ep * (2 * LOCAL) + e_off)
    s_id = lax.broadcasted_iota(jnp.int32, (LOCAL, CAP, GROUP), 1).astype(F32)

    def true_pos(t):
        return ((t // 64) % 2) * 128 + (t // 128) * 64 + t % 64

    t_row = lax.broadcasted_iota(jnp.int32, (GROUP, GROUP), 0)
    t_col = lax.broadcasted_iota(jnp.int32, (GROUP, GROUP), 1)
    before = jnp.where(true_pos(t_row) < true_pos(t_col), 1.0, 0.0).astype(BF16)
    eye = jnp.where(t_row == t_col, 1.0, 0.0).astype(BF16)
    for g in range(2):
        ids = jnp.concatenate([mids[c * 4 + g * 2 + x] for c in range(2) for x in range(2)], axis=1)
        gates = jnp.concatenate([mgates[c * 4 + g * 2 + x] for c in range(2) for x in range(2)], axis=1)
        chosen = jnp.zeros((LOCAL, GROUP), F32)
        gate = jnp.zeros((LOCAL, GROUP), F32)
        for j in range(TOPK):
            hit = ids[j:j + 1, :] == e_id
            chosen = jnp.where(hit, 1.0, chosen)
            gate = jnp.where(hit, gates[j:j + 1, :], gate)
        slot = dot(chosen.astype(BF16), before)
        slot = jnp.where(chosen > 0.0, slot, -1.0)
        here = slot[:, None, :] == s_id
        disp[g] = jnp.where(here, 1.0, 0.0).reshape(LOCAL * CAP, GROUP).astype(BF16)
        weight = jnp.where(here, gate[:, None, :], 0.0).reshape(LOCAL * CAP, GROUP)
        for piece in range(3):
            part = weight.astype(BF16)
            turned = tdot(part, eye).astype(BF16)
            if piece < 2:
                comb[g, :, pl.ds(piece * GROUP, GROUP)] = turned
            else:
                comb3[g] = turned
            weight = weight - part.astype(F32)

    MARK('share0')
    share(0)
    MARK('g2b')
    send_on(1)
    for k in range(NK):
        MARK(f'gw{k}')
        wait_all(tok.at[2 * k], gdr.at[k])
        MARK(f'dsp{k}')
        for h in range(2):
            i = 2 * k + h
            for g in range(2):
                rows = tok[i, :, :, g] if over_y(i) else tok[i, :, g]
                picked = dot(disp[g], rows.reshape(GROUP, T)).astype(BF16)
                xs[:, pl.ds(g * CAP, CAP), pl.ds(h * T, T)] = picked.reshape(LOCAL, CAP, T)
        for half in range(2):
            steps = [k * NEG + half * 2 + q for q in range(2)]
            MARK(f'aw{k}{half}')
            for s in steps:
                w_wait(s)
            MARK(f'a{k}{half}')
            for s in steps:
                eg = s % NEG
                batch = pl.ds(eg * EG, EG)
                for n in range(NF):
                    cols = pl.ds(n * T, T)
                    acc = bdot(xs[batch], ring[s % NS, n].reshape(EG, KS, T))
                    if k > 0:
                        acc = acc + hacc[batch, :, cols]
                    if k < NK - 1:
                        hacc[batch, :, cols] = acc
                        continue
                    act = jax.nn.gelu(acc).astype(BF16)
                    if n < 2:
                        hid[batch, :, cols] = act
                    else:
                        act = act.reshape(EG // 2, 2, 2 * CAP, T)
                        for m in range(2):
                            hid3[pl.ds(eg * EG // 2, EG // 2), pl.ds(m * 2 * CAP, 2 * CAP), pl.ds(m * T, T)] = act[:, m]
            for s in steps:
                w_start(s + NS)
            MARK(f'fw{k}')
            if half == 0 and k < NK - 1:
                if k == 0:
                    send_on(2)
                    send_on(3)
                share(k + 1)

    def route(d):
        if d == 0:
            return my_x, my_dp, x_nbr, y_nbr
        return my_dp, my_x, y_nbr, x_nbr

    def reduce0(c):
        return remote(ypart.at[c, 1 - my_c], r0.at[c], t0s, t0r.at[c], partner)

    def reduce1(c, d, last):
        a, b, dev, _ = route(d)
        side = b if last else 1 - b
        return remote(ypart.at[c, my_c, d, 1 - a, side], r1.at[c, d, side], t1s, fin.at[c] if last else t1r.at[c], dev)

    def reduce2(c, d):
        a, b, _, dev = route(d)
        return remote(ypart.at[c, my_c, d, a, 1 - b], r2.at[c, d], t2s, fin.at[c], dev)

    def rest1(c):
        for d in range(2):
            reduce1(c, d, 1).start()

    def stage1(c):
        MARK(f's1_{c}')
        reduce0(c).wait_recv()
        for last in range(2):
            for d in range(2):
                a, b, _, _ = route(d)
                side = b if last else 1 - b
                ypart[c, my_c, d, 1 - a, side] = ypart[c, my_c, d, 1 - a, side] + r0[c, d, 1 - a, side]
        for d in range(2):
            reduce1(c, d, 0).start()
        if c >= DEFER:
            rest1(c - DEFER)
        for d in range(2):
            a, _, _, _ = route(d)
            ypart[c, my_c, d, a] = ypart[c, my_c, d, a] + r0[c, d, a]

    def stage2(c):
        MARK(f's2_{c}')
        wait_all(r1.at[c, 0], t1r.at[c])
        for d in range(2):
            a, b, _, _ = route(d)
            ypart[c, my_c, d, a, 1 - b] = ypart[c, my_c, d, a, 1 - b] + r1[c, d, 1 - b]
        for d in range(2):
            reduce2(c, d).start()

    def final(c):
        MARK(f'fin{c}')
        wait_all(r0.at[c, 0], fin.at[c])
        for d in range(2):
            a, b, _, _ = route(d)
            moe = ypart[c, my_c, d, a, b] + r1[c, d, b] + r2[c, d]
            x_own = own(c)[:, pl.ds(d * H, H)].astype(F32)
            shared = shy[:, pl.ds(c * T + d * H, H)].astype(F32)
            o_ref[:, pl.ds(c * T + d * H, H)] = (x_own + shared + moe).astype(BF16)

    for c in range(NCH):
        for h in range(NHB):
            s = A_STEPS + c * NHB + h
            MARK(f'bw{s}')
            w_wait(s)
            MARK(f'b{s}')
            third = bdot(hid3[pl.ds(h * EG, EG)], ring[s % NS, 2].reshape(EG, 2 * T, T)).reshape(EB, 2 * CAP, T)
            for q in range(2):
                first = h * EB + q * EG
                out = bdot(hid[pl.ds(first, EG)], ring[s % NS, q].reshape(EG, 2 * T, T))
                out = (out + third[q * EG:(q + 1) * EG]).astype(BF16)
                for g in range(2):
                    for copy in range(2):
                        osc[g, copy, pl.ds(first, EG)] = out[:, g * CAP:(g + 1) * CAP]
            w_start(s + NS)
        if c >= 1:
            stage1(c - 1)
        MARK(f'cmb{c}')
        for g in range(2):
            y = dot(comb[g], osc[g].reshape(2 * GROUP, T)) + dot(comb3[g], osc[g, 0].reshape(GROUP, T))
            y = y.reshape(2, 2, ROWS, T)
            for core in range(2):
                for x in range(2):
                    ypart[c, core, 0, x, g] = y[core, x, :, :H]
                    ypart[c, core, 1, g, x] = y[core, x, :, H:]
        MARK(f'r0_{c}')
        reduce0(c).start()
        if c >= LAG2:
            stage2(c - LAG2)

    MARK('shw')
    w_wait(SH_IN)
    MARK('sh')
    for n in range(NF):
        acc = jnp.zeros((ROWS, T), F32)
        weights = ring[SH_IN % NS, n].reshape(NCH, T, T)
        for k in range(NCH):
            acc = acc + dot(own(k)[...], weights[k])
        hs[:, pl.ds(n * T, T)] = jax.nn.gelu(acc).astype(BF16)
    stage1(NCH - 1)
    for c in range(NCH - DEFER, NCH):
        rest1(c)
    stage2(NCH - 3)
    MARK('show')
    w_wait(SH_OUT)
    MARK('so')
    for c in range(NCH):
        acc = jnp.zeros((ROWS, T), F32)
        for j in range(NF):
            acc = acc + dot(hs[:, pl.ds(j * T, T)], ring[SH_OUT % NS, j, c // 2, c % 2])
        shy[:, pl.ds(c * T, T)] = acc.astype(BF16)
    stage2(NCH - 2)
    stage2(NCH - 1)
    for c in range(NCH):
        final(c)
    MARK('drain')
    wait_all(mids.at[pl.ds(0, 7)], rts.at[0])
    wait_all(mgates.at[pl.ds(0, 7)], rts.at[1])
    wait_all(tok.at[pl.ds(0, 3), 0], g1s)
    wait_all(tok.at[pl.ds(0, 3), 0], g2s)
    wait_all(tok.at[pl.ds(0, 4)], gds)
    wait_all(r0, t0s)
    wait_all(r1, t1s)
    wait_all(r2, t2s)
    MARK(None)


def solution(mesh):
    def layer(tok_x, route_ids, route_gate, w_in, w_out, shared_in, shared_out):
        local = w_in.shape[0]
        any_space = pl.BlockSpec(memory_space=pl.ANY)
        dma = pltpu.SemaphoreType.DMA
        vmem = pltpu.VMEM
        return pl.pallas_call(
            kernel,
            out_shape=pltpu.VMEM((ROWS, WIDTH), BF16),
            in_specs=[any_space] * 8,
            out_specs=pl.BlockSpec(memory_space=pltpu.VMEM),
            scratch_shapes=[
                vmem((NCH, 2, 2, 2, ROWS, T), BF16),
                vmem((8, TOPK, ROWS), jnp.int32),
                vmem((8, TOPK, ROWS), F32),
                vmem((NS, NF, EG, 2, T, T), BF16),
                vmem((LOCAL, 2 * CAP, KS), BF16),
                vmem((LOCAL, 2 * CAP, FF), F32),
                vmem((LOCAL, 2 * CAP, 2 * T), BF16),
                vmem((LOCAL // 2, 4 * CAP, 2 * T), BF16),
                vmem((2, 2, LOCAL, CAP, T), BF16),
                vmem((2, LOCAL * CAP, GROUP), BF16),
                vmem((2, GROUP, 2 * GROUP), BF16),
                vmem((2, GROUP, GROUP), BF16),
                vmem((NCH, 2, 2, 2, 2, ROWS, H), F32),
                vmem((NCH, 2, 2, 2, ROWS, H), F32),
                vmem((NCH, 2, 2, ROWS, H), F32),
                vmem((NCH, 2, ROWS, H), F32),
                vmem((ROWS, FF), BF16),
                vmem((ROWS, WIDTH), BF16),
                dma((3,)), dma((2,)), dma((2,)),
                dma, dma((NK,)), dma, dma((NK,)), dma, dma((NK,)),
                dma((NS,)),
                dma, dma((NCH,)), dma, dma((NCH,)), dma, dma((NCH,)),
            ],
            compiler_params=pltpu.CompilerParams(
                collective_id=0, has_side_effects=True, vmem_limit_bytes=61_000_000),
            name='moe_layer',
        )(tok_x, route_ids.T, route_gate.T,
          w_in.reshape(local, WIDTH // T, T, FF), w_out.reshape(local, NF, T, WIDTH),
          w_out.reshape(local // 2, 2, NF, T, WIDTH),
          shared_in.reshape(EG, 2, T, FF), shared_out.reshape(NF, T, WIDTH))

    row_spec = P(('dp', 'ep'), None)
    expert_spec = P('ep', None, None)
    whole_spec = P(None, None)
    return jax.shard_map(layer, mesh=mesh,
                         in_specs=(row_spec, row_spec, row_spec, expert_spec, expert_spec, whole_spec, whole_spec),
                         out_specs=row_spec, check_vma=False)
```

```python
import jax
import jax.numpy as jnp
from jax import lax
from jax.experimental import pallas as pl
from jax.experimental.pallas import tpu as pltpu
from jax.sharding import PartitionSpec as P

F32 = jnp.float32
BF16 = jnp.bfloat16
MESH = pl.DeviceIdType.MESH

ROWS = 64
WIDTH = 2048
FF = 768
TOPK = 8
LOCAL = 16
CAP = 16
H = 128
T = 256
NCH = WIDTH // T
EG = 4
KS = 2 * T
NK = WIDTH // KS
NEG = LOCAL // EG
EB = 8
NHB = LOCAL // EB
NF = FF // T
GROUP = 256
NS = 13
A_STEPS = NK * NEG
B_STEPS = NCH * NHB
SH_IN = A_STEPS + B_STEPS
SH_OUT = SH_IN + 1
STEPS = SH_OUT + 1
DEFER = 0
LAG2 = 3


def dot(a, b):
    return jnp.dot(a, b, preferred_element_type=F32)


class Mark:
    def __init__(self):
        self.cm = None

    def __call__(self, name):
        if self.cm is not None:
            self.cm.__exit__(None, None, None)
            self.cm = None
        if name:
            self.cm = jax.named_scope(name)
            self.cm.__enter__()


MARK = Mark()


def tdot(a, b):
    return lax.dot_general(a, b, (((0,), (0,)), ((), ())), preferred_element_type=F32)


def bdot(a, b):
    return lax.dot_general(a, b, (((2,), (1,)), ((0,), (0,))), preferred_element_type=F32)


def kernel(x_ref, ids_ref, gates_ref, win_ref, wout_ref, wpair_ref, sin_ref, sout_ref, o_ref,
           tok, mids, mgates, ring, xs, hacc, hid, hid3, osc, disp, comb, comb3, ypart, r0, r1, r2, hs, shy,
           ld_sem, rts, rtr, g1s, g1r, g2s, g2r, gds, gdr, w_sem, t0s, t0r, t1s, t1r, t2s, fin):
    my_dp = lax.axis_index('dp')
    my_ep = lax.axis_index('ep')
    my_x = my_ep // 2
    my_c = my_ep % 2
    my_pos = my_c * 4 + my_dp * 2 + my_x
    partner = (my_dp, my_x * 2 + (1 - my_c))
    x_nbr = (my_dp, (1 - my_x) * 2 + my_c)
    y_nbr = (1 - my_dp, my_ep)
    e_off = my_dp * LOCAL

    def wait_all(ref, sem):
        pltpu.make_async_copy(ref, ref, sem).wait()

    def w_copies(s):
        slot = s % NS
        if s == SH_OUT:
            return [pltpu.make_async_copy(
                sout_ref.at[:, :, pl.ds(c * T, T)], ring.at[slot, :, c // 2, c % 2], w_sem.at[slot]) for c in range(NCH)]
        copies = []
        for n in range(NF):
            if s < A_STEPS:
                k, eg = divmod(s, NEG)
                src = win_ref.at[pl.ds(e_off + eg * EG, EG), pl.ds(2 * k, 2), :, pl.ds(n * T, T)]
            elif s < SH_IN:
                c, h = divmod(s - A_STEPS, NHB)
                if n < 2:
                    src = wout_ref.at[pl.ds(e_off + h * EB + n * EG, EG), pl.ds(0, 2), :, pl.ds(c * T, T)]
                else:
                    src = wpair_ref.at[pl.ds(e_off // 2 + h * EG, EG), :, 2, :, pl.ds(c * T, T)]
            else:
                src = sin_ref.at[:, :, :, pl.ds(n * T, T)]
            copies.append(pltpu.make_async_copy(src, ring.at[slot, n], w_sem.at[slot]))
        return copies

    def w_start(s):
        if s < STEPS:
            for copy in w_copies(s):
                copy.start()

    def w_wait(s):
        wait_all(ring.at[s % NS], w_sem.at[s % NS])

    IDS, GATES = NCH, NCH + 1

    def over_y(i):
        return i % 2 == 1

    def own_core(i):
        return tok.at[i, my_c]

    def own_pair(i):
        return tok.at[i, my_c, my_x if over_y(i) else my_dp]

    def own(i):
        if i == IDS:
            return mids.at[my_pos]
        if i == GATES:
            return mgates.at[my_pos]
        return tok.at[i, my_c, my_x, my_dp] if over_y(i) else tok.at[i, my_c, my_dp, my_x]

    def load(i):
        src = ids_ref if i == IDS else gates_ref if i == GATES else x_ref.at[:, pl.ds(i * T, T)]
        return pltpu.make_async_copy(src, own(i), ld_sem.at[max(0, i - NCH + 1)])

    def remote(src, dst, ssem, rsem, dev):
        return pltpu.make_async_remote_copy(
            src_ref=src, dst_ref=dst, send_sem=ssem, recv_sem=rsem, device_id=dev, device_id_type=MESH)

    def gather1(i):
        return remote(own(i), own(i), g1s, g1r.at[i // 2], y_nbr if over_y(i) else x_nbr)

    def gather2(i):
        return remote(own_pair(i), own_pair(i), g2s, g2r.at[i // 2], x_nbr if over_y(i) else y_nbr)

    def gatherd(i):
        return remote(own_core(i), own_core(i), gds, gdr.at[i // 2], partner)

    routing = [IDS, GATES]
    items = routing + list(range(NCH))

    def peer(r):
        dp = 1 - my_dp if r & 1 else my_dp
        x = 1 - my_x if r & 2 else my_x
        c = 1 - my_c if r & 4 else my_c
        return dp, x * 2 + c

    def tell(i, r):
        return remote(own(i), own(i), rts.at[i - NCH], rtr.at[i - NCH], peer(r))

    MARK('sig')
    barrier = pltpu.get_barrier_semaphore()
    for r in range(1, 8):
        pl.semaphore_signal(barrier, inc=1, device_id=peer(r), device_id_type=MESH)
    for i in items:
        load(i).start()
    hid3[...] = jnp.zeros_like(hid3)
    MARK('ld')
    wait_all(tok.at[0], ld_sem.at[0])
    for i in routing:
        load(i).wait()
    MARK('ws')
    for s in range(NS):
        w_start(s)
    MARK('barrier')
    pl.semaphore_wait(barrier, 7)

    def direct(i, r):
        return remote(own(i), own(i), g1s, g2r.at[0], peer(r))

    def send(p):
        for i in (2 * p, 2 * p + 1):
            gather1(i).start()

    def send_on(p):
        wait_all(tok.at[2 * p, 0, 0], g1r.at[p])
        for i in (2 * p, 2 * p + 1):
            gather2(i).start()

    def share(p):
        wait_all(tok.at[pl.ds(0, 3), 0, 0] if p == 0 else tok.at[2 * p, 0], g2r.at[p])
        for i in (2 * p, 2 * p + 1):
            gatherd(i).start()

    for r in (3, 7, 1, 2, 5, 6, 4):
        for i in routing:
            tell(i, r).start()
    MARK('g1')
    for r in (3, 2, 1):
        for i in (0, 1):
            direct(i, r).start()
    send(1)
    MARK('rtw')
    wait_all(mids.at[pl.ds(0, 7)], rtr.at[0])
    wait_all(mgates.at[pl.ds(0, 7)], rtr.at[1])
    send(2)
    send(3)

    MARK('route')
    e_id = lax.broadcasted_iota(jnp.int32, (LOCAL, GROUP), 0) + (my_ep * (2 * LOCAL) + e_off)
    s_id = lax.broadcasted_iota(jnp.int32, (LOCAL, CAP, GROUP), 1).astype(F32)

    def true_pos(t):
        return ((t // 64) % 2) * 128 + (t // 128) * 64 + t % 64

    t_row = lax.broadcasted_iota(jnp.int32, (GROUP, GROUP), 0)
    t_col = lax.broadcasted_iota(jnp.int32, (GROUP, GROUP), 1)
    before = jnp.where(true_pos(t_row) < true_pos(t_col), 1.0, 0.0).astype(BF16)
    eye = jnp.where(t_row == t_col, 1.0, 0.0).astype(BF16)
    for g in range(2):
        ids = jnp.concatenate([mids[c * 4 + g * 2 + x] for c in range(2) for x in range(2)], axis=1)
        gates = jnp.concatenate([mgates[c * 4 + g * 2 + x] for c in range(2) for x in range(2)], axis=1)
        chosen = jnp.zeros((LOCAL, GROUP), F32)
        gate = jnp.zeros((LOCAL, GROUP), F32)
        for j in range(TOPK):
            hit = ids[j:j + 1, :] == e_id
            chosen = jnp.where(hit, 1.0, chosen)
            gate = jnp.where(hit, gates[j:j + 1, :], gate)
        slot = dot(chosen.astype(BF16), before)
        slot = jnp.where(chosen > 0.0, slot, -1.0)
        here = slot[:, None, :] == s_id
        disp[g] = jnp.where(here, 1.0, 0.0).reshape(LOCAL * CAP, GROUP).astype(BF16)
        weight = jnp.where(here, gate[:, None, :], 0.0).reshape(LOCAL * CAP, GROUP)
        for piece in range(3):
            part = weight.astype(BF16)
            turned = tdot(part, eye).astype(BF16)
            if piece < 2:
                comb[g, :, pl.ds(piece * GROUP, GROUP)] = turned
            else:
                comb3[g] = turned
            weight = weight - part.astype(F32)

    MARK('g2b')
    send_on(1)
    MARK('share0')
    share(0)
    for k in range(NK):
        MARK(f'gw{k}')
        wait_all(tok.at[2 * k], gdr.at[k])
        MARK(f'dsp{k}')
        for h in range(2):
            i = 2 * k + h
            for g in range(2):
                rows = tok[i, :, :, g] if over_y(i) else tok[i, :, g]
                picked = dot(disp[g], rows.reshape(GROUP, T)).astype(BF16)
                xs[:, pl.ds(g * CAP, CAP), pl.ds(h * T, T)] = picked.reshape(LOCAL, CAP, T)
        for half in range(2):
            steps = [k * NEG + half * 2 + q for q in range(2)]
            MARK(f'aw{k}{half}')
            for s in steps:
                w_wait(s)
            MARK(f'a{k}{half}')
            for s in steps:
                eg = s % NEG
                batch = pl.ds(eg * EG, EG)
                for n in range(NF):
                    cols = pl.ds(n * T, T)
                    acc = bdot(xs[batch], ring[s % NS, n].reshape(EG, KS, T))
                    if k > 0:
                        acc = acc + hacc[batch, :, cols]
                    if k < NK - 1:
                        hacc[batch, :, cols] = acc
                        continue
                    act = jax.nn.gelu(acc).astype(BF16)
                    if n < 2:
                        hid[batch, :, cols] = act
                    else:
                        act = act.reshape(EG // 2, 2, 2 * CAP, T)
                        for m in range(2):
                            hid3[pl.ds(eg * EG // 2, EG // 2), pl.ds(m * 2 * CAP, 2 * CAP), pl.ds(m * T, T)] = act[:, m]
            for s in steps:
                w_start(s + NS)
            MARK(f'fw{k}')
            if half == 0 and k < NK - 1:
                if k == 0:
                    send_on(2)
                    send_on(3)
                share(k + 1)

    def route(d):
        if d == 0:
            return my_x, my_dp, x_nbr, y_nbr
        return my_dp, my_x, y_nbr, x_nbr

    def reduce0(c):
        return remote(ypart.at[c, 1 - my_c], r0.at[c], t0s, t0r.at[c], partner)

    def reduce1(c, d, last):
        a, b, dev, _ = route(d)
        side = b if last else 1 - b
        return remote(ypart.at[c, my_c, d, 1 - a, side], r1.at[c, d, side], t1s, fin.at[c] if last else t1r.at[c], dev)

    def reduce2(c, d):
        a, b, _, dev = route(d)
        return remote(ypart.at[c, my_c, d, a, 1 - b], r2.at[c, d], t2s, fin.at[c], dev)

    def rest1(c):
        for d in range(2):
            reduce1(c, d, 1).start()

    def stage1(c):
        MARK(f's1_{c}')
        reduce0(c).wait_recv()
        for last in range(2):
            for d in range(2):
                a, b, _, _ = route(d)
                side = b if last else 1 - b
                ypart[c, my_c, d, 1 - a, side] = ypart[c, my_c, d, 1 - a, side] + r0[c, d, 1 - a, side]
        for d in range(2):
            reduce1(c, d, 0).start()
        if c >= DEFER:
            rest1(c - DEFER)
        for d in range(2):
            a, _, _, _ = route(d)
            ypart[c, my_c, d, a] = ypart[c, my_c, d, a] + r0[c, d, a]

    def stage2(c):
        MARK(f's2_{c}')
        wait_all(r1.at[c, 0], t1r.at[c])
        for d in range(2):
            a, b, _, _ = route(d)
            ypart[c, my_c, d, a, 1 - b] = ypart[c, my_c, d, a, 1 - b] + r1[c, d, 1 - b]
        for d in range(2):
            reduce2(c, d).start()

    def final(c):
        MARK(f'fin{c}')
        wait_all(r0.at[c, 0], fin.at[c])
        for d in range(2):
            a, b, _, _ = route(d)
            moe = ypart[c, my_c, d, a, b] + r1[c, d, b] + r2[c, d]
            x_own = own(c)[:, pl.ds(d * H, H)].astype(F32)
            shared = shy[:, pl.ds(c * T + d * H, H)].astype(F32)
            o_ref[:, pl.ds(c * T + d * H, H)] = (x_own + shared + moe).astype(BF16)

    for c in range(NCH):
        for h in range(NHB):
            s = A_STEPS + c * NHB + h
            MARK(f'bw{s}')
            w_wait(s)
            MARK(f'b{s}')
            third = bdot(hid3[pl.ds(h * EG, EG)], ring[s % NS, 2].reshape(EG, 2 * T, T)).reshape(EB, 2 * CAP, T)
            for q in range(2):
                first = h * EB + q * EG
                out = bdot(hid[pl.ds(first, EG)], ring[s % NS, q].reshape(EG, 2 * T, T))
                out = (out + third[q * EG:(q + 1) * EG]).astype(BF16)
                for g in range(2):
                    for copy in range(2):
                        osc[g, copy, pl.ds(first, EG)] = out[:, g * CAP:(g + 1) * CAP]
            w_start(s + NS)
        if c >= 1:
            stage1(c - 1)
        MARK(f'cmb{c}')
        for g in range(2):
            y = dot(comb[g], osc[g].reshape(2 * GROUP, T)) + dot(comb3[g], osc[g, 0].reshape(GROUP, T))
            y = y.reshape(2, 2, ROWS, T)
            for core in range(2):
                for x in range(2):
                    ypart[c, core, 0, x, g] = y[core, x, :, :H]
                    ypart[c, core, 1, g, x] = y[core, x, :, H:]
        MARK(f'r0_{c}')
        reduce0(c).start()
        if c >= LAG2:
            stage2(c - LAG2)

    MARK('shw')
    w_wait(SH_IN)
    MARK('sh')
    for n in range(NF):
        acc = jnp.zeros((ROWS, T), F32)
        weights = ring[SH_IN % NS, n].reshape(NCH, T, T)
        for k in range(NCH):
            acc = acc + dot(own(k)[...], weights[k])
        hs[:, pl.ds(n * T, T)] = jax.nn.gelu(acc).astype(BF16)
    stage1(NCH - 1)
    for c in range(NCH - DEFER, NCH):
        rest1(c)
    stage2(NCH - 3)
    MARK('show')
    w_wait(SH_OUT)
    MARK('so')
    for c in range(NCH):
        acc = jnp.zeros((ROWS, T), F32)
        for j in range(NF):
            acc = acc + dot(hs[:, pl.ds(j * T, T)], ring[SH_OUT % NS, j, c // 2, c % 2])
        shy[:, pl.ds(c * T, T)] = acc.astype(BF16)
    stage2(NCH - 2)
    stage2(NCH - 1)
    for c in range(NCH):
        final(c)
    MARK('drain')
    wait_all(mids.at[pl.ds(0, 7)], rts.at[0])
    wait_all(mgates.at[pl.ds(0, 7)], rts.at[1])
    wait_all(tok.at[pl.ds(0, 3), 0], g1s)
    wait_all(tok.at[pl.ds(0, 3), 0], g2s)
    wait_all(tok.at[pl.ds(0, 4)], gds)
    wait_all(r0, t0s)
    wait_all(r1, t1s)
    wait_all(r2, t2s)
    MARK(None)


def solution(mesh):
    def layer(tok_x, route_ids, route_gate, w_in, w_out, shared_in, shared_out):
        local = w_in.shape[0]
        any_space = pl.BlockSpec(memory_space=pl.ANY)
        dma = pltpu.SemaphoreType.DMA
        vmem = pltpu.VMEM
        return pl.pallas_call(
            kernel,
            out_shape=pltpu.VMEM((ROWS, WIDTH), BF16),
            in_specs=[any_space] * 8,
            out_specs=pl.BlockSpec(memory_space=pltpu.VMEM),
            scratch_shapes=[
                vmem((NCH, 2, 2, 2, ROWS, T), BF16),
                vmem((8, TOPK, ROWS), jnp.int32),
                vmem((8, TOPK, ROWS), F32),
                vmem((NS, NF, EG, 2, T, T), BF16),
                vmem((LOCAL, 2 * CAP, KS), BF16),
                vmem((LOCAL, 2 * CAP, FF), F32),
                vmem((LOCAL, 2 * CAP, 2 * T), BF16),
                vmem((LOCAL // 2, 4 * CAP, 2 * T), BF16),
                vmem((2, 2, LOCAL, CAP, T), BF16),
                vmem((2, LOCAL * CAP, GROUP), BF16),
                vmem((2, GROUP, 2 * GROUP), BF16),
                vmem((2, GROUP, GROUP), BF16),
                vmem((NCH, 2, 2, 2, 2, ROWS, H), F32),
                vmem((NCH, 2, 2, 2, ROWS, H), F32),
                vmem((NCH, 2, 2, ROWS, H), F32),
                vmem((NCH, 2, ROWS, H), F32),
                vmem((ROWS, FF), BF16),
                vmem((ROWS, WIDTH), BF16),
                dma((3,)), dma((2,)), dma((2,)),
                dma, dma((NK,)), dma, dma((NK,)), dma, dma((NK,)),
                dma((NS,)),
                dma, dma((NCH,)), dma, dma((NCH,)), dma, dma((NCH,)),
            ],
            compiler_params=pltpu.CompilerParams(
                collective_id=0, has_side_effects=True, vmem_limit_bytes=61_000_000),
            name='moe_layer',
        )(tok_x, route_ids.T, route_gate.T,
          w_in.reshape(local, WIDTH // T, T, FF), w_out.reshape(local, NF, T, WIDTH),
          w_out.reshape(local // 2, 2, NF, T, WIDTH),
          shared_in.reshape(EG, 2, T, FF), shared_out.reshape(NF, T, WIDTH))

    row_spec = P(('dp', 'ep'), None)
    expert_spec = P('ep', None, None)
    whole_spec = P(None, None)
    return jax.shard_map(layer, mesh=mesh,
                         in_specs=(row_spec, row_spec, row_spec, expert_spec, expert_spec, whole_spec, whole_spec),
                         out_specs=row_spec, check_vma=False)
```

```python
import jax
import jax.numpy as jnp
from jax import lax
from jax.experimental import pallas as pl
from jax.experimental.pallas import tpu as pltpu
from jax.sharding import PartitionSpec as P

F32 = jnp.float32
BF16 = jnp.bfloat16
MESH = pl.DeviceIdType.MESH

ROWS = 64
WIDTH = 2048
FF = 768
TOPK = 8
LOCAL = 16
CAP = 16
H = 128
T = 256
NCH = WIDTH // T
EG = 4
KS = 2 * T
NK = WIDTH // KS
NEG = LOCAL // EG
EB = 8
NHB = LOCAL // EB
NF = FF // T
GROUP = 256
NS = 13
A_STEPS = NK * NEG
B_STEPS = NCH * NHB
SH_IN = A_STEPS + B_STEPS
SH_OUT = SH_IN + 1
STEPS = SH_OUT + 1
DEFER = 0
LAG2 = 3


def dot(a, b):
    return jnp.dot(a, b, preferred_element_type=F32)


class Mark:
    def __init__(self):
        self.cm = None

    def __call__(self, name):
        if self.cm is not None:
            self.cm.__exit__(None, None, None)
            self.cm = None
        if name:
            self.cm = jax.named_scope(name)
            self.cm.__enter__()


MARK = Mark()


def tdot(a, b):
    return lax.dot_general(a, b, (((0,), (0,)), ((), ())), preferred_element_type=F32)


def bdot(a, b):
    return lax.dot_general(a, b, (((2,), (1,)), ((0,), (0,))), preferred_element_type=F32)


def kernel(x_ref, ids_ref, gates_ref, win_ref, wout_ref, wpair_ref, sin_ref, sout_ref, o_ref,
           tok, mids, mgates, ring, xs, hacc, hid, hid3, osc, disp, comb, comb3, ypart, r0, r1, r2, hs, shy,
           ld_sem, rts, rtr, g1s, g1r, g2s, g2r, gds, gdr, w_sem, t0s, t0r, t1s, t1r, t2s, fin):
    my_dp = lax.axis_index('dp')
    my_ep = lax.axis_index('ep')
    my_x = my_ep // 2
    my_c = my_ep % 2
    my_pos = my_c * 4 + my_dp * 2 + my_x
    partner = (my_dp, my_x * 2 + (1 - my_c))
    x_nbr = (my_dp, (1 - my_x) * 2 + my_c)
    y_nbr = (1 - my_dp, my_ep)
    e_off = my_dp * LOCAL

    def wait_all(ref, sem):
        pltpu.make_async_copy(ref, ref, sem).wait()

    def w_copies(s):
        slot = s % NS
        if s == SH_OUT:
            return [pltpu.make_async_copy(
                sout_ref.at[:, :, pl.ds(c * T, T)], ring.at[slot, :, c // 2, c % 2], w_sem.at[slot]) for c in range(NCH)]
        copies = []
        for n in range(NF):
            if s < A_STEPS:
                k, eg = divmod(s, NEG)
                src = win_ref.at[pl.ds(e_off + eg * EG, EG), pl.ds(2 * k, 2), :, pl.ds(n * T, T)]
            elif s < SH_IN:
                c, h = divmod(s - A_STEPS, NHB)
                if n < 2:
                    src = wout_ref.at[pl.ds(e_off + h * EB + n * EG, EG), pl.ds(0, 2), :, pl.ds(c * T, T)]
                else:
                    src = wpair_ref.at[pl.ds(e_off // 2 + h * EG, EG), :, 2, :, pl.ds(c * T, T)]
            else:
                src = sin_ref.at[:, :, :, pl.ds(n * T, T)]
            copies.append(pltpu.make_async_copy(src, ring.at[slot, n], w_sem.at[slot]))
        return copies

    def w_start(s):
        if s < STEPS:
            for copy in w_copies(s):
                copy.start()

    def w_wait(s):
        wait_all(ring.at[s % NS], w_sem.at[s % NS])

    IDS, GATES = NCH, NCH + 1

    def over_y(i):
        return i % 2 == 1

    def own_core(i):
        return tok.at[i, my_c]

    def own_pair(i):
        return tok.at[i, my_c, my_x if over_y(i) else my_dp]

    def own(i):
        if i == IDS:
            return mids.at[my_pos]
        if i == GATES:
            return mgates.at[my_pos]
        return tok.at[i, my_c, my_x, my_dp] if over_y(i) else tok.at[i, my_c, my_dp, my_x]

    def load(i):
        src = ids_ref if i == IDS else gates_ref if i == GATES else x_ref.at[:, pl.ds(i * T, T)]
        return pltpu.make_async_copy(src, own(i), ld_sem.at[max(0, i - NCH + 1)])

    def remote(src, dst, ssem, rsem, dev):
        return pltpu.make_async_remote_copy(
            src_ref=src, dst_ref=dst, send_sem=ssem, recv_sem=rsem, device_id=dev, device_id_type=MESH)

    def gather1(i):
        return remote(own(i), own(i), g1s, g1r.at[i // 2], y_nbr if over_y(i) else x_nbr)

    def gather2(i):
        return remote(own_pair(i), own_pair(i), g2s, g2r.at[i // 2], x_nbr if over_y(i) else y_nbr)

    def gatherd(i):
        return remote(own_core(i), own_core(i), gds, gdr.at[i // 2], partner)

    routing = [IDS, GATES]
    items = routing + list(range(NCH))

    def peer(r):
        dp = 1 - my_dp if r & 1 else my_dp
        x = 1 - my_x if r & 2 else my_x
        c = 1 - my_c if r & 4 else my_c
        return dp, x * 2 + c

    def tell(i, r):
        return remote(own(i), own(i), rts.at[i - NCH], rtr.at[2 if r == 4 and i == GATES else i - NCH], peer(r))

    MARK('sig')
    barrier = pltpu.get_barrier_semaphore()
    for r in range(1, 8):
        pl.semaphore_signal(barrier, inc=1, device_id=peer(r), device_id_type=MESH)
    for i in items:
        load(i).start()
    hid3[...] = jnp.zeros_like(hid3)
    MARK('ld')
    wait_all(tok.at[0], ld_sem.at[0])
    for i in routing:
        load(i).wait()
    MARK('ws')
    for s in range(NS):
        w_start(s)
    MARK('barrier')
    pl.semaphore_wait(barrier, 7)

    def send(p):
        for i in (2 * p, 2 * p + 1):
            gather1(i).start()

    def send_on(p):
        wait_all(tok.at[2 * p, 0, 0], g1r.at[p])
        for i in (2 * p, 2 * p + 1):
            gather2(i).start()

    def share(p):
        wait_all(tok.at[2 * p, 0], g2r.at[p])
        for i in (2 * p, 2 * p + 1):
            gatherd(i).start()

    for r in (4, 3, 7, 1, 2, 5, 6):
        for i in routing:
            tell(i, r).start()
    MARK('g1')
    send(0)
    MARK('g1b')
    tell(GATES, 4).wait_recv()
    for p in range(1, NK):
        send(p)
    MARK('g2a')
    send_on(0)
    MARK('rtw')
    wait_all(mids.at[pl.ds(0, 7)], rtr.at[0])
    wait_all(mgates.at[pl.ds(0, 6)], rtr.at[1])

    MARK('route')
    e_id = lax.broadcasted_iota(jnp.int32, (LOCAL, GROUP), 0) + (my_ep * (2 * LOCAL) + e_off)
    s_id = lax.broadcasted_iota(jnp.int32, (LOCAL, CAP, GROUP), 1).astype(F32)

    def true_pos(t):
        return ((t // 64) % 2) * 128 + (t // 128) * 64 + t % 64

    t_row = lax.broadcasted_iota(jnp.int32, (GROUP, GROUP), 0)
    t_col = lax.broadcasted_iota(jnp.int32, (GROUP, GROUP), 1)
    before = jnp.where(true_pos(t_row) < true_pos(t_col), 1.0, 0.0).astype(BF16)
    eye = jnp.where(t_row == t_col, 1.0, 0.0).astype(BF16)
    for g in range(2):
        ids = jnp.concatenate([mids[c * 4 + g * 2 + x] for c in range(2) for x in range(2)], axis=1)
        gates = jnp.concatenate([mgates[c * 4 + g * 2 + x] for c in range(2) for x in range(2)], axis=1)
        chosen = jnp.zeros((LOCAL, GROUP), F32)
        gate = jnp.zeros((LOCAL, GROUP), F32)
        for j in range(TOPK):
            hit = ids[j:j + 1, :] == e_id
            chosen = jnp.where(hit, 1.0, chosen)
            gate = jnp.where(hit, gates[j:j + 1, :], gate)
        slot = dot(chosen.astype(BF16), before)
        slot = jnp.where(chosen > 0.0, slot, -1.0)
        here = slot[:, None, :] == s_id
        disp[g] = jnp.where(here, 1.0, 0.0).reshape(LOCAL * CAP, GROUP).astype(BF16)
        weight = jnp.where(here, gate[:, None, :], 0.0).reshape(LOCAL * CAP, GROUP)
        for piece in range(3):
            part = weight.astype(BF16)
            turned = tdot(part, eye).astype(BF16)
            if piece < 2:
                comb[g, :, pl.ds(piece * GROUP, GROUP)] = turned
            else:
                comb3[g] = turned
            weight = weight - part.astype(F32)

    MARK('g2b')
    for p in range(1, NK):
        send_on(p)
    MARK('share0')
    share(0)
    for k in range(NK):
        MARK(f'gw{k}')
        wait_all(tok.at[2 * k], gdr.at[k])
        MARK(f'dsp{k}')
        for h in range(2):
            i = 2 * k + h
            for g in range(2):
                rows = tok[i, :, :, g] if over_y(i) else tok[i, :, g]
                picked = dot(disp[g], rows.reshape(GROUP, T)).astype(BF16)
                xs[:, pl.ds(g * CAP, CAP), pl.ds(h * T, T)] = picked.reshape(LOCAL, CAP, T)
        for half in range(2):
            steps = [k * NEG + half * 2 + q for q in range(2)]
            MARK(f'aw{k}{half}')
            for s in steps:
                w_wait(s)
            MARK(f'a{k}{half}')
            for s in steps:
                eg = s % NEG
                batch = pl.ds(eg * EG, EG)
                for n in range(NF):
                    cols = pl.ds(n * T, T)
                    acc = bdot(xs[batch], ring[s % NS, n].reshape(EG, KS, T))
                    if k > 0:
                        acc = acc + hacc[batch, :, cols]
                    if k < NK - 1:
                        hacc[batch, :, cols] = acc
                        continue
                    act = jax.nn.gelu(acc).astype(BF16)
                    if n < 2:
                        hid[batch, :, cols] = act
                    else:
                        act = act.reshape(EG // 2, 2, 2 * CAP, T)
                        for m in range(2):
                            hid3[pl.ds(eg * EG // 2, EG // 2), pl.ds(m * 2 * CAP, 2 * CAP), pl.ds(m * T, T)] = act[:, m]
            for s in steps:
                w_start(s + NS)
            MARK(f'fw{k}')
            if half == 0 and k < NK - 1:
                share(k + 1)

    def route(d):
        if d == 0:
            return my_x, my_dp, x_nbr, y_nbr
        return my_dp, my_x, y_nbr, x_nbr

    def reduce0(c):
        return remote(ypart.at[c, 1 - my_c], r0.at[c], t0s, t0r.at[c], partner)

    def reduce1(c, d, last):
        a, b, dev, _ = route(d)
        side = b if last else 1 - b
        return remote(ypart.at[c, my_c, d, 1 - a, side], r1.at[c, d, side], t1s, fin.at[c] if last else t1r.at[c], dev)

    def reduce2(c, d):
        a, b, _, dev = route(d)
        return remote(ypart.at[c, my_c, d, a, 1 - b], r2.at[c, d], t2s, fin.at[c], dev)

    def rest1(c):
        for d in range(2):
            reduce1(c, d, 1).start()

    def stage1(c):
        MARK(f's1_{c}')
        reduce0(c).wait_recv()
        for last in range(2):
            for d in range(2):
                a, b, _, _ = route(d)
                side = b if last else 1 - b
                ypart[c, my_c, d, 1 - a, side] = ypart[c, my_c, d, 1 - a, side] + r0[c, d, 1 - a, side]
        for d in range(2):
            reduce1(c, d, 0).start()
        if c >= DEFER:
            rest1(c - DEFER)
        for d in range(2):
            a, _, _, _ = route(d)
            ypart[c, my_c, d, a] = ypart[c, my_c, d, a] + r0[c, d, a]

    def stage2(c):
        MARK(f's2_{c}')
        wait_all(r1.at[c, 0], t1r.at[c])
        for d in range(2):
            a, b, _, _ = route(d)
            ypart[c, my_c, d, a, 1 - b] = ypart[c, my_c, d, a, 1 - b] + r1[c, d, 1 - b]
        for d in range(2):
            reduce2(c, d).start()

    def final(c):
        MARK(f'fin{c}')
        wait_all(r0.at[c, 0], fin.at[c])
        for d in range(2):
            a, b, _, _ = route(d)
            moe = ypart[c, my_c, d, a, b] + r1[c, d, b] + r2[c, d]
            x_own = own(c)[:, pl.ds(d * H, H)].astype(F32)
            shared = shy[:, pl.ds(c * T + d * H, H)].astype(F32)
            o_ref[:, pl.ds(c * T + d * H, H)] = (x_own + shared + moe).astype(BF16)

    for c in range(NCH):
        for h in range(NHB):
            s = A_STEPS + c * NHB + h
            MARK(f'bw{s}')
            w_wait(s)
            MARK(f'b{s}')
            third = bdot(hid3[pl.ds(h * EG, EG)], ring[s % NS, 2].reshape(EG, 2 * T, T)).reshape(EB, 2 * CAP, T)
            for q in range(2):
                first = h * EB + q * EG
                out = bdot(hid[pl.ds(first, EG)], ring[s % NS, q].reshape(EG, 2 * T, T))
                out = (out + third[q * EG:(q + 1) * EG]).astype(BF16)
                for g in range(2):
                    for copy in range(2):
                        osc[g, copy, pl.ds(first, EG)] = out[:, g * CAP:(g + 1) * CAP]
            w_start(s + NS)
        if c >= 1:
            stage1(c - 1)
        MARK(f'cmb{c}')
        for g in range(2):
            y = dot(comb[g], osc[g].reshape(2 * GROUP, T)) + dot(comb3[g], osc[g, 0].reshape(GROUP, T))
            y = y.reshape(2, 2, ROWS, T)
            for core in range(2):
                for x in range(2):
                    ypart[c, core, 0, x, g] = y[core, x, :, :H]
                    ypart[c, core, 1, g, x] = y[core, x, :, H:]
        MARK(f'r0_{c}')
        reduce0(c).start()
        if c >= LAG2:
            stage2(c - LAG2)

    MARK('shw')
    w_wait(SH_IN)
    MARK('sh')
    for n in range(NF):
        acc = jnp.zeros((ROWS, T), F32)
        weights = ring[SH_IN % NS, n].reshape(NCH, T, T)
        for k in range(NCH):
            acc = acc + dot(own(k)[...], weights[k])
        hs[:, pl.ds(n * T, T)] = jax.nn.gelu(acc).astype(BF16)
    stage1(NCH - 1)
    for c in range(NCH - DEFER, NCH):
        rest1(c)
    stage2(NCH - 3)
    MARK('show')
    w_wait(SH_OUT)
    MARK('so')
    for c in range(NCH):
        acc = jnp.zeros((ROWS, T), F32)
        for j in range(NF):
            acc = acc + dot(hs[:, pl.ds(j * T, T)], ring[SH_OUT % NS, j, c // 2, c % 2])
        shy[:, pl.ds(c * T, T)] = acc.astype(BF16)
    stage2(NCH - 2)
    stage2(NCH - 1)
    for c in range(NCH):
        final(c)
    MARK('drain')
    wait_all(mids.at[pl.ds(0, 7)], rts.at[0])
    wait_all(mgates.at[pl.ds(0, 7)], rts.at[1])
    wait_all(tok.at[0], g1s)
    wait_all(tok.at[pl.ds(0, 2)], g2s)
    wait_all(tok.at[pl.ds(0, 4)], gds)
    wait_all(r0, t0s)
    wait_all(r1, t1s)
    wait_all(r2, t2s)
    MARK(None)


def solution(mesh):
    def layer(tok_x, route_ids, route_gate, w_in, w_out, shared_in, shared_out):
        local = w_in.shape[0]
        any_space = pl.BlockSpec(memory_space=pl.ANY)
        dma = pltpu.SemaphoreType.DMA
        vmem = pltpu.VMEM
        return pl.pallas_call(
            kernel,
            out_shape=pltpu.VMEM((ROWS, WIDTH), BF16),
            in_specs=[any_space] * 8,
            out_specs=pl.BlockSpec(memory_space=pltpu.VMEM),
            scratch_shapes=[
                vmem((NCH, 2, 2, 2, ROWS, T), BF16),
                vmem((8, TOPK, ROWS), jnp.int32),
                vmem((8, TOPK, ROWS), F32),
                vmem((NS, NF, EG, 2, T, T), BF16),
                vmem((LOCAL, 2 * CAP, KS), BF16),
                vmem((LOCAL, 2 * CAP, FF), F32),
                vmem((LOCAL, 2 * CAP, 2 * T), BF16),
                vmem((LOCAL // 2, 4 * CAP, 2 * T), BF16),
                vmem((2, 2, LOCAL, CAP, T), BF16),
                vmem((2, LOCAL * CAP, GROUP), BF16),
                vmem((2, GROUP, 2 * GROUP), BF16),
                vmem((2, GROUP, GROUP), BF16),
                vmem((NCH, 2, 2, 2, 2, ROWS, H), F32),
                vmem((NCH, 2, 2, 2, ROWS, H), F32),
                vmem((NCH, 2, 2, ROWS, H), F32),
                vmem((NCH, 2, ROWS, H), F32),
                vmem((ROWS, FF), BF16),
                vmem((ROWS, WIDTH), BF16),
                dma((3,)), dma((2,)), dma((3,)),
                dma, dma((NK,)), dma, dma((NK,)), dma, dma((NK,)),
                dma((NS,)),
                dma, dma((NCH,)), dma, dma((NCH,)), dma, dma((NCH,)),
            ],
            compiler_params=pltpu.CompilerParams(
                collective_id=0, has_side_effects=True, vmem_limit_bytes=61_000_000),
            name='moe_layer',
        )(tok_x, route_ids.T, route_gate.T,
          w_in.reshape(local, WIDTH // T, T, FF), w_out.reshape(local, NF, T, WIDTH),
          w_out.reshape(local // 2, 2, NF, T, WIDTH),
          shared_in.reshape(EG, 2, T, FF), shared_out.reshape(NF, T, WIDTH))

    row_spec = P(('dp', 'ep'), None)
    expert_spec = P('ep', None, None)
    whole_spec = P(None, None)
    return jax.shard_map(layer, mesh=mesh,
                         in_specs=(row_spec, row_spec, row_spec, expert_spec, expert_spec, whole_spec, whole_spec),
                         out_specs=row_spec, check_vma=False)
```

```python
import jax
import jax.numpy as jnp
from jax import lax
from jax.experimental import pallas as pl
from jax.experimental.pallas import tpu as pltpu
from jax.sharding import PartitionSpec as P

F32 = jnp.float32
BF16 = jnp.bfloat16
MESH = pl.DeviceIdType.MESH

ROWS = 64
WIDTH = 2048
FF = 768
TOPK = 8
LOCAL = 16
CAP = 16
H = 128
T = 256
NCH = WIDTH // T
EG = 4
KS = 2 * T
NK = WIDTH // KS
NEG = LOCAL // EG
EB = 8
NHB = LOCAL // EB
NF = FF // T
GROUP = 256
NS = 13
A_STEPS = NK * NEG
B_STEPS = NCH * NHB
SH_IN = A_STEPS + B_STEPS
SH_OUT = SH_IN + 1
STEPS = SH_OUT + 1
LAG2 = 3


def dot(a, b):
    return jnp.dot(a, b, preferred_element_type=F32)


def tdot(a, b):
    return lax.dot_general(a, b, (((0,), (0,)), ((), ())), preferred_element_type=F32)


def bdot(a, b):
    return lax.dot_general(a, b, (((2,), (1,)), ((0,), (0,))), preferred_element_type=F32)


def kernel(x_ref, ids_ref, gates_ref, win_ref, wout_ref, wpair_ref, sin_ref, sout_ref, o_ref,
           tok, mids, mgates, ring, xs, hacc, hid, hid3, osc, disp, comb, comb3, ypart, r0, r1, r2, hs, shy,
           ld_sem, rts, rtr, g1s, g1r, g2s, g2r, gds, gdr, w_sem, t0s, t0r, t1s, t1r, t2s, fin):
    my_dp = lax.axis_index('dp')
    my_ep = lax.axis_index('ep')
    my_x = my_ep // 2
    my_c = my_ep % 2
    my_pos = my_c * 4 + my_dp * 2 + my_x
    partner = (my_dp, my_x * 2 + (1 - my_c))
    x_nbr = (my_dp, (1 - my_x) * 2 + my_c)
    y_nbr = (1 - my_dp, my_ep)
    e_off = my_dp * LOCAL

    def wait_all(ref, sem):
        pltpu.make_async_copy(ref, ref, sem).wait()

    def w_copies(s):
        slot = s % NS
        if s == SH_OUT:
            return [pltpu.make_async_copy(
                sout_ref.at[:, :, pl.ds(c * T, T)], ring.at[slot, :, c // 2, c % 2], w_sem.at[slot]) for c in range(NCH)]
        copies = []
        for n in range(NF):
            if s < A_STEPS:
                k, eg = divmod(s, NEG)
                src = win_ref.at[pl.ds(e_off + eg * EG, EG), pl.ds(2 * k, 2), :, pl.ds(n * T, T)]
            elif s < SH_IN:
                c, h = divmod(s - A_STEPS, NHB)
                if n < 2:
                    src = wout_ref.at[pl.ds(e_off + h * EB + n * EG, EG), pl.ds(0, 2), :, pl.ds(c * T, T)]
                else:
                    src = wpair_ref.at[pl.ds(e_off // 2 + h * EG, EG), :, 2, :, pl.ds(c * T, T)]
            else:
                src = sin_ref.at[:, :, :, pl.ds(n * T, T)]
            copies.append(pltpu.make_async_copy(src, ring.at[slot, n], w_sem.at[slot]))
        return copies

    def w_start(s):
        if s < STEPS:
            for copy in w_copies(s):
                copy.start()

    def w_wait(s):
        wait_all(ring.at[s % NS], w_sem.at[s % NS])

    IDS, GATES = NCH, NCH + 1

    def over_y(i):
        return i % 2 == 1

    def own_core(i):
        return tok.at[i, my_c]

    def own_pair(i):
        return tok.at[i, my_c, my_x if over_y(i) else my_dp]

    def own(i):
        if i == IDS:
            return mids.at[my_pos]
        if i == GATES:
            return mgates.at[my_pos]
        return tok.at[i, my_c, my_x, my_dp] if over_y(i) else tok.at[i, my_c, my_dp, my_x]

    def load(i):
        src = ids_ref if i == IDS else gates_ref if i == GATES else x_ref.at[:, pl.ds(i * T, T)]
        return pltpu.make_async_copy(src, own(i), ld_sem.at[max(0, i - NCH + 1)])

    def remote(src, dst, ssem, rsem, dev):
        return pltpu.make_async_remote_copy(
            src_ref=src, dst_ref=dst, send_sem=ssem, recv_sem=rsem, device_id=dev, device_id_type=MESH)

    def gather1(i):
        return remote(own(i), own(i), g1s, g1r.at[i // 2], y_nbr if over_y(i) else x_nbr)

    def gather2(i):
        return remote(own_pair(i), own_pair(i), g2s, g2r.at[i // 2], x_nbr if over_y(i) else y_nbr)

    def gatherd(i):
        return remote(own_core(i), own_core(i), gds, gdr.at[i // 2], partner)

    routing = [IDS, GATES]
    items = routing + list(range(NCH))

    def peer(r):
        dp = 1 - my_dp if r & 1 else my_dp
        x = 1 - my_x if r & 2 else my_x
        c = 1 - my_c if r & 4 else my_c
        return dp, x * 2 + c

    def tell(i, r):
        return remote(own(i), own(i), rts.at[i - NCH], rtr.at[i - NCH], peer(r))

    barrier = pltpu.get_barrier_semaphore()
    for r in range(1, 8):
        pl.semaphore_signal(barrier, inc=1, device_id=peer(r), device_id_type=MESH)
    for i in items:
        load(i).start()
    hid3[...] = jnp.zeros_like(hid3)
    wait_all(tok.at[0], ld_sem.at[0])
    for i in routing:
        load(i).wait()
    for s in range(NS):
        w_start(s)
    pl.semaphore_wait(barrier, 7)

    def direct(i, r):
        return remote(own(i), own(i), g1s, g2r.at[0], peer(r))

    def send(p):
        for i in (2 * p, 2 * p + 1):
            gather1(i).start()

    def send_on(p):
        wait_all(tok.at[2 * p, 0, 0], g1r.at[p])
        for i in (2 * p, 2 * p + 1):
            gather2(i).start()

    def share(p):
        wait_all(tok.at[pl.ds(0, 3), 0, 0] if p == 0 else tok.at[2 * p, 0], g2r.at[p])
        for i in (2 * p, 2 * p + 1):
            gatherd(i).start()

    for r in (3, 7, 1, 2, 5, 6, 4):
        for i in routing:
            tell(i, r).start()
    for r in (3, 2, 1):
        for i in (0, 1):
            direct(i, r).start()
    send(1)
    wait_all(mids.at[pl.ds(0, 7)], rtr.at[0])
    wait_all(mgates.at[pl.ds(0, 7)], rtr.at[1])

    e_id = lax.broadcasted_iota(jnp.int32, (LOCAL, GROUP), 0) + (my_ep * (2 * LOCAL) + e_off)
    s_id = lax.broadcasted_iota(jnp.int32, (LOCAL, CAP, GROUP), 1).astype(F32)

    def true_pos(t):
        return ((t // 64) % 2) * 128 + (t // 128) * 64 + t % 64

    t_row = lax.broadcasted_iota(jnp.int32, (GROUP, GROUP), 0)
    t_col = lax.broadcasted_iota(jnp.int32, (GROUP, GROUP), 1)
    before = jnp.where(true_pos(t_row) < true_pos(t_col), 1.0, 0.0).astype(BF16)
    eye = jnp.where(t_row == t_col, 1.0, 0.0).astype(BF16)
    for g in range(2):
        ids = jnp.concatenate([mids[c * 4 + g * 2 + x] for c in range(2) for x in range(2)], axis=1)
        gates = jnp.concatenate([mgates[c * 4 + g * 2 + x] for c in range(2) for x in range(2)], axis=1)
        chosen = jnp.zeros((LOCAL, GROUP), F32)
        gate = jnp.zeros((LOCAL, GROUP), F32)
        for j in range(TOPK):
            hit = ids[j:j + 1, :] == e_id
            chosen = jnp.where(hit, 1.0, chosen)
            gate = jnp.where(hit, gates[j:j + 1, :], gate)
        slot = dot(chosen.astype(BF16), before)
        slot = jnp.where(chosen > 0.0, slot, -1.0)
        here = slot[:, None, :] == s_id
        disp[g] = jnp.where(here, 1.0, 0.0).reshape(LOCAL * CAP, GROUP).astype(BF16)
        weight = jnp.where(here, gate[:, None, :], 0.0).reshape(LOCAL * CAP, GROUP)
        for piece in range(3):
            part = weight.astype(BF16)
            turned = tdot(part, eye).astype(BF16)
            if piece < 2:
                comb[g, :, pl.ds(piece * GROUP, GROUP)] = turned
            else:
                comb3[g] = turned
            weight = weight - part.astype(F32)

    send(2)
    send(3)
    send_on(1)
    share(0)
    for k in range(NK):
        wait_all(tok.at[2 * k], gdr.at[k])
        for h in range(2):
            i = 2 * k + h
            for g in range(2):
                rows = tok[i, :, :, g] if over_y(i) else tok[i, :, g]
                picked = dot(disp[g], rows.reshape(GROUP, T)).astype(BF16)
                xs[:, pl.ds(g * CAP, CAP), pl.ds(h * T, T)] = picked.reshape(LOCAL, CAP, T)
        for half in range(2):
            steps = [k * NEG + half * 2 + q for q in range(2)]
            for s in steps:
                w_wait(s)
            for s in steps:
                eg = s % NEG
                batch = pl.ds(eg * EG, EG)
                for n in range(NF):
                    cols = pl.ds(n * T, T)
                    acc = bdot(xs[batch], ring[s % NS, n].reshape(EG, KS, T))
                    if k > 0:
                        acc = acc + hacc[batch, :, cols]
                    if k < NK - 1:
                        hacc[batch, :, cols] = acc
                        continue
                    act = jax.nn.gelu(acc).astype(BF16)
                    if n < 2:
                        hid[batch, :, cols] = act
                    else:
                        act = act.reshape(EG // 2, 2, 2 * CAP, T)
                        for m in range(2):
                            hid3[pl.ds(eg * EG // 2, EG // 2), pl.ds(m * 2 * CAP, 2 * CAP), pl.ds(m * T, T)] = act[:, m]
            for s in steps:
                w_start(s + NS)
            if half == 0 and k < NK - 1:
                if k == 0:
                    send_on(2)
                    send_on(3)
                share(k + 1)

    def route(d):
        if d == 0:
            return my_x, my_dp, x_nbr, y_nbr
        return my_dp, my_x, y_nbr, x_nbr

    def reduce0(c):
        return remote(ypart.at[c, 1 - my_c], r0.at[c], t0s, t0r.at[c], partner)

    def reduce1(c, d, last):
        a, b, dev, _ = route(d)
        side = b if last else 1 - b
        return remote(ypart.at[c, my_c, d, 1 - a, side], r1.at[c, d, side], t1s, fin.at[c] if last else t1r.at[c], dev)

    def reduce2(c, d):
        a, b, _, dev = route(d)
        return remote(ypart.at[c, my_c, d, a, 1 - b], r2.at[c, d], t2s, fin.at[c], dev)

    def stage1(c):
        reduce0(c).wait_recv()
        for last in range(2):
            for d in range(2):
                a, b, _, _ = route(d)
                side = b if last else 1 - b
                ypart[c, my_c, d, 1 - a, side] = ypart[c, my_c, d, 1 - a, side] + r0[c, d, 1 - a, side]
        for last in range(2):
            for d in range(2):
                reduce1(c, d, last).start()
        for d in range(2):
            a, _, _, _ = route(d)
            ypart[c, my_c, d, a] = ypart[c, my_c, d, a] + r0[c, d, a]

    def stage2(c):
        wait_all(r1.at[c, 0], t1r.at[c])
        for d in range(2):
            a, b, _, _ = route(d)
            ypart[c, my_c, d, a, 1 - b] = ypart[c, my_c, d, a, 1 - b] + r1[c, d, 1 - b]
        for d in range(2):
            reduce2(c, d).start()

    def final(c):
        wait_all(r0.at[c, 0], fin.at[c])
        for d in range(2):
            a, b, _, _ = route(d)
            moe = ypart[c, my_c, d, a, b] + r1[c, d, b] + r2[c, d]
            x_own = own(c)[:, pl.ds(d * H, H)].astype(F32)
            shared = shy[:, pl.ds(c * T + d * H, H)].astype(F32)
            o_ref[:, pl.ds(c * T + d * H, H)] = (x_own + shared + moe).astype(BF16)

    for c in range(NCH):
        for h in range(NHB):
            s = A_STEPS + c * NHB + h
            w_wait(s)
            third = bdot(hid3[pl.ds(h * EG, EG)], ring[s % NS, 2].reshape(EG, 2 * T, T)).reshape(EB, 2 * CAP, T)
            for q in range(2):
                first = h * EB + q * EG
                out = bdot(hid[pl.ds(first, EG)], ring[s % NS, q].reshape(EG, 2 * T, T))
                out = (out + third[q * EG:(q + 1) * EG]).astype(BF16)
                for g in range(2):
                    for copy in range(2):
                        osc[g, copy, pl.ds(first, EG)] = out[:, g * CAP:(g + 1) * CAP]
            w_start(s + NS)
        if c >= 1:
            stage1(c - 1)
        for g in range(2):
            y = dot(comb[g], osc[g].reshape(2 * GROUP, T)) + dot(comb3[g], osc[g, 0].reshape(GROUP, T))
            y = y.reshape(2, 2, ROWS, T)
            for core in range(2):
                for x in range(2):
                    ypart[c, core, 0, x, g] = y[core, x, :, :H]
                    ypart[c, core, 1, g, x] = y[core, x, :, H:]
        reduce0(c).start()
        if c >= LAG2:
            stage2(c - LAG2)

    w_wait(SH_IN)
    for n in range(NF):
        acc = jnp.zeros((ROWS, T), F32)
        weights = ring[SH_IN % NS, n].reshape(NCH, T, T)
        for k in range(NCH):
            acc = acc + dot(own(k)[...], weights[k])
        hs[:, pl.ds(n * T, T)] = jax.nn.gelu(acc).astype(BF16)
    stage1(NCH - 1)
    stage2(NCH - 3)
    w_wait(SH_OUT)
    for c in range(NCH):
        acc = jnp.zeros((ROWS, T), F32)
        for j in range(NF):
            acc = acc + dot(hs[:, pl.ds(j * T, T)], ring[SH_OUT % NS, j, c // 2, c % 2])
        shy[:, pl.ds(c * T, T)] = acc.astype(BF16)
    stage2(NCH - 2)
    stage2(NCH - 1)
    for c in range(NCH):
        final(c)
    wait_all(mids.at[pl.ds(0, 7)], rts.at[0])
    wait_all(mgates.at[pl.ds(0, 7)], rts.at[1])
    wait_all(tok.at[pl.ds(0, 3), 0], g1s)
    wait_all(tok.at[pl.ds(0, 3), 0], g2s)
    wait_all(tok.at[pl.ds(0, 4)], gds)
    wait_all(r0, t0s)
    wait_all(r1, t1s)
    wait_all(r2, t2s)


def solution(mesh):
    def layer(tok_x, route_ids, route_gate, w_in, w_out, shared_in, shared_out):
        local = w_in.shape[0]
        any_space = pl.BlockSpec(memory_space=pl.ANY)
        dma = pltpu.SemaphoreType.DMA
        vmem = pltpu.VMEM
        return pl.pallas_call(
            kernel,
            out_shape=pltpu.VMEM((ROWS, WIDTH), BF16),
            in_specs=[any_space] * 8,
            out_specs=pl.BlockSpec(memory_space=pltpu.VMEM),
            scratch_shapes=[
                vmem((NCH, 2, 2, 2, ROWS, T), BF16),
                vmem((8, TOPK, ROWS), jnp.int32),
                vmem((8, TOPK, ROWS), F32),
                vmem((NS, NF, EG, 2, T, T), BF16),
                vmem((LOCAL, 2 * CAP, KS), BF16),
                vmem((LOCAL, 2 * CAP, FF), F32),
                vmem((LOCAL, 2 * CAP, 2 * T), BF16),
                vmem((LOCAL // 2, 4 * CAP, 2 * T), BF16),
                vmem((2, 2, LOCAL, CAP, T), BF16),
                vmem((2, LOCAL * CAP, GROUP), BF16),
                vmem((2, GROUP, 2 * GROUP), BF16),
                vmem((2, GROUP, GROUP), BF16),
                vmem((NCH, 2, 2, 2, 2, ROWS, H), F32),
                vmem((NCH, 2, 2, 2, ROWS, H), F32),
                vmem((NCH, 2, 2, ROWS, H), F32),
                vmem((NCH, 2, ROWS, H), F32),
                vmem((ROWS, FF), BF16),
                vmem((ROWS, WIDTH), BF16),
                dma((3,)), dma((2,)), dma((2,)),
                dma, dma((NK,)), dma, dma((NK,)), dma, dma((NK,)),
                dma((NS,)),
                dma, dma((NCH,)), dma, dma((NCH,)), dma, dma((NCH,)),
            ],
            compiler_params=pltpu.CompilerParams(
                collective_id=0, has_side_effects=True, vmem_limit_bytes=61_000_000),
            name='moe_layer',
        )(tok_x, route_ids.T, route_gate.T,
          w_in.reshape(local, WIDTH // T, T, FF), w_out.reshape(local, NF, T, WIDTH),
          w_out.reshape(local // 2, 2, NF, T, WIDTH),
          shared_in.reshape(EG, 2, T, FF), shared_out.reshape(NF, T, WIDTH))

    row_spec = P(('dp', 'ep'), None)
    expert_spec = P('ep', None, None)
    whole_spec = P(None, None)
    return jax.shard_map(layer, mesh=mesh,
                         in_specs=(row_spec, row_spec, row_spec, expert_spec, expert_spec, whole_spec, whole_spec),
                         out_specs=row_spec, check_vma=False)
```

```python
import jax
import jax.numpy as jnp
from jax import lax
from jax.experimental import pallas as pl
from jax.experimental.pallas import tpu as pltpu
from jax.sharding import PartitionSpec as P

F32 = jnp.float32
BF16 = jnp.bfloat16
MESH = pl.DeviceIdType.MESH

ROWS = 64
WIDTH = 2048
FF = 768
TOPK = 8
LOCAL = 16
CAP = 16
H = 128
T = 256
NCH = WIDTH // T
EG = 4
KS = 2 * T
NK = WIDTH // KS
NEG = LOCAL // EG
EB = 8
NHB = LOCAL // EB
NF = FF // T
GROUP = 256
NS = 12
A_STEPS = NK * NEG
SLOT_IN = (A_STEPS + 4) % NS
SLOT_OUT = SLOT_IN + 1
LAG2 = 3


def dot(a, b):
    return jnp.dot(a, b, preferred_element_type=F32)


def tdot(a, b):
    return lax.dot_general(a, b, (((0,), (0,)), ((), ())), preferred_element_type=F32)


def bdot(a, b):
    return lax.dot_general(a, b, (((2,), (1,)), ((0,), (0,))), preferred_element_type=F32)


def kernel(x_ref, ids_ref, gates_ref, win_ref, wout_ref, wpair_ref, sin_ref, sout_ref, o_ref,
           tok, mids, mgates, ring, xs, hacc, hid, hid3, osc, disp, comb, comb3, ypart, r0, r1, r2, hs, shy,
           ld_sem, rts, rtr, g1s, g1r, g2s, g2r, gds, gdr, w_sem, t0s, t0r, t1s, t1r, t2s, fin):
    my_dp = lax.axis_index('dp')
    my_ep = lax.axis_index('ep')
    my_x = my_ep // 2
    my_c = my_ep % 2
    my_pos = my_c * 4 + my_dp * 2 + my_x
    partner = (my_dp, my_x * 2 + (1 - my_c))
    x_nbr = (my_dp, (1 - my_x) * 2 + my_c)
    y_nbr = (1 - my_dp, my_ep)
    e_off = my_dp * LOCAL

    def wait_all(ref, sem):
        pltpu.make_async_copy(ref, ref, sem).wait()

    def start_all(slot, sources):
        for n, src in enumerate(sources):
            pltpu.make_async_copy(src, ring.at[slot, n], w_sem.at[slot]).start()

    def start_a(slot, k, eg):
        rows = pl.ds(e_off + eg * EG, EG)
        start_all(slot, [win_ref.at[rows, pl.ds(2 * k, 2), :, pl.ds(n * T, T)] for n in range(NF)])

    def start_b(slot, c, h):
        cols = pl.ds(pl.multiple_of(c * T, T), T)
        start_all(slot, [wout_ref.at[pl.ds(e_off + h * EB + n * EG, EG), pl.ds(0, 2), :, cols] for n in range(2)]
                  + [wpair_ref.at[pl.ds(e_off // 2 + h * EG, EG), :, 2, :, cols]])

    def start_in(slot):
        start_all(slot, [sin_ref.at[:, :, :, pl.ds(n * T, T)] for n in range(NF)])

    def start_out(slot):
        for c in range(NCH):
            pltpu.make_async_copy(
                sout_ref.at[:, :, pl.ds(c * T, T)], ring.at[slot, :, c // 2, c % 2], w_sem.at[slot]).start()

    def w_wait(slot):
        wait_all(ring.at[slot], w_sem.at[slot])

    IDS, GATES = NCH, NCH + 1

    def over_y(i):
        return i % 2 == 1

    def own_core(i):
        return tok.at[i, my_c]

    def own_pair(i):
        return tok.at[i, my_c, my_x if over_y(i) else my_dp]

    def own(i):
        if i == IDS:
            return mids.at[my_pos]
        if i == GATES:
            return mgates.at[my_pos]
        return tok.at[i, my_c, my_x, my_dp] if over_y(i) else tok.at[i, my_c, my_dp, my_x]

    def load(i):
        src = ids_ref if i == IDS else gates_ref if i == GATES else x_ref.at[:, pl.ds(i * T, T)]
        return pltpu.make_async_copy(src, own(i), ld_sem.at[max(0, i - NCH + 1)])

    def remote(src, dst, ssem, rsem, dev):
        return pltpu.make_async_remote_copy(
            src_ref=src, dst_ref=dst, send_sem=ssem, recv_sem=rsem, device_id=dev, device_id_type=MESH)

    def gather1(i):
        return remote(own(i), own(i), g1s, g1r.at[i // 2], y_nbr if over_y(i) else x_nbr)

    def gather2(i):
        return remote(own_pair(i), own_pair(i), g2s, g2r.at[i // 2], x_nbr if over_y(i) else y_nbr)

    def gatherd(i):
        return remote(own_core(i), own_core(i), gds, gdr.at[i // 2], partner)

    routing = [IDS, GATES]
    items = routing + list(range(NCH))

    def peer(r):
        dp = 1 - my_dp if r & 1 else my_dp
        x = 1 - my_x if r & 2 else my_x
        c = 1 - my_c if r & 4 else my_c
        return dp, x * 2 + c

    def tell(i, r):
        return remote(own(i), own(i), rts.at[i - NCH], rtr.at[i - NCH], peer(r))

    barrier = pltpu.get_barrier_semaphore()
    for r in range(1, 8):
        pl.semaphore_signal(barrier, inc=1, device_id=peer(r), device_id_type=MESH)
    for i in items:
        load(i).start()
    hid3[...] = jnp.zeros_like(hid3)
    hacc[...] = jnp.zeros_like(hacc)
    wait_all(tok.at[0], ld_sem.at[0])
    for i in routing:
        load(i).wait()
    for s in range(NS):
        start_a(s, s // NEG, s % NEG)
    pl.semaphore_wait(barrier, 7)

    def direct(i, r):
        return remote(own(i), own(i), g1s, g2r.at[0], peer(r))

    def send(p):
        for i in (2 * p, 2 * p + 1):
            gather1(i).start()

    def send_on(p):
        wait_all(tok.at[2 * p, 0, 0], g1r.at[p])
        for i in (2 * p, 2 * p + 1):
            gather2(i).start()

    def share(p):
        wait_all(tok.at[pl.ds(0, 3), 0, 0] if p == 0 else tok.at[2 * p, 0], g2r.at[p])
        for i in (2 * p, 2 * p + 1):
            gatherd(i).start()

    for r in (3, 7, 1, 2, 5, 6, 4):
        for i in routing:
            tell(i, r).start()
    for r in (3, 2, 1):
        for i in (0, 1):
            direct(i, r).start()
    send(1)
    wait_all(mids.at[pl.ds(0, 7)], rtr.at[0])
    wait_all(mgates.at[pl.ds(0, 7)], rtr.at[1])

    e_id = lax.broadcasted_iota(jnp.int32, (LOCAL, GROUP), 0) + (my_ep * (2 * LOCAL) + e_off)
    s_id = lax.broadcasted_iota(jnp.int32, (LOCAL, CAP, GROUP), 1).astype(F32)

    def true_pos(t):
        return ((t // 64) % 2) * 128 + (t // 128) * 64 + t % 64

    t_row = lax.broadcasted_iota(jnp.int32, (GROUP, GROUP), 0)
    t_col = lax.broadcasted_iota(jnp.int32, (GROUP, GROUP), 1)
    before = jnp.where(true_pos(t_row) < true_pos(t_col), 1.0, 0.0).astype(BF16)
    eye = jnp.where(t_row == t_col, 1.0, 0.0).astype(BF16)
    for g in range(2):
        ids = jnp.concatenate([mids[c * 4 + g * 2 + x] for c in range(2) for x in range(2)], axis=1)
        gates = jnp.concatenate([mgates[c * 4 + g * 2 + x] for c in range(2) for x in range(2)], axis=1)
        chosen = jnp.zeros((LOCAL, GROUP), F32)
        gate = jnp.zeros((LOCAL, GROUP), F32)
        for j in range(TOPK):
            hit = ids[j:j + 1, :] == e_id
            chosen = jnp.where(hit, 1.0, chosen)
            gate = jnp.where(hit, gates[j:j + 1, :], gate)
        slot = dot(chosen.astype(BF16), before)
        slot = jnp.where(chosen > 0.0, slot, -1.0)
        here = slot[:, None, :] == s_id
        disp[g] = jnp.where(here, 1.0, 0.0).reshape(LOCAL * CAP, GROUP).astype(BF16)
        weight = jnp.where(here, gate[:, None, :], 0.0).reshape(LOCAL * CAP, GROUP)
        for piece in range(3):
            part = weight.astype(BF16)
            turned = tdot(part, eye).astype(BF16)
            if piece < 2:
                comb[g, :, pl.ds(piece * GROUP, GROUP)] = turned
            else:
                comb3[g] = turned
            weight = weight - part.astype(F32)

    send(2)
    send(3)
    send_on(1)
    share(0)

    def pick(k):
        wait_all(tok.at[2 * k], gdr.at[k])
        for h in range(2):
            for g in range(2):
                rows = tok[2 * k + h, :, :, g] if h else tok[2 * k + h, :, g]
                picked = dot(disp[g], rows.reshape(GROUP, T)).astype(BF16)
                xs[:, pl.ds(g * CAP, CAP), pl.ds(h * T, T)] = picked.reshape(LOCAL, CAP, T)

    def first_product(t, slots, last):
        for slot in slots:
            w_wait(slot)
        for q, slot in enumerate(slots):
            eg = 2 * lax.rem(t, 2) + q if not last else 2 * (t % 2) + q
            batch = pl.ds(eg * EG, EG)
            for n in range(NF):
                cols = pl.ds(n * T, T)
                acc = bdot(xs[batch], ring[slot, n].reshape(EG, KS, T)) + hacc[batch, :, cols]
                if not last:
                    hacc[batch, :, cols] = acc
                    continue
                act = jax.nn.gelu(acc).astype(BF16)
                if n < 2:
                    hid[batch, :, cols] = act
                else:
                    act = act.reshape(EG // 2, 2, 2 * CAP, T)
                    for m in range(2):
                        hid3[pl.ds(eg * EG // 2, EG // 2), pl.ds(m * 2 * CAP, 2 * CAP), pl.ds(m * T, T)] = act[:, m]

    def k_step(k, carry):
        pick(k)

        def half_step(half, carry):
            t = 2 * k + half
            first_product(t, [2 * t, 2 * t + 1], False)

            @pl.when(t < 2)
            def _():
                for q in range(2):
                    start_a(2 * t + q, NK - 1, 2 * t + q)

            @pl.when(t >= 2)
            def _():
                for q in range(2):
                    start_b(2 * t + q, t - 2, q)

            @pl.when(t == 0)
            def _():
                send_on(2)
                send_on(3)

            for p in range(1, NK):
                @pl.when(t == 2 * p - 2)
                def _():
                    share(p)

            return carry

        return lax.fori_loop(0, 2, half_step, carry)

    lax.fori_loop(0, NK - 1, k_step, 0)
    pick(NK - 1)
    for t in (2 * NK - 2, 2 * NK - 1):
        slots = [2 * t - NS, 2 * t + 1 - NS]
        first_product(t, slots, True)
        for q in range(2):
            start_b(slots[q], t - 2, q)

    def route(d):
        if d == 0:
            return my_x, my_dp, x_nbr, y_nbr
        return my_dp, my_x, y_nbr, x_nbr

    def reduce0(c):
        return remote(ypart.at[c, 1 - my_c], r0.at[c], t0s, t0r.at[c], partner)

    def reduce1(c, d, last):
        a, b, dev, _ = route(d)
        side = b if last else 1 - b
        return remote(ypart.at[c, my_c, d, 1 - a, side], r1.at[c, d, side], t1s, fin.at[c] if last else t1r.at[c], dev)

    def reduce2(c, d):
        a, b, _, dev = route(d)
        return remote(ypart.at[c, my_c, d, a, 1 - b], r2.at[c, d], t2s, fin.at[c], dev)

    def stage1(c):
        reduce0(c).wait_recv()
        for last in range(2):
            for d in range(2):
                a, b, _, _ = route(d)
                side = b if last else 1 - b
                ypart[c, my_c, d, 1 - a, side] = ypart[c, my_c, d, 1 - a, side] + r0[c, d, 1 - a, side]
        for last in range(2):
            for d in range(2):
                reduce1(c, d, last).start()
        for d in range(2):
            a, _, _, _ = route(d)
            ypart[c, my_c, d, a] = ypart[c, my_c, d, a] + r0[c, d, a]

    def stage2(c):
        wait_all(r1.at[c, 0], t1r.at[c])
        for d in range(2):
            a, b, _, _ = route(d)
            ypart[c, my_c, d, a, 1 - b] = ypart[c, my_c, d, a, 1 - b] + r1[c, d, 1 - b]
        for d in range(2):
            reduce2(c, d).start()

    def final(c):
        wait_all(r0.at[c, 0], fin.at[c])
        for d in range(2):
            a, b, _, _ = route(d)
            moe = ypart[c, my_c, d, a, b] + r1[c, d, b] + r2[c, d]
            x_own = own(c)[:, pl.ds(d * H, H)].astype(F32)
            shared = shy[:, pl.ds(c * T + d * H, H)].astype(F32)
            o_ref[:, pl.ds(c * T + d * H, H)] = (x_own + shared + moe).astype(BF16)

    def chunk(c, carry):
        base = lax.rem(2 * c + A_STEPS, NS)
        for h in range(NHB):
            slot = base + h
            w_wait(slot)
            third = bdot(hid3[pl.ds(h * EG, EG)], ring[slot, 2].reshape(EG, 2 * T, T)).reshape(EB, 2 * CAP, T)
            for q in range(2):
                first = h * EB + q * EG
                out = bdot(hid[pl.ds(first, EG)], ring[slot, q].reshape(EG, 2 * T, T))
                out = (out + third[q * EG:(q + 1) * EG]).astype(BF16)
                for g in range(2):
                    for copy in range(2):
                        osc[g, copy, pl.ds(first, EG)] = out[:, g * CAP:(g + 1) * CAP]

            @pl.when(c < 2)
            def _():
                start_b(slot, c + 6, h)

            @pl.when(c == 2)
            def _():
                if h == 0:
                    start_in(SLOT_IN)
                else:
                    start_out(SLOT_OUT)

        @pl.when(c >= 1)
        def _():
            stage1(c - 1)

        for g in range(2):
            y = dot(comb[g], osc[g].reshape(2 * GROUP, T)) + dot(comb3[g], osc[g, 0].reshape(GROUP, T))
            y = y.reshape(2, 2, ROWS, T)
            for core in range(2):
                for x in range(2):
                    ypart[c, core, 0, x, g] = y[core, x, :, :H]
                    ypart[c, core, 1, g, x] = y[core, x, :, H:]
        reduce0(c).start()

        @pl.when(c >= LAG2)
        def _():
            stage2(c - LAG2)

        return carry

    lax.fori_loop(0, NCH, chunk, 0)

    w_wait(SLOT_IN)
    for n in range(NF):
        acc = jnp.zeros((ROWS, T), F32)
        weights = ring[SLOT_IN, n].reshape(NCH, T, T)
        for k in range(NCH):
            acc = acc + dot(own(k)[...], weights[k])
        hs[:, pl.ds(n * T, T)] = jax.nn.gelu(acc).astype(BF16)
    stage1(NCH - 1)
    stage2(NCH - 3)
    w_wait(SLOT_OUT)
    for c in range(NCH):
        acc = jnp.zeros((ROWS, T), F32)
        for j in range(NF):
            acc = acc + dot(hs[:, pl.ds(j * T, T)], ring[SLOT_OUT, j, c // 2, c % 2])
        shy[:, pl.ds(c * T, T)] = acc.astype(BF16)
    stage2(NCH - 2)
    stage2(NCH - 1)
    for c in range(NCH):
        final(c)
    wait_all(mids.at[pl.ds(0, 7)], rts.at[0])
    wait_all(mgates.at[pl.ds(0, 7)], rts.at[1])
    wait_all(tok.at[pl.ds(0, 3), 0], g1s)
    wait_all(tok.at[pl.ds(0, 3), 0], g2s)
    wait_all(tok.at[pl.ds(0, 4)], gds)
    wait_all(r0, t0s)
    wait_all(r1, t1s)
    wait_all(r2, t2s)


def solution(mesh):
    def layer(tok_x, route_ids, route_gate, w_in, w_out, shared_in, shared_out):
        local = w_in.shape[0]
        any_space = pl.BlockSpec(memory_space=pl.ANY)
        dma = pltpu.SemaphoreType.DMA
        vmem = pltpu.VMEM
        return pl.pallas_call(
            kernel,
            out_shape=pltpu.VMEM((ROWS, WIDTH), BF16),
            in_specs=[any_space] * 8,
            out_specs=pl.BlockSpec(memory_space=pltpu.VMEM),
            scratch_shapes=[
                vmem((NCH, 2, 2, 2, ROWS, T), BF16),
                vmem((8, TOPK, ROWS), jnp.int32),
                vmem((8, TOPK, ROWS), F32),
                vmem((NS, NF, EG, 2, T, T), BF16),
                vmem((LOCAL, 2 * CAP, KS), BF16),
                vmem((LOCAL, 2 * CAP, FF), F32),
                vmem((LOCAL, 2 * CAP, 2 * T), BF16),
                vmem((LOCAL // 2, 4 * CAP, 2 * T), BF16),
                vmem((2, 2, LOCAL, CAP, T), BF16),
                vmem((2, LOCAL * CAP, GROUP), BF16),
                vmem((2, GROUP, 2 * GROUP), BF16),
                vmem((2, GROUP, GROUP), BF16),
                vmem((NCH, 2, 2, 2, 2, ROWS, H), F32),
                vmem((NCH, 2, 2, 2, ROWS, H), F32),
                vmem((NCH, 2, 2, ROWS, H), F32),
                vmem((NCH, 2, ROWS, H), F32),
                vmem((ROWS, FF), BF16),
                vmem((ROWS, WIDTH), BF16),
                dma((3,)), dma((2,)), dma((2,)),
                dma, dma((NK,)), dma, dma((NK,)), dma, dma((NK,)),
                dma((NS,)),
                dma, dma((NCH,)), dma, dma((NCH,)), dma, dma((NCH,)),
            ],
            compiler_params=pltpu.CompilerParams(
                collective_id=0, has_side_effects=True, vmem_limit_bytes=58_000_000),
            name='moe_layer',
        )(tok_x, route_ids.T, route_gate.T,
          w_in.reshape(local, WIDTH // T, T, FF), w_out.reshape(local, NF, T, WIDTH),
          w_out.reshape(local // 2, 2, NF, T, WIDTH),
          shared_in.reshape(EG, 2, T, FF), shared_out.reshape(NF, T, WIDTH))

    row_spec = P(('dp', 'ep'), None)
    expert_spec = P('ep', None, None)
    whole_spec = P(None, None)
    return jax.shard_map(layer, mesh=mesh,
                         in_specs=(row_spec, row_spec, row_spec, expert_spec, expert_spec, whole_spec, whole_spec),
                         out_specs=row_spec, check_vma=False)
```

```python
import jax
import jax.numpy as jnp
from jax import lax
from jax.experimental import pallas as pl
from jax.experimental.pallas import tpu as pltpu
from jax.sharding import PartitionSpec as P

F32 = jnp.float32
BF16 = jnp.bfloat16
MESH = pl.DeviceIdType.MESH

ROWS = 64
WIDTH = 2048
FF = 768
TOPK = 8
LOCAL = 16
CAP = 16
H = 128
T = 256
NCH = WIDTH // T
EG = 4
KS = 2 * T
NK = WIDTH // KS
NEG = LOCAL // EG
EB = 8
NHB = LOCAL // EB
NF = FF // T
GROUP = 256
NS = 13
A_STEPS = NK * NEG
B_STEPS = NCH * NHB
SH_IN = A_STEPS + B_STEPS
SH_OUT = SH_IN + 1
STEPS = SH_OUT + 1
LAG2 = 3


def dot(a, b):
    return jnp.dot(a, b, preferred_element_type=F32)


def tdot(a, b):
    return lax.dot_general(a, b, (((0,), (0,)), ((), ())), preferred_element_type=F32)


def bdot(a, b):
    return lax.dot_general(a, b, (((2,), (1,)), ((0,), (0,))), preferred_element_type=F32)


def kernel(x_ref, ids_ref, gates_ref, win_ref, wout_ref, wpair_ref, sin_ref, sout_ref, o_ref,
           tok, mids, mgates, ring, xs, hacc, hid, hid3, osc, disp, comb, comb3, ypart, r0, r1, r2, hs, shy,
           ld_sem, rts, rtr, g1s, g1r, g2s, g2r, gds, gdr, w_sem, t0s, t0r, t1s, t1r, t2s, fin):
    my_dp = lax.axis_index('dp')
    my_ep = lax.axis_index('ep')
    my_x = my_ep // 2
    my_c = my_ep % 2
    my_pos = my_c * 4 + my_dp * 2 + my_x
    partner = (my_dp, my_x * 2 + (1 - my_c))
    x_nbr = (my_dp, (1 - my_x) * 2 + my_c)
    y_nbr = (1 - my_dp, my_ep)
    e_off = my_dp * LOCAL

    def wait_all(ref, sem):
        pltpu.make_async_copy(ref, ref, sem).wait()

    def w_copies(s):
        slot = s % NS
        if s == SH_OUT:
            return [pltpu.make_async_copy(
                sout_ref.at[:, :, pl.ds(c * T, T)], ring.at[slot, :, c // 2, c % 2], w_sem.at[slot]) for c in range(NCH)]
        copies = []
        for n in range(NF):
            if s < A_STEPS:
                k, eg = divmod(s, NEG)
                src = win_ref.at[pl.ds(e_off + eg * EG, EG), pl.ds(2 * k, 2), :, pl.ds(n * T, T)]
            elif s < SH_IN:
                c, h = divmod(s - A_STEPS, NHB)
                if n < 2:
                    src = wout_ref.at[pl.ds(e_off + h * EB + n * EG, EG), pl.ds(0, 2), :, pl.ds(c * T, T)]
                else:
                    src = wpair_ref.at[pl.ds(e_off // 2 + h * EG, EG), :, 2, :, pl.ds(c * T, T)]
            else:
                src = sin_ref.at[:, :, :, pl.ds(n * T, T)]
            copies.append(pltpu.make_async_copy(src, ring.at[slot, n], w_sem.at[slot]))
        return copies

    def w_start(s):
        if s < STEPS:
            for copy in w_copies(s):
                copy.start()

    def w_wait(s):
        wait_all(ring.at[s % NS], w_sem.at[s % NS])

    IDS, GATES = NCH, NCH + 1

    def over_y(i):
        return i % 2 == 1

    def own_core(i):
        return tok.at[i, my_c]

    def own_pair(i):
        return tok.at[i, my_c, my_x if over_y(i) else my_dp]

    def own(i):
        if i == IDS:
            return mids.at[my_pos]
        if i == GATES:
            return mgates.at[my_pos]
        return tok.at[i, my_c, my_x, my_dp] if over_y(i) else tok.at[i, my_c, my_dp, my_x]

    def load(i):
        src = ids_ref if i == IDS else gates_ref if i == GATES else x_ref.at[:, pl.ds(i * T, T)]
        return pltpu.make_async_copy(src, own(i), ld_sem.at[max(0, i - NCH + 1)])

    def remote(src, dst, ssem, rsem, dev):
        return pltpu.make_async_remote_copy(
            src_ref=src, dst_ref=dst, send_sem=ssem, recv_sem=rsem, device_id=dev, device_id_type=MESH)

    def gather1(i):
        return remote(own(i), own(i), g1s, g1r.at[i // 2], y_nbr if over_y(i) else x_nbr)

    def gather2(i):
        return remote(own_pair(i), own_pair(i), g2s, g2r.at[i // 2], x_nbr if over_y(i) else y_nbr)

    def gatherd(i):
        return remote(own_core(i), own_core(i), gds, gdr.at[i // 2], partner)

    routing = [IDS, GATES]
    items = routing + list(range(NCH))

    def peer(r):
        dp = 1 - my_dp if r & 1 else my_dp
        x = 1 - my_x if r & 2 else my_x
        c = 1 - my_c if r & 4 else my_c
        return dp, x * 2 + c

    def tell(i, r):
        return remote(own(i), own(i), rts.at[i - NCH], rtr.at[i - NCH], peer(r))

    barrier = pltpu.get_barrier_semaphore()
    for r in range(1, 8):
        pl.semaphore_signal(barrier, inc=1, device_id=peer(r), device_id_type=MESH)
    for i in items:
        load(i).start()
    hid3[...] = jnp.zeros_like(hid3)
    wait_all(tok.at[0], ld_sem.at[0])
    for i in routing:
        load(i).wait()
    pl.semaphore_wait(barrier, 7)

    def direct(i, r):
        return remote(own(i), own(i), g1s, g2r.at[0], peer(r))

    def send(p):
        for i in (2 * p, 2 * p + 1):
            gather1(i).start()

    def send_on(p):
        wait_all(tok.at[2 * p, 0, 0], g1r.at[p])
        for i in (2 * p, 2 * p + 1):
            gather2(i).start()

    def share(p):
        wait_all(tok.at[pl.ds(0, 3), 0, 0] if p == 0 else tok.at[2 * p, 0], g2r.at[p])
        for i in (2 * p, 2 * p + 1):
            gatherd(i).start()

    for r in (3, 7, 1, 2, 5, 6, 4):
        for i in routing:
            tell(i, r).start()
    for r in (3, 2, 1):
        for i in (0, 1):
            direct(i, r).start()
    for s in range(NS):
        w_start(s)
    send(1)
    wait_all(mids.at[pl.ds(0, 7)], rtr.at[0])
    wait_all(mgates.at[pl.ds(0, 7)], rtr.at[1])

    e_id = lax.broadcasted_iota(jnp.int32, (LOCAL, GROUP), 0) + (my_ep * (2 * LOCAL) + e_off)
    s_id = lax.broadcasted_iota(jnp.int32, (LOCAL, CAP, GROUP), 1).astype(F32)

    def true_pos(t):
        return ((t // 64) % 2) * 128 + (t // 128) * 64 + t % 64

    t_row = lax.broadcasted_iota(jnp.int32, (GROUP, GROUP), 0)
    t_col = lax.broadcasted_iota(jnp.int32, (GROUP, GROUP), 1)
    before = jnp.where(true_pos(t_row) < true_pos(t_col), 1.0, 0.0).astype(BF16)
    eye = jnp.where(t_row == t_col, 1.0, 0.0).astype(BF16)
    for g in range(2):
        ids = jnp.concatenate([mids[c * 4 + g * 2 + x] for c in range(2) for x in range(2)], axis=1)
        gates = jnp.concatenate([mgates[c * 4 + g * 2 + x] for c in range(2) for x in range(2)], axis=1)
        chosen = jnp.zeros((LOCAL, GROUP), F32)
        gate = jnp.zeros((LOCAL, GROUP), F32)
        for j in range(TOPK):
            hit = ids[j:j + 1, :] == e_id
            chosen = jnp.where(hit, 1.0, chosen)
            gate = jnp.where(hit, gates[j:j + 1, :], gate)
        slot = dot(chosen.astype(BF16), before)
        slot = jnp.where(chosen > 0.0, slot, -1.0)
        here = slot[:, None, :] == s_id
        disp[g] = jnp.where(here, 1.0, 0.0).reshape(LOCAL * CAP, GROUP).astype(BF16)
        weight = jnp.where(here, gate[:, None, :], 0.0).reshape(LOCAL * CAP, GROUP)
        for piece in range(3):
            part = weight.astype(BF16)
            turned = tdot(part, eye).astype(BF16)
            if piece < 2:
                comb[g, :, pl.ds(piece * GROUP, GROUP)] = turned
            else:
                comb3[g] = turned
            weight = weight - part.astype(F32)

    send(2)
    send(3)
    send_on(1)
    share(0)
    for k in range(NK):
        wait_all(tok.at[2 * k], gdr.at[k])
        for h in range(2):
            i = 2 * k + h
            for g in range(2):
                rows = tok[i, :, :, g] if over_y(i) else tok[i, :, g]
                picked = dot(disp[g], rows.reshape(GROUP, T)).astype(BF16)
                xs[:, pl.ds(g * CAP, CAP), pl.ds(h * T, T)] = picked.reshape(LOCAL, CAP, T)
        for half in range(2):
            steps = [k * NEG + half * 2 + q for q in range(2)]
            for s in steps:
                w_wait(s)
            for s in steps:
                eg = s % NEG
                batch = pl.ds(eg * EG, EG)
                for n in range(NF):
                    cols = pl.ds(n * T, T)
                    acc = bdot(xs[batch], ring[s % NS, n].reshape(EG, KS, T))
                    if k > 0:
                        acc = acc + hacc[batch, :, cols]
                    if k < NK - 1:
                        hacc[batch, :, cols] = acc
                        continue
                    act = jax.nn.gelu(acc).astype(BF16)
                    if n < 2:
                        hid[batch, :, cols] = act
                    else:
                        act = act.reshape(EG // 2, 2, 2 * CAP, T)
                        for m in range(2):
                            hid3[pl.ds(eg * EG // 2, EG // 2), pl.ds(m * 2 * CAP, 2 * CAP), pl.ds(m * T, T)] = act[:, m]
            for s in steps:
                w_start(s + NS)
            if half == 0 and k < NK - 1:
                if k == 0:
                    send_on(2)
                    send_on(3)
                share(k + 1)

    def route(d):
        if d == 0:
            return my_x, my_dp, x_nbr, y_nbr
        return my_dp, my_x, y_nbr, x_nbr

    def reduce0(c):
        return remote(ypart.at[c, 1 - my_c], r0.at[c], t0s, t0r.at[c], partner)

    def reduce1(c, d, last):
        a, b, dev, _ = route(d)
        side = b if last else 1 - b
        return remote(ypart.at[c, my_c, d, 1 - a, side], r1.at[c, d, side], t1s, fin.at[c] if last else t1r.at[c], dev)

    def reduce2(c, d):
        a, b, _, dev = route(d)
        return remote(ypart.at[c, my_c, d, a, 1 - b], r2.at[c, d], t2s, fin.at[c], dev)

    def stage1(c):
        reduce0(c).wait_recv()
        for last in range(2):
            for d in range(2):
                a, b, _, _ = route(d)
                side = b if last else 1 - b
                ypart[c, my_c, d, 1 - a, side] = ypart[c, my_c, d, 1 - a, side] + r0[c, d, 1 - a, side]
        for last in range(2):
            for d in range(2):
                reduce1(c, d, last).start()
        for d in range(2):
            a, _, _, _ = route(d)
            ypart[c, my_c, d, a] = ypart[c, my_c, d, a] + r0[c, d, a]

    def stage2(c):
        wait_all(r1.at[c, 0], t1r.at[c])
        for d in range(2):
            a, b, _, _ = route(d)
            ypart[c, my_c, d, a, 1 - b] = ypart[c, my_c, d, a, 1 - b] + r1[c, d, 1 - b]
        for d in range(2):
            reduce2(c, d).start()

    def final(c):
        wait_all(r0.at[c, 0], fin.at[c])
        for d in range(2):
            a, b, _, _ = route(d)
            moe = ypart[c, my_c, d, a, b] + r1[c, d, b] + r2[c, d]
            x_own = own(c)[:, pl.ds(d * H, H)].astype(F32)
            shared = shy[:, pl.ds(c * T + d * H, H)].astype(F32)
            o_ref[:, pl.ds(c * T + d * H, H)] = (x_own + shared + moe).astype(BF16)

    for c in range(NCH):
        for h in range(NHB):
            s = A_STEPS + c * NHB + h
            w_wait(s)
            third = bdot(hid3[pl.ds(h * EG, EG)], ring[s % NS, 2].reshape(EG, 2 * T, T)).reshape(EB, 2 * CAP, T)
            for q in range(2):
                first = h * EB + q * EG
                out = bdot(hid[pl.ds(first, EG)], ring[s % NS, q].reshape(EG, 2 * T, T))
                out = (out + third[q * EG:(q + 1) * EG]).astype(BF16)
                for g in range(2):
                    for copy in range(2):
                        osc[g, copy, pl.ds(first, EG)] = out[:, g * CAP:(g + 1) * CAP]
            w_start(s + NS)
        if c >= 1:
            stage1(c - 1)
        if c >= LAG2:
            stage2(c - LAG2)
        for g in range(2):
            y = dot(comb[g], osc[g].reshape(2 * GROUP, T)) + dot(comb3[g], osc[g, 0].reshape(GROUP, T))
            y = y.reshape(2, 2, ROWS, T)
            for core in range(2):
                for x in range(2):
                    ypart[c, core, 0, x, g] = y[core, x, :, :H]
                    ypart[c, core, 1, g, x] = y[core, x, :, H:]
        reduce0(c).start()

    w_wait(SH_IN)
    for n in range(NF):
        acc = jnp.zeros((ROWS, T), F32)
        weights = ring[SH_IN % NS, n].reshape(NCH, T, T)
        for k in range(NCH):
            acc = acc + dot(own(k)[...], weights[k])
        hs[:, pl.ds(n * T, T)] = jax.nn.gelu(acc).astype(BF16)
    stage1(NCH - 1)
    stage2(NCH - 3)
    w_wait(SH_OUT)
    for c in range(NCH):
        acc = jnp.zeros((ROWS, T), F32)
        for j in range(NF):
            acc = acc + dot(hs[:, pl.ds(j * T, T)], ring[SH_OUT % NS, j, c // 2, c % 2])
        shy[:, pl.ds(c * T, T)] = acc.astype(BF16)
    stage2(NCH - 2)
    stage2(NCH - 1)
    for c in range(NCH):
        final(c)
    wait_all(mids.at[pl.ds(0, 7)], rts.at[0])
    wait_all(mgates.at[pl.ds(0, 7)], rts.at[1])
    wait_all(tok.at[pl.ds(0, 3), 0], g1s)
    wait_all(tok.at[pl.ds(0, 3), 0], g2s)
    wait_all(tok.at[pl.ds(0, 4)], gds)
    wait_all(r0, t0s)
    wait_all(r1, t1s)
    wait_all(r2, t2s)


def solution(mesh):
    def layer(tok_x, route_ids, route_gate, w_in, w_out, shared_in, shared_out):
        local = w_in.shape[0]
        any_space = pl.BlockSpec(memory_space=pl.ANY)
        dma = pltpu.SemaphoreType.DMA
        vmem = pltpu.VMEM
        return pl.pallas_call(
            kernel,
            out_shape=pltpu.VMEM((ROWS, WIDTH), BF16),
            in_specs=[any_space] * 8,
            out_specs=pl.BlockSpec(memory_space=pltpu.VMEM),
            scratch_shapes=[
                vmem((NCH, 2, 2, 2, ROWS, T), BF16),
                vmem((8, TOPK, ROWS), jnp.int32),
                vmem((8, TOPK, ROWS), F32),
                vmem((NS, NF, EG, 2, T, T), BF16),
                vmem((LOCAL, 2 * CAP, KS), BF16),
                vmem((LOCAL, 2 * CAP, FF), F32),
                vmem((LOCAL, 2 * CAP, 2 * T), BF16),
                vmem((LOCAL // 2, 4 * CAP, 2 * T), BF16),
                vmem((2, 2, LOCAL, CAP, T), BF16),
                vmem((2, LOCAL * CAP, GROUP), BF16),
                vmem((2, GROUP, 2 * GROUP), BF16),
                vmem((2, GROUP, GROUP), BF16),
                vmem((NCH, 2, 2, 2, 2, ROWS, H), F32),
                vmem((NCH, 2, 2, 2, ROWS, H), F32),
                vmem((NCH, 2, 2, ROWS, H), F32),
                vmem((NCH, 2, ROWS, H), F32),
                vmem((ROWS, FF), BF16),
                vmem((ROWS, WIDTH), BF16),
                dma((3,)), dma((2,)), dma((2,)),
                dma, dma((NK,)), dma, dma((NK,)), dma, dma((NK,)),
                dma((NS,)),
                dma, dma((NCH,)), dma, dma((NCH,)), dma, dma((NCH,)),
            ],
            compiler_params=pltpu.CompilerParams(
                collective_id=0, has_side_effects=True, vmem_limit_bytes=61_000_000),
            name='moe_layer',
        )(tok_x, route_ids.T, route_gate.T,
          w_in.reshape(local, WIDTH // T, T, FF), w_out.reshape(local, NF, T, WIDTH),
          w_out.reshape(local // 2, 2, NF, T, WIDTH),
          shared_in.reshape(EG, 2, T, FF), shared_out.reshape(NF, T, WIDTH))

    row_spec = P(('dp', 'ep'), None)
    expert_spec = P('ep', None, None)
    whole_spec = P(None, None)
    return jax.shard_map(layer, mesh=mesh,
                         in_specs=(row_spec, row_spec, row_spec, expert_spec, expert_spec, whole_spec, whole_spec),
                         out_specs=row_spec, check_vma=False)
```

```python
import jax
import jax.numpy as jnp
from jax import lax
from jax.experimental import pallas as pl
from jax.experimental.pallas import tpu as pltpu
from jax.sharding import PartitionSpec as P

F32 = jnp.float32
BF16 = jnp.bfloat16
MESH = pl.DeviceIdType.MESH

ROWS = 64
WIDTH = 2048
FF = 768
TOPK = 8
LOCAL = 16
CAP = 16
H = 128
T = 256
NCH = WIDTH // T
EG = 4
KS = 2 * T
NK = WIDTH // KS
NEG = LOCAL // EG
EB = 8
NHB = LOCAL // EB
NF = FF // T
GROUP = 256
NS = 13
A_STEPS = NK * NEG
B_STEPS = NCH * NHB
SH_IN = A_STEPS + B_STEPS
SH_OUT = SH_IN + 1
STEPS = SH_OUT + 1
LAG2 = 3


def dot(a, b):
    return jnp.dot(a, b, preferred_element_type=F32)


def tdot(a, b):
    return lax.dot_general(a, b, (((0,), (0,)), ((), ())), preferred_element_type=F32)


def bdot(a, b):
    return lax.dot_general(a, b, (((2,), (1,)), ((0,), (0,))), preferred_element_type=F32)


def kernel(x_ref, ids_ref, gates_ref, win_ref, wout_ref, wpair_ref, sin_ref, sout_ref, o_ref,
           tok, mids, mgates, ring, xs, hacc, hid, hid3, osc, disp, comb, comb3, ypart, r0, r1, r2, hs, shy,
           ld_sem, rts, rtr, g1s, g1r, g2s, g2r, gds, gdr, w_sem, t0s, t0r, t1s, t1r, t2s, fin):
    my_dp = lax.axis_index('dp')
    my_ep = lax.axis_index('ep')
    my_x = my_ep // 2
    my_c = my_ep % 2
    my_pos = my_c * 4 + my_dp * 2 + my_x
    partner = (my_dp, my_x * 2 + (1 - my_c))
    x_nbr = (my_dp, (1 - my_x) * 2 + my_c)
    y_nbr = (1 - my_dp, my_ep)
    e_off = my_dp * LOCAL

    def wait_all(ref, sem):
        pltpu.make_async_copy(ref, ref, sem).wait()

    def w_copies(s):
        slot = s % NS
        if s == SH_OUT:
            return [pltpu.make_async_copy(
                sout_ref.at[:, :, pl.ds(c * T, T)], ring.at[slot, :, c // 2, c % 2], w_sem.at[slot]) for c in range(NCH)]
        copies = []
        for n in range(NF):
            if s < A_STEPS:
                k, eg = divmod(s, NEG)
                src = win_ref.at[pl.ds(e_off + eg * EG, EG), pl.ds(2 * k, 2), :, pl.ds(n * T, T)]
            elif s < SH_IN:
                c, h = divmod(s - A_STEPS, NHB)
                if n < 2:
                    src = wout_ref.at[pl.ds(e_off + h * EB + n * EG, EG), pl.ds(0, 2), :, pl.ds(c * T, T)]
                else:
                    src = wpair_ref.at[pl.ds(e_off // 2 + h * EG, EG), :, 2, :, pl.ds(c * T, T)]
            else:
                src = sin_ref.at[:, :, :, pl.ds(n * T, T)]
            copies.append(pltpu.make_async_copy(src, ring.at[slot, n], w_sem.at[slot]))
        return copies

    def w_start(s):
        if s < STEPS:
            for copy in w_copies(s):
                copy.start()

    def w_wait(s):
        wait_all(ring.at[s % NS], w_sem.at[s % NS])

    IDS, GATES = NCH, NCH + 1

    def over_y(i):
        return i % 2 == 1

    def own_core(i):
        return tok.at[i, my_c]

    def own_pair(i):
        return tok.at[i, my_c, my_x if over_y(i) else my_dp]

    def own(i):
        if i == IDS:
            return mids.at[my_pos]
        if i == GATES:
            return mgates.at[my_pos]
        return tok.at[i, my_c, my_x, my_dp] if over_y(i) else tok.at[i, my_c, my_dp, my_x]

    def load(i):
        src = ids_ref if i == IDS else gates_ref if i == GATES else x_ref.at[:, pl.ds(i * T, T)]
        return pltpu.make_async_copy(src, own(i), ld_sem.at[max(0, i - NCH + 1)])

    def remote(src, dst, ssem, rsem, dev):
        return pltpu.make_async_remote_copy(
            src_ref=src, dst_ref=dst, send_sem=ssem, recv_sem=rsem, device_id=dev, device_id_type=MESH)

    def gather1(i):
        return remote(own(i), own(i), g1s, g1r.at[i // 2], y_nbr if over_y(i) else x_nbr)

    def gather2(i):
        return remote(own_pair(i), own_pair(i), g2s, g2r.at[i // 2], x_nbr if over_y(i) else y_nbr)

    def gatherd(i):
        return remote(own_core(i), own_core(i), gds, gdr.at[i // 2], partner)

    routing = [IDS, GATES]
    items = routing + list(range(NCH))

    def peer(r):
        dp = 1 - my_dp if r & 1 else my_dp
        x = 1 - my_x if r & 2 else my_x
        c = 1 - my_c if r & 4 else my_c
        return dp, x * 2 + c

    def tell(i, r):
        return remote(own(i), own(i), rts.at[i - NCH], rtr.at[i - NCH], peer(r))

    barrier = pltpu.get_barrier_semaphore()
    for r in range(1, 8):
        pl.semaphore_signal(barrier, inc=1, device_id=peer(r), device_id_type=MESH)
    for i in items:
        load(i).start()
    hid3[...] = jnp.zeros_like(hid3)
    wait_all(tok.at[0], ld_sem.at[0])
    for i in routing:
        load(i).wait()
    pl.semaphore_wait(barrier, 7)

    def direct(i, r):
        return remote(own(i), own(i), g1s, g2r.at[i // 2], peer(r))

    def send(p):
        for i in (2 * p, 2 * p + 1):
            gather1(i).start()

    def send_on(p):
        wait_all(tok.at[2 * p, 0, 0], g1r.at[p])
        for i in (2 * p, 2 * p + 1):
            gather2(i).start()

    def share(p):
        wait_all(tok.at[pl.ds(0, 3), 0, 0] if p < 2 else tok.at[2 * p, 0], g2r.at[p])
        for i in (2 * p, 2 * p + 1):
            gatherd(i).start()

    for r in (3, 7, 1, 2, 5, 6, 4):
        for i in routing:
            tell(i, r).start()
    for p in range(2):
        for r in (3, 2, 1):
            for i in (2 * p, 2 * p + 1):
                direct(i, r).start()
    for s in range(NS):
        w_start(s)
    wait_all(mids.at[pl.ds(0, 7)], rtr.at[0])
    wait_all(mgates.at[pl.ds(0, 7)], rtr.at[1])

    e_id = lax.broadcasted_iota(jnp.int32, (LOCAL, GROUP), 0) + (my_ep * (2 * LOCAL) + e_off)
    s_id = lax.broadcasted_iota(jnp.int32, (LOCAL, CAP, GROUP), 1).astype(F32)

    def true_pos(t):
        return ((t // 64) % 2) * 128 + (t // 128) * 64 + t % 64

    t_row = lax.broadcasted_iota(jnp.int32, (GROUP, GROUP), 0)
    t_col = lax.broadcasted_iota(jnp.int32, (GROUP, GROUP), 1)
    before = jnp.where(true_pos(t_row) < true_pos(t_col), 1.0, 0.0).astype(BF16)
    eye = jnp.where(t_row == t_col, 1.0, 0.0).astype(BF16)
    for g in range(2):
        ids = jnp.concatenate([mids[c * 4 + g * 2 + x] for c in range(2) for x in range(2)], axis=1)
        gates = jnp.concatenate([mgates[c * 4 + g * 2 + x] for c in range(2) for x in range(2)], axis=1)
        chosen = jnp.zeros((LOCAL, GROUP), F32)
        gate = jnp.zeros((LOCAL, GROUP), F32)
        for j in range(TOPK):
            hit = ids[j:j + 1, :] == e_id
            chosen = jnp.where(hit, 1.0, chosen)
            gate = jnp.where(hit, gates[j:j + 1, :], gate)
        slot = dot(chosen.astype(BF16), before)
        slot = jnp.where(chosen > 0.0, slot, -1.0)
        here = slot[:, None, :] == s_id
        disp[g] = jnp.where(here, 1.0, 0.0).reshape(LOCAL * CAP, GROUP).astype(BF16)
        weight = jnp.where(here, gate[:, None, :], 0.0).reshape(LOCAL * CAP, GROUP)
        for piece in range(3):
            part = weight.astype(BF16)
            turned = tdot(part, eye).astype(BF16)
            if piece < 2:
                comb[g, :, pl.ds(piece * GROUP, GROUP)] = turned
            else:
                comb3[g] = turned
            weight = weight - part.astype(F32)

    send(2)
    send(3)
    share(0)
    for k in range(NK):
        wait_all(tok.at[2 * k], gdr.at[k])
        for h in range(2):
            i = 2 * k + h
            for g in range(2):
                rows = tok[i, :, :, g] if over_y(i) else tok[i, :, g]
                picked = dot(disp[g], rows.reshape(GROUP, T)).astype(BF16)
                xs[:, pl.ds(g * CAP, CAP), pl.ds(h * T, T)] = picked.reshape(LOCAL, CAP, T)
        for half in range(2):
            steps = [k * NEG + half * 2 + q for q in range(2)]
            for s in steps:
                w_wait(s)
            for s in steps:
                eg = s % NEG
                batch = pl.ds(eg * EG, EG)
                for n in range(NF):
                    cols = pl.ds(n * T, T)
                    acc = bdot(xs[batch], ring[s % NS, n].reshape(EG, KS, T))
                    if k > 0:
                        acc = acc + hacc[batch, :, cols]
                    if k < NK - 1:
                        hacc[batch, :, cols] = acc
                        continue
                    act = jax.nn.gelu(acc).astype(BF16)
                    if n < 2:
                        hid[batch, :, cols] = act
                    else:
                        act = act.reshape(EG // 2, 2, 2 * CAP, T)
                        for m in range(2):
                            hid3[pl.ds(eg * EG // 2, EG // 2), pl.ds(m * 2 * CAP, 2 * CAP), pl.ds(m * T, T)] = act[:, m]
            for s in steps:
                w_start(s + NS)
            if half == 0 and k < NK - 1:
                share(k + 1)
                if k == 0:
                    send_on(2)
                    send_on(3)

    def route(d):
        if d == 0:
            return my_x, my_dp, x_nbr, y_nbr
        return my_dp, my_x, y_nbr, x_nbr

    def reduce0(c):
        return remote(ypart.at[c, 1 - my_c], r0.at[c], t0s, t0r.at[c], partner)

    def reduce1(c, d, last):
        a, b, dev, _ = route(d)
        side = b if last else 1 - b
        return remote(ypart.at[c, my_c, d, 1 - a, side], r1.at[c, d, side], t1s, fin.at[c] if last else t1r.at[c], dev)

    def reduce2(c, d):
        a, b, _, dev = route(d)
        return remote(ypart.at[c, my_c, d, a, 1 - b], r2.at[c, d], t2s, fin.at[c], dev)

    def stage1(c):
        reduce0(c).wait_recv()
        for last in range(2):
            for d in range(2):
                a, b, _, _ = route(d)
                side = b if last else 1 - b
                ypart[c, my_c, d, 1 - a, side] = ypart[c, my_c, d, 1 - a, side] + r0[c, d, 1 - a, side]
        for last in range(2):
            for d in range(2):
                reduce1(c, d, last).start()
        for d in range(2):
            a, _, _, _ = route(d)
            ypart[c, my_c, d, a] = ypart[c, my_c, d, a] + r0[c, d, a]

    def stage2(c):
        wait_all(r1.at[c, 0], t1r.at[c])
        for d in range(2):
            a, b, _, _ = route(d)
            ypart[c, my_c, d, a, 1 - b] = ypart[c, my_c, d, a, 1 - b] + r1[c, d, 1 - b]
        for d in range(2):
            reduce2(c, d).start()

    def final(c):
        wait_all(r0.at[c, 0], fin.at[c])
        for d in range(2):
            a, b, _, _ = route(d)
            moe = ypart[c, my_c, d, a, b] + r1[c, d, b] + r2[c, d]
            x_own = own(c)[:, pl.ds(d * H, H)].astype(F32)
            shared = shy[:, pl.ds(c * T + d * H, H)].astype(F32)
            o_ref[:, pl.ds(c * T + d * H, H)] = (x_own + shared + moe).astype(BF16)

    for c in range(NCH):
        for h in range(NHB):
            s = A_STEPS + c * NHB + h
            w_wait(s)
            third = bdot(hid3[pl.ds(h * EG, EG)], ring[s % NS, 2].reshape(EG, 2 * T, T)).reshape(EB, 2 * CAP, T)
            for q in range(2):
                first = h * EB + q * EG
                out = bdot(hid[pl.ds(first, EG)], ring[s % NS, q].reshape(EG, 2 * T, T))
                out = (out + third[q * EG:(q + 1) * EG]).astype(BF16)
                for g in range(2):
                    for copy in range(2):
                        osc[g, copy, pl.ds(first, EG)] = out[:, g * CAP:(g + 1) * CAP]
            w_start(s + NS)
        if c >= 1:
            stage1(c - 1)
        if c >= LAG2:
            stage2(c - LAG2)
        for g in range(2):
            y = dot(comb[g], osc[g].reshape(2 * GROUP, T)) + dot(comb3[g], osc[g, 0].reshape(GROUP, T))
            y = y.reshape(2, 2, ROWS, T)
            for core in range(2):
                for x in range(2):
                    ypart[c, core, 0, x, g] = y[core, x, :, :H]
                    ypart[c, core, 1, g, x] = y[core, x, :, H:]
        reduce0(c).start()

    w_wait(SH_IN)
    for n in range(NF):
        acc = jnp.zeros((ROWS, T), F32)
        weights = ring[SH_IN % NS, n].reshape(NCH, T, T)
        for k in range(NCH):
            acc = acc + dot(own(k)[...], weights[k])
        hs[:, pl.ds(n * T, T)] = jax.nn.gelu(acc).astype(BF16)
    stage1(NCH - 1)
    stage2(NCH - 3)
    w_wait(SH_OUT)
    for c in range(NCH):
        acc = jnp.zeros((ROWS, T), F32)
        for j in range(NF):
            acc = acc + dot(hs[:, pl.ds(j * T, T)], ring[SH_OUT % NS, j, c // 2, c % 2])
        shy[:, pl.ds(c * T, T)] = acc.astype(BF16)
    stage2(NCH - 2)
    stage2(NCH - 1)
    for c in range(NCH):
        final(c)
    wait_all(mids.at[pl.ds(0, 7)], rts.at[0])
    wait_all(mgates.at[pl.ds(0, 7)], rts.at[1])
    wait_all(tok.at[pl.ds(0, 2)], g1s)
    wait_all(tok.at[0], g2s)
    wait_all(tok.at[pl.ds(0, 4)], gds)
    wait_all(r0, t0s)
    wait_all(r1, t1s)
    wait_all(r2, t2s)


def solution(mesh):
    def layer(tok_x, route_ids, route_gate, w_in, w_out, shared_in, shared_out):
        local = w_in.shape[0]
        any_space = pl.BlockSpec(memory_space=pl.ANY)
        dma = pltpu.SemaphoreType.DMA
        vmem = pltpu.VMEM
        return pl.pallas_call(
            kernel,
            out_shape=pltpu.VMEM((ROWS, WIDTH), BF16),
            in_specs=[any_space] * 8,
            out_specs=pl.BlockSpec(memory_space=pltpu.VMEM),
            scratch_shapes=[
                vmem((NCH, 2, 2, 2, ROWS, T), BF16),
                vmem((8, TOPK, ROWS), jnp.int32),
                vmem((8, TOPK, ROWS), F32),
                vmem((NS, NF, EG, 2, T, T), BF16),
                vmem((LOCAL, 2 * CAP, KS), BF16),
                vmem((LOCAL, 2 * CAP, FF), F32),
                vmem((LOCAL, 2 * CAP, 2 * T), BF16),
                vmem((LOCAL // 2, 4 * CAP, 2 * T), BF16),
                vmem((2, 2, LOCAL, CAP, T), BF16),
                vmem((2, LOCAL * CAP, GROUP), BF16),
                vmem((2, GROUP, 2 * GROUP), BF16),
                vmem((2, GROUP, GROUP), BF16),
                vmem((NCH, 2, 2, 2, 2, ROWS, H), F32),
                vmem((NCH, 2, 2, 2, ROWS, H), F32),
                vmem((NCH, 2, 2, ROWS, H), F32),
                vmem((NCH, 2, ROWS, H), F32),
                vmem((ROWS, FF), BF16),
                vmem((ROWS, WIDTH), BF16),
                dma((3,)), dma((2,)), dma((2,)),
                dma, dma((NK,)), dma, dma((NK,)), dma, dma((NK,)),
                dma((NS,)),
                dma, dma((NCH,)), dma, dma((NCH,)), dma, dma((NCH,)),
            ],
            compiler_params=pltpu.CompilerParams(
                collective_id=0, has_side_effects=True, vmem_limit_bytes=61_000_000),
            name='moe_layer',
        )(tok_x, route_ids.T, route_gate.T,
          w_in.reshape(local, WIDTH // T, T, FF), w_out.reshape(local, NF, T, WIDTH),
          w_out.reshape(local // 2, 2, NF, T, WIDTH),
          shared_in.reshape(EG, 2, T, FF), shared_out.reshape(NF, T, WIDTH))

    row_spec = P(('dp', 'ep'), None)
    expert_spec = P('ep', None, None)
    whole_spec = P(None, None)
    return jax.shard_map(layer, mesh=mesh,
                         in_specs=(row_spec, row_spec, row_spec, expert_spec, expert_spec, whole_spec, whole_spec),
                         out_specs=row_spec, check_vma=False)
```
